128 devices in a mesh: row: 8 (over x, y_hi), col: 16 (over y_lo, z, core).
Axes of the slice: x: 4, y: 4 (y_hi: 2, y_lo: 2; y = y_hi * 2 + y_lo), z: 4, core: 2. Of those that a mesh axis runs over, the one named last changes fastest.
Arguments:
- tokens: bfloat16 [256, 1024, 192], P('row', 'col'), may hold values from -6 to 6
- norm_gain: float32 [2, 3, 192], replicated, may hold values from 0.1 to 1.9
- qkv_weight: bfloat16 [2, 192, 576], replicated, may hold values from -0.4375 to 0.4375
- proj_weight: bfloat16 [2, 192, 192], replicated, may hold values from -0.4375 to 0.4375
- bias_table: float32 [2, 6, 225], replicated, may hold values from -4 to 4
- conv_weight: float32 [2, 49, 192], replicated, may hold values from -0.875 to 0.875
- up_weight: bfloat16 [2, 192, 768], replicated, may hold values from -0.4375 to 0.4375
- down_weight: bfloat16 [2, 768, 192], replicated, may hold values from -0.21875 to 0.21875
Outputs:
- mixed: bfloat16 [256, 1024, 192], P('row', 'col')
The draws below stay inside these ranges and needn't reach their ends.
All inputs are finite; a program needn't handle non-finite values.
Results may differ from the reference program's by a relative error of at most 0.013.
Values may be sent and summed in bfloat16 or wider, within the bound.
No kernel may reach another device: no remote copies, remote signals or barrier semaphores. Data moves between devices by JAX's collectives and lax.ppermute only.
A program may use at most 64 MiB of HBM per device.

```python
import math
import jax
import jax.numpy as jnp
from jax import lax

D = 192
HEADS = 6
HID = 768
WS = 8
KS = 7
LAYERS = 2
HEAD = 32
ROWS = 256
COLS = 1024


def block_scale(key, dims, split, low, high):
    loudness = 1.0
    for dim, shards_of in split:
        steps = jax.random.uniform(jax.random.fold_in(jax.random.fold_in(key, 6), dim), (shards_of,), jnp.float32, low / len(split), high / len(split))
        loudness = loudness * jnp.repeat(jnp.exp(steps), dims[dim] // shards_of).reshape((-1,) + (1,) * (len(dims) - 1 - dim))
    return loudness


def scatter_about(stream_key, dims, scale, bound, pieces=(), held_as=jnp.bfloat16):
    factor_of = block_scale(stream_key, dims, pieces, -0.22, 0.18) if pieces else 1.0
    values = jax.random.normal(stream_key, dims, jnp.float32) * scale * factor_of
    return jnp.minimum(jnp.maximum(values, -bound), bound).astype(held_as)


def setup_inputs(seed: int = 0) -> dict:
    streams_of = jax.random.split(jax.random.key(seed), 9)
    return {
        "tokens": scatter_about(streams_of[0], (ROWS, COLS, D), 1.0, 6.0, ((0, 8), (1, 16))),
        "norm_gain": jnp.clip(1.0 + 0.18 * jax.random.normal(streams_of[1], (LAYERS, 3, D), jnp.float32), 0.1, 1.9),
        "qkv_weight": scatter_about(streams_of[2], (LAYERS, D, 3 * D), D ** -0.5, 0.4375),
        "proj_weight": scatter_about(streams_of[3], (LAYERS, D, D), D ** -0.5, 0.4375),
        "bias_table": scatter_about(streams_of[4], (LAYERS, HEADS, (2 * WS - 1) * (2 * WS - 1)), 1.0, 4.0, (), jnp.float32),
        "conv_weight": scatter_about(streams_of[5], (LAYERS, KS * KS, D), (KS * KS) ** -0.5, 0.875, (), jnp.float32),
        "up_weight": scatter_about(streams_of[6], (LAYERS, D, HID), D ** -0.5, 0.4375),
        "down_weight": scatter_about(streams_of[7], (LAYERS, HID, D), HID ** -0.5, 0.21875),
    }


epsilon = 1e-05

def layer_norm(values, scaling):
    values = values.astype(jnp.float32)
    centre = lax.optimization_barrier(jnp.mean(values, axis=-1, keepdims=True))
    centred = values - centre
    spread = lax.optimization_barrier(jnp.mean(centred * centred, axis=-1, keepdims=True))
    return (centred * lax.rsqrt(spread + epsilon) * scaling).astype(jnp.bfloat16)

def position_bias(lookup_table):
    window_area = WS * WS
    places = jnp.arange(window_area, dtype=jnp.int32)
    place_row = places // WS
    place_col = places % WS
    offsets = (place_row[:, None] - place_row[None, :] + WS - 1) * (2 * WS - 1) + (place_col[:, None] - place_col[None, :] + WS - 1)
    entries = jnp.arange((2 * WS - 1) * (2 * WS - 1), dtype=jnp.int32)
    selector = (offsets.reshape(-1)[:, None] == entries[None, :]).astype(jnp.float32)
    expanded = jnp.dot(selector, lookup_table.T, precision=lax.Precision.HIGHEST)
    return expanded.reshape(window_area, window_area, HEADS).transpose(2, 0, 1)

def window_attention(windows, qkv_matrix, proj_matrix, score_bias):
    window_count = windows.shape[0]
    projected = jnp.dot(windows.reshape(-1, D), qkv_matrix, preferred_element_type=jnp.float32)
    projected = projected.astype(jnp.bfloat16).reshape(window_count, WS * WS, 3, HEADS, HEAD)
    query = projected[:, :, 0].astype(jnp.float32)
    keys_all = projected[:, :, 1].astype(jnp.float32)
    value_all = projected[:, :, 2].astype(jnp.float32)
    scores = jnp.einsum('wqhd,wkhd->whqk', query, keys_all, precision=lax.Precision.HIGHEST)
    scores = scores * HEAD ** (-0.5) + score_bias[None]
    weights = jnp.exp(scores)
    attention_weights = (weights / lax.optimization_barrier(jnp.sum(weights, axis=-1, keepdims=True))).astype(jnp.bfloat16)
    attended = jnp.einsum('whqk,wkhd->wqhd', attention_weights.astype(jnp.float32), value_all, precision=lax.Precision.HIGHEST)
    attended = attended.astype(jnp.bfloat16).reshape(window_count * WS * WS, D)
    branch = jnp.dot(attended, proj_matrix, preferred_element_type=jnp.float32).astype(jnp.bfloat16)
    return branch.reshape(window_count, WS * WS, D)

def shuffle_windows(token_grid):
    height, width = (token_grid.shape[0], token_grid.shape[1])
    return token_grid.reshape(WS, height // WS, WS, width // WS, D).transpose(1, 3, 0, 2, 4).reshape(-1, WS * WS, D)

def shuffle_back(windows, height, width):
    return windows.reshape(height // WS, width // WS, WS, WS, D).transpose(2, 0, 3, 1, 4).reshape(height, width, D)

def plain_windows(token_grid):
    height, width = (token_grid.shape[0], token_grid.shape[1])
    return token_grid.reshape(height // WS, WS, width // WS, WS, D).transpose(0, 2, 1, 3, 4).reshape(-1, WS * WS, D)

def plain_back(windows, height, width):
    return windows.reshape(height // WS, width // WS, WS, WS, D).transpose(0, 2, 1, 3, 4).reshape(height, width, D)

def depthwise(padded, kernel, height, width):
    accumulated = jnp.zeros((height, width, D), jnp.float32)
    for tap_row in range(KS):
        for tap_col in range(KS):
            accumulated = accumulated + padded[tap_row:tap_row + height, tap_col:tap_col + width].astype(jnp.float32) * kernel[tap_row * KS + tap_col]
    return accumulated

def feed_forward(normed, up_matrix, down_matrix):
    hidden = jax.nn.gelu(jnp.dot(normed, up_matrix, preferred_element_type=jnp.float32), approximate=False).astype(jnp.bfloat16)
    return jnp.dot(hidden, down_matrix, preferred_element_type=jnp.float32)

def reference(tokens, norm_gain, qkv_weight, proj_weight, bias_table, conv_weight, up_weight, down_weight):
    height, width = (tokens.shape[0], tokens.shape[1])
    halo_width = KS // 2
    current = tokens
    for layer_index in range(LAYERS):
        normed = layer_norm(current, norm_gain[layer_index, 0])
        if layer_index % 2 == 1:
            windows = shuffle_windows(normed)
        else:
            windows = plain_windows(normed)
        score_bias = position_bias(bias_table[layer_index])
        window_count = windows.shape[0]
        group_size = math.gcd(window_count, 256)
        qkv_matrix = qkv_weight[layer_index]
        proj_matrix = proj_weight[layer_index]
        attended = lax.map(lambda window_block: window_attention(window_block, qkv_matrix, proj_matrix, score_bias), windows.reshape(window_count // group_size, group_size, WS * WS, D))
        attended = attended.reshape(window_count, WS * WS, D)
        if layer_index % 2 == 1:
            branch = shuffle_back(attended, height, width)
        else:
            branch = plain_back(attended, height, width)
        after_attention = current.astype(jnp.float32) + branch.astype(jnp.float32)
        normed_two = layer_norm(after_attention, norm_gain[layer_index, 1])
        padded = jnp.pad(normed_two, ((halo_width, halo_width), (halo_width, halo_width), (0, 0)))
        after_conv = after_attention + depthwise(padded, conv_weight[layer_index], height, width)
        stripe_rows = math.gcd(height, 16)
        gain_three = norm_gain[layer_index, 2]
        up_matrix = up_weight[layer_index]
        down_matrix = down_weight[layer_index]

        def finish(rows_in):
            flat_rows = rows_in.reshape(-1, D)
            normed_three = layer_norm(flat_rows, gain_three)
            return (flat_rows + feed_forward(normed_three, up_matrix, down_matrix)).astype(jnp.bfloat16).reshape(rows_in.shape)
        current = lax.map(finish, after_conv.reshape(height // stripe_rows, stripe_rows, width, D)).reshape(height, width, D)
    return current
```

```python
import functools
import jax
import jax.numpy as jnp
from jax import lax
from jax.experimental import pallas as pl
from jax.experimental.pallas import tpu as pltpu
from jax.sharding import Mesh, PartitionSpec as P

D = 192
HEADS = 6
HID = 768
WS = 8
KS = 7
HEAD = 32
AREA = WS * WS
PAD = 256
LANES = 128
HALO = KS // 2
STRIDE = 40
EPSILON = 1e-05

f32 = jnp.float32
bf16 = jnp.bfloat16


def layer_norm(values, gain):
    centre = jnp.mean(values, axis=-1, keepdims=True)
    centred = values - centre
    spread = jnp.mean(centred * centred, axis=-1, keepdims=True)
    return centred * lax.rsqrt(spread + EPSILON) * gain


def mxu(a, b):
    return jnp.dot(a, b, preferred_element_type=f32)


def prepare_attention(table_ref, qkv_ref, bias_s, rows_s, qkv_s):
    table = table_ref[0]
    high = table.astype(bf16)
    rest = table - high.astype(f32)
    middle = rest.astype(bf16)
    low = (rest - middle.astype(f32)).astype(bf16)
    entries = (2 * WS - 1) ** 2
    lane = lax.broadcasted_iota(jnp.int32, (entries, WS * LANES), 1)
    entry = lax.broadcasted_iota(jnp.int32, (entries, WS * LANES), 0)
    target = (
        (2 * WS - 2 - ((lane & (LANES - 1)) >> 3)) * (2 * WS - 1)
        + (lane >> 7)
        - (lane & 7)
        + WS
        - 1
    )
    chosen = jnp.where(entry == target, 1.0, 0.0).astype(bf16)
    spread = mxu(high, chosen) + mxu(middle, chosen) + mxu(low, chosen)
    for place in range(WS):
        rows_s[place, 0:HEADS, :] = spread[:, place * LANES : (place + 1) * LANES]
    first = lax.broadcasted_iota(jnp.int32, (WS, LANES), 1) < AREA
    for group in range(HEADS // 2):
        left = rows_s[:, 2 * group, :]
        right = rows_s[:, 2 * group + 1, :]
        for row in range(WS):
            shift = LANES - (WS - 1 - row) * WS
            piece = jnp.where(
                first,
                pltpu.roll(left, shift % LANES, 1),
                pltpu.roll(right, (shift + AREA) % LANES, 1),
            )
            bias_s[group * AREA + row * WS : group * AREA + (row + 1) * WS, :] = piece
    weights = qkv_ref[0].astype(f32)
    gap = jnp.zeros((D, PAD - D), f32)
    qkv_s[...] = jnp.concatenate(
        [
            weights[:, 0:D],
            gap,
            weights[:, D : 2 * D],
            gap,
            weights[:, 2 * D : 3 * D],
            gap,
        ],
        axis=1,
    ).astype(bf16)


def attention_masks():
    lane = lax.broadcasted_iota(jnp.int32, (1, PAD), 1)
    groups = [
        jnp.where((lane >> 6) == g, 1.0, 0.0).astype(bf16) for g in range(HEADS // 2)
    ]
    parities = [
        jnp.where(((lane >> 5) & 1) == h, 1.0, 0.0).astype(bf16) for h in range(2)
    ]
    rows = lax.broadcasted_iota(jnp.int32, (LANES, LANES), 0) >> 6
    cols = lax.broadcasted_iota(jnp.int32, (LANES, LANES), 1) >> 6
    summing = jnp.where(rows == cols, 1.0, 0.0).astype(bf16)
    return groups, parities, summing


def attend(q, k, v, bias, masks):
    groups, parities, summing = masks
    queries = jnp.concatenate([q * m for m in groups], axis=0)
    keys = jnp.concatenate([k * m for m in parities], axis=0)
    values = jnp.concatenate([v * m for m in parities], axis=0)
    scores = lax.dot_general(
        queries, keys, (((1,), (1,)), ((), ())), preferred_element_type=f32
    )
    weights = jnp.exp(scores * HEAD ** (-0.5) + bias)
    total = mxu(weights.astype(bf16), summing)
    attention_weights = (weights / total).astype(bf16)
    mixed = mxu(attention_weights, values)
    lane = lax.broadcasted_iota(jnp.int32, (AREA, PAD), 1) >> 6
    return jnp.where(
        lane == 0,
        mixed[0:AREA],
        jnp.where(lane == 1, mixed[AREA : 2 * AREA], mixed[2 * AREA : 3 * AREA]),
    )


def plain_kernel(
    x_ref, gain_ref, qkv_ref, proj_ref, table_ref, sum_ref, normed_ref, bias_s, rows_s, qkv_s
):
    @pl.when(pl.program_id(0) == 0)
    def _():
        prepare_attention(table_ref, qkv_ref, bias_s, rows_s, qkv_s)

    cols = x_ref.shape[1]
    count = cols // WS
    grid = x_ref[...].astype(f32)
    current = jnp.concatenate(
        [grid[:, j * WS : (j + 1) * WS, :].reshape(AREA, D) for j in range(count)], axis=0
    )
    normed = layer_norm(current, gain_ref[0, 0:1, :]).astype(bf16)
    projected = mxu(normed, qkv_s[...]).astype(bf16)
    masks = attention_masks()
    bias = bias_s[...]
    outs = []
    for j in range(count):
        rows = projected[j * AREA : (j + 1) * AREA]
        outs.append(
            attend(
                rows[:, 0:PAD], rows[:, PAD : 2 * PAD], rows[:, 2 * PAD : 3 * PAD], bias, masks
            )[:, 0:D].astype(bf16)
        )
    branch = mxu(jnp.concatenate(outs, axis=0), proj_ref[0]).astype(bf16)
    after = current + branch.astype(f32)
    normed_two = layer_norm(after, gain_ref[0, 1:2, :])

    def spatial(value):
        return jnp.concatenate(
            [value[j * AREA : (j + 1) * AREA].reshape(WS, WS, D) for j in range(count)], axis=1
        )

    sum_ref[...] = spatial(after)
    normed_ref[...] = spatial(normed_two).astype(bf16)


def attention_scratch():
    return [
        pltpu.VMEM((HEADS // 2 * AREA, LANES), f32),
        pltpu.VMEM((WS, WS, LANES), f32),
        pltpu.VMEM((D, 3 * PAD), bf16),
    ]


def plain_attention(tokens, norm_gain, qkv_weight, proj_weight, bias_table, layer):
    height, width = tokens.shape[:2]
    whole = lambda *shape: pl.BlockSpec(
        (1, *shape), lambda i: (layer,) + (0,) * len(shape)
    )
    block = pl.BlockSpec((WS, width, D), lambda i: (i, 0, 0))
    return pl.pallas_call(
        plain_kernel,
        grid=(height // WS,),
        in_specs=[
            block,
            whole(3, D),
            whole(D, 3 * D),
            whole(D, D),
            whole(HEADS, (2 * WS - 1) ** 2),
        ],
        out_specs=[block, block],
        out_shape=[
            jax.ShapeDtypeStruct(tokens.shape, f32),
            jax.ShapeDtypeStruct(tokens.shape, bf16),
        ],
        scratch_shapes=attention_scratch(),
        name="plain_attention",
    )(tokens, norm_gain, qkv_weight, proj_weight, bias_table)


def pack(value):
    half = value.shape[1] // 2
    upper = jnp.concatenate(
        [value[:, :half, LANES:D], value[:, half:, LANES:D]], axis=-1
    )
    return jnp.concatenate([value[:, :, :LANES], upper], axis=1)


def unpack(value):
    count = value.shape[1] * LANES // D
    upper = value[:, count:, :]
    upper = jnp.concatenate(
        [upper[:, :, : D - LANES], upper[:, :, D - LANES :]], axis=1
    )
    return jnp.concatenate([value[:, :count, :], upper], axis=-1)


def shuffled_kernel(
    got_ref, qkv_ref, proj_ref, table_ref, out_ref, bias_s, rows_s, qkv_s, projected_s, attended_s
):
    prepare_attention(table_ref, qkv_ref, bias_s, rows_s, qkv_s)
    count = got_ref.shape[1] * LANES // D
    step = 8

    def project(c, carry):
        rows = unpack(got_ref[pl.ds(c * step, step)].astype(f32)).reshape(step * count, D)
        projected = mxu(rows.astype(bf16), qkv_s[...])
        for p in range(step):
            for t in range(6):
                projected_s[t, pl.ds((c * step + p) * STRIDE, count), :] = projected[
                    p * count : (p + 1) * count, t * LANES : (t + 1) * LANES
                ]
        return carry

    lax.fori_loop(0, AREA // step, project, 0)
    masks = attention_masks()
    unroll = 4

    def windows(c, carry):
        for n in range(unroll):
            w = c * unroll + n
            parts = [
                jnp.concatenate(
                    [
                        projected_s[2 * t, pl.ds(w, AREA, stride=STRIDE), :],
                        projected_s[2 * t + 1, pl.ds(w, AREA, stride=STRIDE), :],
                    ],
                    axis=1,
                ).astype(bf16)
                for t in range(3)
            ]
            result = attend(*parts, bias_s[...], masks)
            for t in range(2):
                attended_s[t, pl.ds(w, AREA, stride=STRIDE), :] = result[
                    :, t * LANES : (t + 1) * LANES
                ]
        return carry

    lax.fori_loop(0, count // unroll, windows, 0)

    def finish(c, carry):
        rows = jnp.concatenate(
            [
                jnp.concatenate(
                    [
                        attended_s[t, pl.ds((c * step + p) * STRIDE, count), :]
                        for p in range(step)
                    ],
                    axis=0,
                )
                for t in range(2)
            ],
            axis=1,
        )[:, 0:D]
        branch = mxu(rows.astype(bf16), proj_ref[0])
        out_ref[pl.ds(c * step, step)] = pack(branch.reshape(step, count, D)).astype(bf16)
        return carry

    lax.fori_loop(0, AREA // step, finish, 0)


def shuffled_attention(got, qkv_weight, proj_weight, bias_table, layer):
    whole = lambda *shape: pl.BlockSpec(
        (1, *shape), lambda i: (layer,) + (0,) * len(shape)
    )
    block = pl.BlockSpec(got.shape, lambda i: (0, 0, 0))
    return pl.pallas_call(
        shuffled_kernel,
        grid=(1,),
        in_specs=[block, whole(D, 3 * D), whole(D, D), whole(HEADS, (2 * WS - 1) ** 2)],
        out_specs=block,
        out_shape=jax.ShapeDtypeStruct(got.shape, bf16),
        scratch_shapes=attention_scratch()
        + [
            pltpu.VMEM((6, AREA * STRIDE, LANES), f32),
            pltpu.VMEM((2, AREA * STRIDE, LANES), f32),
        ],
        name="shuffled_attention",
    )(got, qkv_weight, proj_weight, bias_table)


def residual_kernel(back_ref, current_ref, gain_ref, sum_ref, normed_ref):
    rows, cols, _ = current_ref.shape
    count = back_ref.shape[1] * LANES // D
    high = count // WS
    branch = unpack(back_ref[...].astype(f32)).reshape(rows // high, cols // WS, high, WS, D)
    branch = branch.transpose(0, 2, 1, 3, 4).reshape(rows, cols, D)
    after = current_ref[...].astype(f32) + branch
    sum_ref[...] = after
    normed_ref[...] = layer_norm(after, gain_ref[0, 1:2, :]).astype(bf16)


def residual(back, current, norm_gain, layer):
    height, width = current.shape[:2]
    steps = height // WS
    block = pl.BlockSpec((WS, width, D), lambda i: (i, 0, 0))
    return pl.pallas_call(
        residual_kernel,
        grid=(steps,),
        in_specs=[
            pl.BlockSpec((back.shape[0] // steps, *back.shape[1:]), lambda i: (i, 0, 0)),
            block,
            pl.BlockSpec((1, 3, D), lambda i: (layer, 0, 0)),
        ],
        out_specs=[block, block],
        out_shape=[
            jax.ShapeDtypeStruct(current.shape, f32),
            jax.ShapeDtypeStruct(current.shape, bf16),
        ],
        name="residual",
    )(back, current, norm_gain)


def finish_kernel(send, *refs):
    (
        sum_ref,
        normed_ref,
        top_ref,
        bottom_ref,
        left_ref,
        right_ref,
        gain_ref,
        next_ref,
        taps_ref,
        up_ref,
        down_ref,
        out_ref,
        *refs,
    ) = refs
    if send:
        send_ref, *refs = refs
    padded_s, after_s, taps_s = refs
    step = pl.program_id(0)
    height, width, _ = normed_ref.shape
    rows = sum_ref.shape[0]

    @pl.when(step == 0)
    def _():
        def place(r, middle):
            padded_s[r] = jnp.concatenate(
                [left_ref[r].astype(f32), middle.astype(f32), right_ref[r].astype(f32)], axis=0
            ).astype(bf16)

        for r in range(HALO):
            place(r, top_ref[r])
            place(height + HALO + r, bottom_ref[r])

        def body(r, carry):
            place(r + HALO, normed_ref[r])
            return carry

        lax.fori_loop(0, height, body, 0)
        for t in range(KS * KS):
            taps_s[t] = jnp.broadcast_to(taps_ref[0, t : t + 1, :], (16, D)).astype(bf16)

    def row(r, carry):
        total = sum_ref[r]
        for v in range(KS):
            part = None
            for u in range(KS):
                x = padded_s[step * rows + r + u].reshape(-1, 16, D)
                term = x * taps_s[u * KS + v][None]
                part = term if part is None else part + term
            part = part.reshape(-1, D).astype(f32)
            start = WS - HALO + v
            total = total + part[start : start + width]
        after_s[pl.ds(pl.multiple_of(r * width, width), width), :] = total
        return carry

    lax.fori_loop(0, rows, row, 0)
    after = after_s[...]
    normed = layer_norm(after, gain_ref[0, 2:3, :]).astype(bf16)
    raised = mxu(normed, up_ref[0])
    hidden = (0.5 * raised * (1.0 + lax.erf(raised * 0.5**0.5))).astype(bf16)
    outcome = (after + mxu(hidden, down_ref[0])).astype(bf16)
    out_ref[...] = outcome.reshape(rows, width, D)
    if send:
        normed = layer_norm(outcome.astype(f32), next_ref[0, 0:1, :])
        high = send_ref.shape[1] * LANES // D // WS
        pieces = normed.reshape(rows // high, high, width // WS, WS, D)
        pieces = pieces.transpose(0, 2, 1, 3, 4).reshape(-1, high * WS, D)
        send_ref[...] = pack(pieces).astype(bf16)


def finish_layer(
    after, normed, halo, norm_gain, conv_weight, up_weight, down_weight, layer, send, group
):
    height, width = normed.shape[:2]
    steps = height // WS
    whole = lambda *shape: pl.BlockSpec(
        (1, *shape), lambda i: (layer,) + (0,) * len(shape)
    )
    full = lambda a: pl.BlockSpec(a.shape, lambda i: (0,) * a.ndim)
    block = pl.BlockSpec((WS, width, D), lambda i: (i, 0, 0))
    out_specs = [block]
    out_shape = [jax.ShapeDtypeStruct(normed.shape, bf16)]
    if send:
        rows = height * width // group * D // LANES
        out_specs.append(pl.BlockSpec((group // steps, rows, LANES), lambda i: (i, 0, 0)))
        out_shape.append(jax.ShapeDtypeStruct((group, rows, LANES), bf16))
    following = min(layer + 1, norm_gain.shape[0] - 1)
    return pl.pallas_call(
        functools.partial(finish_kernel, send),
        grid=(steps,),
        in_specs=[
            block,
            full(normed),
            *[full(h) for h in halo],
            whole(3, D),
            pl.BlockSpec((1, 3, D), lambda i: (following, 0, 0)),
            whole(KS * KS, D),
            whole(D, HID),
            whole(HID, D),
        ],
        out_specs=out_specs,
        out_shape=out_shape,
        scratch_shapes=[
            pltpu.VMEM((height + 2 * HALO, width + 2 * WS, D), bf16),
            pltpu.VMEM((WS * width, D), f32),
            pltpu.VMEM((KS * KS, 16, D), bf16),
        ],
        name="finish_layer",
    )(after, normed, *halo, norm_gain, norm_gain, conv_weight, up_weight, down_weight)


def halo_of(normed):
    height, width = normed.shape[:2]

    def shift(value, axes, forward):
        count = lax.axis_size(axes)
        pairs = [(i, i + 1) if forward else (i + 1, i) for i in range(count - 1)]
        return lax.ppermute(value, axes, pairs)

    top = shift(normed[height - HALO :], "row", True)
    bottom = shift(normed[:HALO], "row", False)
    columns = lambda part: jnp.concatenate([part(top), part(normed), part(bottom)], axis=0)
    left = shift(columns(lambda a: a[:, width - WS :]), ("block", "core"), True)
    right = shift(columns(lambda a: a[:, :WS]), ("block", "core"), False)
    return top, bottom, left, right


def on_device(
    tokens, norm_gain, qkv_weight, proj_weight, bias_table, conv_weight, up_weight, down_weight
):
    members = ("row", "block")
    group = lax.axis_size(members)
    after, normed = plain_attention(tokens, norm_gain, qkv_weight, proj_weight, bias_table, 0)
    current, outgoing = finish_layer(
        after, normed, halo_of(normed), norm_gain, conv_weight, up_weight, down_weight, 0, True, group
    )
    got = lax.all_to_all(outgoing, members, 0, 0, tiled=True)
    branch = shuffled_attention(got, qkv_weight, proj_weight, bias_table, 1)
    back = lax.all_to_all(branch, members, 0, 0, tiled=True)
    after, normed = residual(back, current, norm_gain, 1)
    (outcome,) = finish_layer(
        after, normed, halo_of(normed), norm_gain, conv_weight, up_weight, down_weight, 1, False, group
    )
    return outcome


def solution(mesh):
    split = Mesh(
        mesh.devices.reshape(mesh.shape["row"], mesh.shape["col"] // 2, 2), ("row", "block", "core")
    )
    spec = P("row", ("block", "core"), None)
    return jax.shard_map(
        on_device, mesh=split, in_specs=(spec,) + (P(),) * 7, out_specs=spec, check_vma=False
    )
```

```python
import functools
import jax
import jax.numpy as jnp
from jax import lax
from jax.experimental import pallas as pl
from jax.experimental.pallas import tpu as pltpu
from jax.sharding import Mesh, PartitionSpec as P

D = 192
HEADS = 6
HID = 768
WS = 8
KS = 7
HEAD = 32
AREA = WS * WS
PAD = 256
LANES = 128
HALO = KS // 2
TOGETHER = 4
WINDOW_ROWS = AREA + 8
PIECE_ROWS = 24
RETURN_ROWS = 40
RING = 80
SEGMENT = 16
EPSILON = 1e-05

f32 = jnp.float32
bf16 = jnp.bfloat16


def layer_norm(values, gain):
    centre = jnp.mean(values, axis=-1, keepdims=True)
    centred = values - centre
    spread = jnp.mean(centred * centred, axis=-1, keepdims=True)
    return centred * lax.rsqrt(spread + EPSILON) * gain


def mxu(a, b):
    return jnp.dot(a, b, preferred_element_type=f32)


def prepare_attention(table_ref, qkv_ref, bias_s, rows_s, qkv_s):
    table = table_ref[0]
    high = table.astype(bf16)
    rest = table - high.astype(f32)
    middle = rest.astype(bf16)
    low = (rest - middle.astype(f32)).astype(bf16)
    entries = (2 * WS - 1) ** 2
    lane = lax.broadcasted_iota(jnp.int32, (entries, WS * LANES), 1)
    entry = lax.broadcasted_iota(jnp.int32, (entries, WS * LANES), 0)
    target = (
        (2 * WS - 2 - ((lane & (LANES - 1)) >> 3)) * (2 * WS - 1)
        + (lane >> 7)
        - (lane & 7)
        + WS
        - 1
    )
    chosen = jnp.where(entry == target, 1.0, 0.0).astype(bf16)
    spread = mxu(high, chosen) + mxu(middle, chosen) + mxu(low, chosen)
    for place in range(WS):
        rows_s[place, 0:HEADS, :] = spread[:, place * LANES : (place + 1) * LANES]
    first = lax.broadcasted_iota(jnp.int32, (WS, LANES), 1) < AREA
    for group in range(HEADS // 2):
        left = rows_s[:, 2 * group, :]
        right = rows_s[:, 2 * group + 1, :]
        for row in range(WS):
            shift = LANES - (WS - 1 - row) * WS
            piece = jnp.where(
                first,
                pltpu.roll(left, shift % LANES, 1),
                pltpu.roll(right, (shift + AREA) % LANES, 1),
            )
            bias_s[group * AREA + row * WS : group * AREA + (row + 1) * WS, :] = piece
    weights = qkv_ref[0].astype(f32)
    gap = jnp.zeros((D, PAD - D), f32)
    qkv_s[...] = jnp.concatenate(
        [
            weights[:, 0:D],
            gap,
            weights[:, D : 2 * D],
            gap,
            weights[:, 2 * D : 3 * D],
            gap,
        ],
        axis=1,
    ).astype(bf16)


def attention_masks():
    lane = lax.broadcasted_iota(jnp.int32, (1, PAD), 1)
    groups = [
        jnp.where((lane >> 6) == g, 1.0, 0.0).astype(bf16) for g in range(HEADS // 2)
    ]
    parities = [
        jnp.where(((lane >> 5) & 1) == h, 1.0, 0.0).astype(bf16) for h in range(2)
    ]
    rows = lax.broadcasted_iota(jnp.int32, (LANES, LANES), 0) >> 6
    cols = lax.broadcasted_iota(jnp.int32, (LANES, LANES), 1) >> 6
    summing = jnp.where(rows == cols, 1.0, 0.0).astype(bf16)
    return groups, parities, summing


def attend(projected, bias, masks):
    groups, parities, summing = masks
    count = projected.shape[0] // AREA
    window = lambda n, t: projected[n * AREA : (n + 1) * AREA, t * PAD : (t + 1) * PAD]
    spread = lambda x, ms: jnp.concatenate([x * m for m in ms], axis=0)
    scores = [
        lax.dot_general(
            spread(window(n, 0), groups),
            spread(window(n, 1), parities),
            (((1,), (1,)), ((), ())),
            preferred_element_type=f32,
        )
        for n in range(count)
    ]
    weights = [jnp.exp(x * HEAD ** (-0.5) + bias) for x in scores]
    totals = [mxu(x.astype(bf16), summing) for x in weights]
    weights = [(x / y).astype(bf16) for x, y in zip(weights, totals)]
    mixed = [mxu(x, spread(window(n, 2), parities)) for n, x in enumerate(weights)]
    lane = lax.broadcasted_iota(jnp.int32, (AREA, PAD), 1) >> 6
    return [
        jnp.where(
            lane == 0, x[0:AREA], jnp.where(lane == 1, x[AREA : 2 * AREA], x[2 * AREA :])
        )[:, 0:D].astype(bf16)
        for x in mixed
    ]


def attention(current, gain, qkv, proj, bias, masks, together):
    normed = layer_norm(current, gain).astype(bf16)
    projected = mxu(normed, qkv).astype(bf16)
    outs = []
    for start in range(0, current.shape[0], together * AREA):
        outs += attend(projected[start : start + together * AREA], bias, masks)
    return current + mxu(jnp.concatenate(outs, axis=0), proj)


def plain_kernel(
    x_ref, gain_ref, qkv_ref, proj_ref, table_ref, sum_ref, normed_ref, bias_s, rows_s, qkv_s
):
    @pl.when(pl.program_id(0) == 0)
    def _():
        prepare_attention(table_ref, qkv_ref, bias_s, rows_s, qkv_s)

    cols = x_ref.shape[1]
    count = cols // WS
    grid = x_ref[...].astype(f32)
    current = jnp.concatenate(
        [grid[:, j * WS : (j + 1) * WS, :].reshape(AREA, D) for j in range(count)], axis=0
    )
    after = attention(
        current,
        gain_ref[0, 0:1, :],
        qkv_s[...],
        proj_ref[0],
        bias_s[...],
        attention_masks(),
        TOGETHER,
    )
    normed_two = layer_norm(after, gain_ref[0, 1:2, :])

    def spatial(value):
        return jnp.concatenate(
            [value[j * AREA : (j + 1) * AREA].reshape(WS, WS, D) for j in range(count)], axis=1
        )

    sum_ref[...] = spatial(after)
    normed_ref[...] = spatial(normed_two).astype(bf16)


def attention_scratch():
    return [
        pltpu.VMEM((HEADS // 2 * AREA, LANES), f32),
        pltpu.VMEM((WS, WS, LANES), f32),
        pltpu.VMEM((D, 3 * PAD), bf16),
    ]


def plain_attention(tokens, norm_gain, qkv_weight, proj_weight, bias_table, layer):
    height, width = tokens.shape[:2]
    whole = lambda *shape: pl.BlockSpec(
        (1, *shape), lambda i: (layer,) + (0,) * len(shape)
    )
    block = pl.BlockSpec((WS, width, D), lambda i: (i, 0, 0))
    return pl.pallas_call(
        plain_kernel,
        grid=(height // WS,),
        in_specs=[
            block,
            whole(3, D),
            whole(D, 3 * D),
            whole(D, D),
            whole(HEADS, (2 * WS - 1) ** 2),
        ],
        out_specs=[block, block],
        out_shape=[
            jax.ShapeDtypeStruct(tokens.shape, f32),
            jax.ShapeDtypeStruct(tokens.shape, bf16),
        ],
        scratch_shapes=attention_scratch(),
        name="plain_attention",
    )(tokens, norm_gain, qkv_weight, proj_weight, bias_table)


def low_half(value):
    lane = lax.broadcasted_iota(jnp.int32, value.shape, value.ndim - 1)
    return jnp.where(lane < D - LANES, value, 0.0)


def join_halves(first, second):
    lane = lax.broadcasted_iota(jnp.int32, first.shape, 1)
    return jnp.where(lane < D - LANES, first, pltpu.roll(second, D - LANES, 1))


def shuffled_kernel(
    got_ref, gain_ref, qkv_ref, proj_ref, table_ref, out_ref, bias_s, rows_s, qkv_s, window_s, piece_s
):
    prepare_attention(table_ref, qkv_ref, bias_s, rows_s, qkv_s)
    blocks = WS * 2

    def gather(a, carry):
        for c in range(blocks):
            piece = got_ref[a * blocks + c].astype(f32)
            upper = piece[SEGMENT:]
            upper = jnp.concatenate(
                [low_half(upper), low_half(pltpu.roll(upper, D - LANES, 1))], axis=0
            )
            place = pl.ds(
                (c % 2) * SEGMENT * WINDOW_ROWS + a * WS + c // 2, SEGMENT, stride=WINDOW_ROWS
            )
            window_s[0, place, :] = piece[:SEGMENT]
            window_s[1, place, :] = upper
        return carry

    lax.fori_loop(0, WS, gather, 0)
    masks = attention_masks()

    def windows(c, carry):
        starts = [
            pl.multiple_of((c * TOGETHER + n) * WINDOW_ROWS, 8) for n in range(TOGETHER)
        ]
        current = jnp.concatenate(
            [
                jnp.concatenate(
                    [window_s[t, pl.ds(start, AREA), :] for start in starts], axis=0
                )
                for t in range(2)
            ],
            axis=1,
        )[:, 0:D]
        after = attention(
            current, gain_ref[0, 0:1, :], qkv_s[...], proj_ref[0], bias_s[...], masks, TOGETHER
        )
        for n, start in enumerate(starts):
            window_s[0, pl.ds(start, AREA), :] = after[n * AREA : (n + 1) * AREA, 0:LANES]
            window_s[1, pl.ds(start, AREA), 0 : D - LANES] = after[
                n * AREA : (n + 1) * AREA, LANES:D
            ]
        return carry

    lax.fori_loop(0, 2 * SEGMENT // TOGETHER, windows, 0)

    below = lax.axis_index("row") < WS // 2
    beside = lax.axis_index("block") < WS // 2
    row_step = jnp.where(below, 1, -1)
    row_window = jnp.where(below, 0, 3)
    col_window = jnp.where(beside, 0, 3)

    def scatter(a, carry):
        other_a = a + row_step
        row_keep = jnp.where((other_a >= 0) & (other_a < WS), 1.0, 0.0).astype(f32)
        other_a = jnp.clip(other_a, 0, WS - 1)
        for c in range(blocks):
            b, core = c // 2, c % 2
            other_b = b + (jnp.where(beside, 1, 0) if core else jnp.where(beside, 0, -1))
            col_keep = jnp.where((other_b >= 0) & (other_b < WS), 1.0, 0.0).astype(f32)
            other_b = jnp.clip(other_b, 0, WS - 1)
            base = core * SEGMENT
            other = (1 - core) * SEGMENT
            main = pl.ds(base * WINDOW_ROWS + a * WS + b, SEGMENT, stride=WINDOW_ROWS)
            row = pl.ds(
                (base + row_window * 4) * WINDOW_ROWS + other_a * WS + b, 4, stride=WINDOW_ROWS
            )
            col = pl.ds(
                (other + col_window) * WINDOW_ROWS + a * WS + other_b, 4, stride=4 * WINDOW_ROWS
            )
            corner = pl.ds(
                (other + row_window * 4 + col_window) * WINDOW_ROWS + other_a * WS + other_b, 1
            )
            keep = row_keep * col_keep
            piece_s[0:16] = window_s[0, main, :]
            piece_s[16:20] = window_s[0, row, :] * row_keep
            piece_s[20:24] = window_s[0, col, :] * col_keep
            upper = window_s[1, main, :]
            piece_s[24:32] = join_halves(upper[0:8], upper[8:16])
            piece_s[32:36] = join_halves(
                window_s[1, row, :] * row_keep, window_s[1, col, :] * col_keep
            )
            piece_s[36:37] = window_s[0, corner, :] * keep
            piece_s[37:38] = window_s[1, corner, :] * keep
            out_ref[a * blocks + c] = piece_s[...].astype(bf16)
        return carry

    piece_s[...] = jnp.zeros_like(piece_s)
    lax.fori_loop(0, WS, scatter, 0)


def shuffled_attention(got, norm_gain, qkv_weight, proj_weight, bias_table, layer):
    whole = lambda *shape: pl.BlockSpec(
        (1, *shape), lambda i: (layer,) + (0,) * len(shape)
    )
    shape = (got.shape[0], RETURN_ROWS, LANES)
    return pl.pallas_call(
        shuffled_kernel,
        grid=(1,),
        in_specs=[
            pl.BlockSpec(got.shape, lambda i: (0, 0, 0)),
            whole(3, D),
            whole(D, 3 * D),
            whole(D, D),
            whole(HEADS, (2 * WS - 1) ** 2),
        ],
        out_specs=pl.BlockSpec(shape, lambda i: (0, 0, 0)),
        out_shape=jax.ShapeDtypeStruct(shape, bf16),
        scratch_shapes=attention_scratch()
        + [
            pltpu.VMEM((2, 2 * SEGMENT * WINDOW_ROWS, LANES), f32),
            pltpu.VMEM((RETURN_ROWS, LANES), f32),
        ],
        name="shuffled_attention",
    )(got, norm_gain, qkv_weight, proj_weight, bias_table)


def broadcast_taps(taps_ref, taps_s):
    for t in range(KS * KS):
        taps_s[t] = jnp.broadcast_to(taps_ref[0, t : t + 1, :], (16, D)).astype(bf16)


def convolve_row(padded_s, taps_s, row, width):
    total = None
    for v in range(KS):
        part = None
        for u in range(KS):
            x = padded_s[row + u].reshape(-1, 16, D)
            term = x * taps_s[u * KS + v][None]
            part = term if part is None else part + term
        part = part.reshape(-1, D).astype(f32)
        shift = v - HALO
        if shift < 0:
            part = jnp.concatenate([part[RING + shift :], part[: width + shift]], axis=0)
        else:
            part = part[shift : shift + width]
        total = part if total is None else total + part
    return total


def feed_forward(after, gain, up, down):
    normed = layer_norm(after, gain).astype(bf16)
    raised = mxu(normed, up)
    hidden = (0.5 * raised * (1.0 + lax.erf(raised * 0.5**0.5))).astype(bf16)
    return (after + mxu(hidden, down)).astype(bf16)


def first_kernel(
    sum_ref,
    normed_ref,
    top_ref,
    bottom_ref,
    left_ref,
    right_ref,
    gain_ref,
    taps_ref,
    up_ref,
    down_ref,
    send_ref,
    padded_s,
    after_s,
    taps_s,
    piece_s,
):
    step = pl.program_id(0)
    height, width, _ = normed_ref.shape
    repeats, rows = sum_ref.shape[:2]

    @pl.when(step == 0)
    def _():
        def place(r, middle):
            padded_s[r] = jnp.concatenate(
                [middle.astype(f32), right_ref[r].astype(f32), left_ref[r].astype(f32)], axis=0
            ).astype(bf16)

        for r in range(HALO):
            place(r, top_ref[r])
            place(height + HALO + r, bottom_ref[r])

        def body(r, carry):
            place(r + HALO, normed_ref[r])
            return carry

        lax.fori_loop(0, height, body, 0)
        broadcast_taps(taps_ref, taps_s)

    def row(j, carry):
        m, q = j // rows, j % rows
        total = sum_ref[m, q] + convolve_row(
            padded_s, taps_s, m * WS + step * rows + q, width
        )
        after_s[pl.ds(pl.multiple_of(j * width, width), width), :] = total
        return carry

    lax.fori_loop(0, repeats * rows, row, 0)
    outcome = feed_forward(after_s[...], gain_ref[0, 2:3, :], up_ref[0], down_ref[0]).astype(f32)
    for m in range(repeats):
        for q in range(rows):
            for n in range(width // SEGMENT):
                start = (m * rows + q) * width + n * SEGMENT
                value = outcome[start : start + SEGMENT]
                place = pl.ds((q * SEGMENT + m * 4 + n) * PIECE_ROWS, SEGMENT)
                piece_s[0, place, :] = value[:, 0:LANES]
                piece_s[1, place, 0 : D - LANES] = value[:, LANES:D]
    for q in range(rows):
        for c in range(SEGMENT):
            place = pl.ds(q * SEGMENT * PIECE_ROWS + c, SEGMENT, stride=PIECE_ROWS)
            upper = piece_s[1, place, :]
            send_ref[q * SEGMENT + c] = jnp.concatenate(
                [piece_s[0, place, :], join_halves(upper[0:8], upper[8:16])], axis=0
            ).astype(bf16)


def first_finish(after, normed, halo, norm_gain, conv_weight, up_weight, down_weight, layer, group):
    height, width = normed.shape[:2]
    repeats = height // WS
    rows = WS // repeats
    whole = lambda *shape: pl.BlockSpec(
        (1, *shape), lambda i: (layer,) + (0,) * len(shape)
    )
    full = lambda a: pl.BlockSpec(a.shape, lambda i: (0,) * a.ndim)
    return pl.pallas_call(
        first_kernel,
        grid=(WS // rows,),
        in_specs=[
            pl.BlockSpec((repeats, rows, width, D), lambda i: (0, i, 0, 0)),
            full(normed),
            *[full(h) for h in halo],
            whole(3, D),
            whole(KS * KS, D),
            whole(D, HID),
            whole(HID, D),
        ],
        out_specs=pl.BlockSpec((rows * SEGMENT, PIECE_ROWS, LANES), lambda i: (i, 0, 0)),
        out_shape=jax.ShapeDtypeStruct((group, PIECE_ROWS, LANES), bf16),
        scratch_shapes=[
            pltpu.VMEM((height + 2 * HALO, RING, D), bf16),
            pltpu.VMEM((repeats * rows * width, D), f32),
            pltpu.VMEM((KS * KS, 16, D), bf16),
            pltpu.VMEM((2, rows * SEGMENT * PIECE_ROWS, LANES), f32),
        ],
        name="first_finish",
    )(
        after.reshape(repeats, WS, width, D),
        normed,
        *halo,
        norm_gain,
        conv_weight,
        up_weight,
        down_weight,
    )


def second_kernel(
    back_ref,
    gain_ref,
    taps_ref,
    up_ref,
    down_ref,
    out_ref,
    padded_s,
    sum_s,
    after_s,
    taps_s,
    piece_s,
):
    step = pl.program_id(0)
    rows, width, _ = out_ref.shape
    height = sum_s.shape[0]
    repeats = height // WS

    @pl.when(step == 0)
    def _():
        broadcast_taps(taps_ref, taps_s)

        def build(r, n, target, keep):
            pieces = []
            for m in range(width // SEGMENT + 1):
                if n < 4 and m < 4:
                    low, high, half = 4 * n + m, 24 + (4 * n + m) % 8, (4 * n + m) // 8
                elif m < 4:
                    low, high, half = 16 + m, 32 + m, 0
                elif n < 4:
                    low, high, half = 20 + n, 32 + n, 1
                else:
                    low, high, half = 36, 37, 0
                at = lambda k: piece_s[pl.ds(k, SEGMENT, stride=RETURN_ROWS), :]
                upper = at(high)
                if half:
                    upper = pltpu.roll(upper, D - LANES, 1)
                pieces.append(jnp.concatenate([at(low), upper], axis=1)[:, 0:D])
            value = jnp.concatenate(pieces, axis=0)
            if keep:
                sum_s[target - HALO] = value[0:width]
            padded_s[target] = layer_norm(value, gain_ref[0, 1:2, :]).astype(bf16)

        def body(r, carry):
            def load(c, carry):
                piece_s[pl.ds(pl.multiple_of(c * RETURN_ROWS, 8), RETURN_ROWS), :] = back_ref[
                    r * SEGMENT + c
                ].astype(f32)
                return carry

            lax.fori_loop(0, SEGMENT, load, 0, unroll=True)
            for n in range(repeats):
                build(r, n, HALO + r + WS * n, True)

            @pl.when(r < HALO)
            def _():
                build(r, repeats, HALO + height + r, False)

            @pl.when(r >= WS - HALO)
            def _():
                build(r, repeats, HALO + r - WS, False)

            return carry

        lax.fori_loop(0, WS, body, 0)

    def row(j, carry):
        r = step * rows + j
        total = sum_s[r] + convolve_row(padded_s, taps_s, r, width)
        after_s[pl.ds(pl.multiple_of(j * width, width), width), :] = total
        return carry

    lax.fori_loop(0, rows, row, 0)
    outcome = feed_forward(after_s[...], gain_ref[0, 2:3, :], up_ref[0], down_ref[0])
    out_ref[...] = outcome.reshape(rows, width, D)


def second_finish(back, shape, norm_gain, conv_weight, up_weight, down_weight, layer):
    height, width = shape[:2]
    whole = lambda *shape: pl.BlockSpec(
        (1, *shape), lambda i: (layer,) + (0,) * len(shape)
    )
    return pl.pallas_call(
        second_kernel,
        grid=(height // WS,),
        in_specs=[
            pl.BlockSpec(back.shape, lambda i: (0, 0, 0)),
            whole(3, D),
            whole(KS * KS, D),
            whole(D, HID),
            whole(HID, D),
        ],
        out_specs=pl.BlockSpec((WS, width, D), lambda i: (i, 0, 0)),
        out_shape=jax.ShapeDtypeStruct(shape, bf16),
        scratch_shapes=[
            pltpu.VMEM((height + 2 * HALO, RING, D), bf16),
            pltpu.VMEM((height, width, D), f32),
            pltpu.VMEM((WS * width, D), f32),
            pltpu.VMEM((KS * KS, 16, D), bf16),
            pltpu.VMEM((SEGMENT * RETURN_ROWS, LANES), f32),
        ],
        name="second_finish",
    )(back, norm_gain, conv_weight, up_weight, down_weight)


def halo_of(normed):
    height, width = normed.shape[:2]

    def shift(value, axes, forward):
        count = lax.axis_size(axes)
        pairs = [(i, i + 1) if forward else (i + 1, i) for i in range(count - 1)]
        return lax.ppermute(value, axes, pairs)

    top = shift(normed[height - HALO :], "row", True)
    bottom = shift(normed[:HALO], "row", False)
    columns = lambda part: jnp.concatenate([part(top), part(normed), part(bottom)], axis=0)
    left = shift(columns(lambda a: a[:, width - WS :]), ("block", "core"), True)
    right = shift(columns(lambda a: a[:, :WS]), ("block", "core"), False)
    return top, bottom, left, right


def on_device(
    tokens, norm_gain, qkv_weight, proj_weight, bias_table, conv_weight, up_weight, down_weight
):
    members = ("row", "block", "core")
    after, normed = plain_attention(tokens, norm_gain, qkv_weight, proj_weight, bias_table, 0)
    outgoing = first_finish(
        after,
        normed,
        halo_of(normed),
        norm_gain,
        conv_weight,
        up_weight,
        down_weight,
        0,
        lax.axis_size(members),
    )
    got = lax.all_to_all(outgoing, members, 0, 0, tiled=True)
    branch = shuffled_attention(got, norm_gain, qkv_weight, proj_weight, bias_table, 1)
    back = lax.all_to_all(branch, members, 0, 0, tiled=True)
    return second_finish(back, tokens.shape, norm_gain, conv_weight, up_weight, down_weight, 1)


def solution(mesh):
    split = Mesh(
        mesh.devices.reshape(mesh.shape["row"], mesh.shape["col"] // 2, 2), ("row", "block", "core")
    )
    spec = P("row", ("block", "core"), None)
    return jax.shard_map(
        on_device, mesh=split, in_specs=(spec,) + (P(),) * 7, out_specs=spec, check_vma=False
    )
```

```python
import functools
import jax
import jax.numpy as jnp
from jax import lax
from jax.experimental import pallas as pl
from jax.experimental.pallas import tpu as pltpu
from jax.sharding import Mesh, PartitionSpec as P

D = 192
HEADS = 6
HID = 768
WS = 8
KS = 7
HEAD = 32
AREA = WS * WS
PAD = 256
LANES = 128
HALO = KS // 2
TOGETHER = 4
WINDOW_ROWS = AREA + 8
PIECE_ROWS = 24
RETURN_ROWS = 40
RING = 80
SEGMENT = 16
EPSILON = 1e-05

f32 = jnp.float32
bf16 = jnp.bfloat16


def layer_norm(values, gain):
    centre = jnp.mean(values, axis=-1, keepdims=True)
    centred = values - centre
    spread = jnp.mean(centred * centred, axis=-1, keepdims=True)
    return centred * lax.rsqrt(spread + EPSILON) * gain


def mxu(a, b):
    return jnp.dot(a, b, preferred_element_type=f32)


def prepare_attention(layer, table_ref, qkv_ref, bias_s, rows_s, qkv_s):
    table = table_ref[:, layer, :]
    high = table.astype(bf16)
    rest = table - high.astype(f32)
    middle = rest.astype(bf16)
    low = (rest - middle.astype(f32)).astype(bf16)
    entries = (2 * WS - 1) ** 2
    lane = lax.broadcasted_iota(jnp.int32, (entries, WS * LANES), 1)
    entry = lax.broadcasted_iota(jnp.int32, (entries, WS * LANES), 0)
    target = (
        (2 * WS - 2 - ((lane & (LANES - 1)) >> 3)) * (2 * WS - 1)
        + (lane >> 7)
        - (lane & 7)
        + WS
        - 1
    )
    chosen = jnp.where(entry == target, 1.0, 0.0).astype(bf16)
    spread = mxu(high, chosen) + mxu(middle, chosen) + mxu(low, chosen)
    for place in range(WS):
        rows_s[place, 0:HEADS, :] = spread[:, place * LANES : (place + 1) * LANES]
    first = lax.broadcasted_iota(jnp.int32, (WS, LANES), 1) < AREA
    for group in range(HEADS // 2):
        left = rows_s[:, 2 * group, :]
        right = rows_s[:, 2 * group + 1, :]
        for row in range(WS):
            shift = LANES - (WS - 1 - row) * WS
            piece = jnp.where(
                first,
                pltpu.roll(left, shift % LANES, 1),
                pltpu.roll(right, (shift + AREA) % LANES, 1),
            )
            bias_s[group * AREA + row * WS : group * AREA + (row + 1) * WS, :] = piece
    weights = qkv_ref[layer].astype(f32)
    gap = jnp.zeros((D, PAD - D), f32)
    qkv_s[...] = jnp.concatenate(
        [
            weights[:, 0:D],
            gap,
            weights[:, D : 2 * D],
            gap,
            weights[:, 2 * D : 3 * D],
            gap,
        ],
        axis=1,
    ).astype(bf16)


def attention_masks():
    lane = lax.broadcasted_iota(jnp.int32, (1, PAD), 1)
    groups = [
        jnp.where((lane >> 6) == g, 1.0, 0.0).astype(bf16) for g in range(HEADS // 2)
    ]
    parities = [
        jnp.where(((lane >> 5) & 1) == h, 1.0, 0.0).astype(bf16) for h in range(2)
    ]
    rows = lax.broadcasted_iota(jnp.int32, (LANES, LANES), 0) >> 6
    cols = lax.broadcasted_iota(jnp.int32, (LANES, LANES), 1) >> 6
    summing = jnp.where(rows == cols, 1.0, 0.0).astype(bf16)
    return groups, parities, summing


def attend(projected, bias, masks):
    groups, parities, summing = masks
    count = projected.shape[0] // AREA
    window = lambda n, t: projected[n * AREA : (n + 1) * AREA, t * PAD : (t + 1) * PAD]
    spread = lambda x, ms: jnp.concatenate([x * m for m in ms], axis=0)
    scores = [
        lax.dot_general(
            spread(window(n, 0), groups),
            spread(window(n, 1), parities),
            (((1,), (1,)), ((), ())),
            preferred_element_type=f32,
        )
        for n in range(count)
    ]
    weights = [jnp.exp(x * HEAD ** (-0.5) + bias) for x in scores]
    totals = [mxu(x.astype(bf16), summing) for x in weights]
    weights = [(x / y).astype(bf16) for x, y in zip(weights, totals)]
    mixed = [mxu(x, spread(window(n, 2), parities)) for n, x in enumerate(weights)]
    lane = lax.broadcasted_iota(jnp.int32, (AREA, PAD), 1) >> 6
    return [
        jnp.where(
            lane == 0, x[0:AREA], jnp.where(lane == 1, x[AREA : 2 * AREA], x[2 * AREA :])
        )[:, 0:D].astype(bf16)
        for x in mixed
    ]


def attention(current, gain, qkv, proj, bias, masks, together):
    normed = layer_norm(current, gain).astype(bf16)
    projected = mxu(normed, qkv).astype(bf16)
    outs = []
    for start in range(0, current.shape[0], together * AREA):
        outs += attend(projected[start : start + together * AREA], bias, masks)
    return current + mxu(jnp.concatenate(outs, axis=0), proj)


def edge_kernel(
    first_ref,
    last_ref,
    gain_ref,
    qkv_ref,
    proj_ref,
    table_ref,
    sum_left_ref,
    sum_right_ref,
    left_out_ref,
    right_out_ref,
    bias_ref,
    pad_ref,
    rows_s,
):
    prepare_attention(0, table_ref, qkv_ref, bias_ref, rows_s, pad_ref)
    sides = [side[...].astype(f32).reshape(-1, D) for side in (first_ref, last_ref)]
    after = attention(
        jnp.concatenate(sides, axis=0),
        gain_ref[0, 0:1, :],
        pad_ref[...],
        proj_ref[0],
        bias_ref[...],
        attention_masks(),
        TOGETHER,
    )
    normed = layer_norm(after, gain_ref[1, 0:1, :])
    half = after.shape[0] // 2
    shape = sum_left_ref.shape
    sum_left_ref[...] = after[:half].reshape(shape)
    sum_right_ref[...] = after[half:].reshape(shape)
    left_out_ref[...] = normed[:half].reshape(shape).astype(bf16)
    right_out_ref[...] = normed[half:].reshape(shape).astype(bf16)


def inner_kernel(
    x_ref,
    gain_ref,
    pad_ref,
    proj_ref,
    bias_ref,
    sum_left_ref,
    sum_right_ref,
    left_ref,
    right_ref,
    sum_ref,
    normed_ref,
):
    rows = pl.ds(pl.program_id(0) * WS, WS)
    inner = range(1, x_ref.shape[1] // WS - 1)
    grid = x_ref[rows].astype(f32)
    current = jnp.concatenate(
        [grid[:, j * WS : (j + 1) * WS, :].reshape(AREA, D) for j in inner], axis=0
    )
    after = attention(
        current,
        gain_ref[0, 0:1, :],
        pad_ref[...],
        proj_ref[0],
        bias_ref[...],
        attention_masks(),
        len(inner) // 2,
    )
    normed = layer_norm(after, gain_ref[1, 0:1, :])

    def spatial(first, value, last):
        pieces = [value[n * AREA : (n + 1) * AREA].reshape(WS, WS, D) for n in range(len(inner))]
        return jnp.concatenate([first, *pieces, last], axis=1)

    sum_ref[rows] = spatial(sum_left_ref[rows], after, sum_right_ref[rows])
    normed_ref[rows] = spatial(
        left_ref[rows].astype(f32), normed, right_ref[rows].astype(f32)
    ).astype(bf16)


def attention_scratch():
    return [
        pltpu.VMEM((HEADS // 2 * AREA, LANES), f32),
        pltpu.VMEM((WS, WS, LANES), f32),
        pltpu.VMEM((D, 3 * PAD), bf16),
    ]


RESIDENT = pl.BlockSpec(memory_space=pltpu.VMEM)
PARAMS = pltpu.CompilerParams(vmem_limit_bytes=24 << 20)


def resident(*arrays):
    return [pltpu.with_memory_space_constraint(a, pltpu.VMEM) for a in arrays]


def work(flops):
    return pl.CostEstimate(flops=int(flops), transcendentals=0, bytes_accessed=1 << 20)


def edge_attention(tokens, gains, qkv_weight, proj_weight, table):
    side = (tokens.shape[0], WS, D)
    last = tokens.shape[1] // WS - 1
    full = lambda a: pl.BlockSpec(a.shape, lambda i: (0,) * a.ndim)
    return pl.pallas_call(
        edge_kernel,
        grid=(1,),
        in_specs=[
            pl.BlockSpec(side, lambda i: (0, 0, 0)),
            pl.BlockSpec(side, lambda i: (0, last, 0)),
            full(gains),
            full(qkv_weight),
            full(proj_weight),
            full(table),
        ],
        out_specs=[RESIDENT] * 6,
        out_shape=[
            pltpu.VMEM(side, f32),
            pltpu.VMEM(side, f32),
            pltpu.VMEM(side, bf16),
            pltpu.VMEM(side, bf16),
            pltpu.VMEM((HEADS // 2 * AREA, LANES), f32),
            pltpu.VMEM((D, 3 * PAD), bf16),
        ],
        scratch_shapes=[pltpu.VMEM((WS, WS, LANES), f32)],
        compiler_params=PARAMS,
        cost_estimate=work(5e8),
        name="edge_attention",
    )(tokens, tokens, gains, qkv_weight, proj_weight, table)


def inner_attention(tokens, gains, padded, proj_weight, bias, edges):
    return pl.pallas_call(
        inner_kernel,
        grid=(tokens.shape[0] // WS,),
        in_specs=[RESIDENT] * 9,
        out_specs=[RESIDENT] * 2,
        out_shape=[pltpu.VMEM(tokens.shape, f32), pltpu.VMEM(tokens.shape, bf16)],
        compiler_params=PARAMS,
        cost_estimate=work(8e9),
        name="inner_attention",
    )(*resident(tokens, gains, padded, proj_weight, bias, *edges))


def low_half(value):
    lane = lax.broadcasted_iota(jnp.int32, value.shape, value.ndim - 1)
    return jnp.where(lane < D - LANES, value, 0.0)


def join_halves(first, second):
    lane = lax.broadcasted_iota(jnp.int32, first.shape, 1)
    return jnp.where(lane < D - LANES, first, pltpu.roll(second, D - LANES, 1))


def shuffled_kernel(
    got_ref, gain_ref, qkv_ref, proj_ref, table_ref, out_ref, bias_s, rows_s, qkv_s, window_s, piece_s
):
    prepare_attention(1, table_ref, qkv_ref, bias_s, rows_s, qkv_s)
    blocks = WS * 2

    def gather(a, carry):
        for c in range(blocks):
            piece = got_ref[a * blocks + c].astype(f32)
            upper = piece[SEGMENT:]
            upper = jnp.concatenate(
                [low_half(upper), low_half(pltpu.roll(upper, D - LANES, 1))], axis=0
            )
            place = pl.ds(
                (c % 2) * SEGMENT * WINDOW_ROWS + a * WS + c // 2, SEGMENT, stride=WINDOW_ROWS
            )
            window_s[0, place, :] = piece[:SEGMENT]
            window_s[1, place, :] = upper
        return carry

    lax.fori_loop(0, WS, gather, 0)
    masks = attention_masks()

    def windows(c, carry):
        starts = [
            pl.multiple_of((c * TOGETHER + n) * WINDOW_ROWS, 8) for n in range(TOGETHER)
        ]
        current = jnp.concatenate(
            [
                jnp.concatenate(
                    [window_s[t, pl.ds(start, AREA), :] for start in starts], axis=0
                )
                for t in range(2)
            ],
            axis=1,
        )[:, 0:D]
        after = attention(
            current, gain_ref[0, 1:2, :], qkv_s[...], proj_ref[1], bias_s[...], masks, TOGETHER
        )
        for n, start in enumerate(starts):
            window_s[0, pl.ds(start, AREA), :] = after[n * AREA : (n + 1) * AREA, 0:LANES]
            window_s[1, pl.ds(start, AREA), 0 : D - LANES] = after[
                n * AREA : (n + 1) * AREA, LANES:D
            ]
        return carry

    lax.fori_loop(0, 2 * SEGMENT // TOGETHER, windows, 0)

    below = lax.axis_index("row") < WS // 2
    beside = lax.axis_index("block") < WS // 2
    row_step = jnp.where(below, 1, -1)
    row_window = jnp.where(below, 0, 3)
    col_window = jnp.where(beside, 0, 3)

    def scatter(a, carry):
        other_a = a + row_step
        row_keep = jnp.where((other_a >= 0) & (other_a < WS), 1.0, 0.0).astype(f32)
        other_a = jnp.clip(other_a, 0, WS - 1)
        for c in range(blocks):
            b, core = c // 2, c % 2
            other_b = b + (jnp.where(beside, 1, 0) if core else jnp.where(beside, 0, -1))
            col_keep = jnp.where((other_b >= 0) & (other_b < WS), 1.0, 0.0).astype(f32)
            other_b = jnp.clip(other_b, 0, WS - 1)
            base = core * SEGMENT
            other = (1 - core) * SEGMENT
            main = pl.ds(base * WINDOW_ROWS + a * WS + b, SEGMENT, stride=WINDOW_ROWS)
            row = pl.ds(
                (base + row_window * 4) * WINDOW_ROWS + other_a * WS + b, 4, stride=WINDOW_ROWS
            )
            col = pl.ds(
                (other + col_window) * WINDOW_ROWS + a * WS + other_b, 4, stride=4 * WINDOW_ROWS
            )
            corner = pl.ds(
                (other + row_window * 4 + col_window) * WINDOW_ROWS + other_a * WS + other_b, 1
            )
            keep = row_keep * col_keep
            piece_s[0:16] = window_s[0, main, :]
            piece_s[16:20] = window_s[0, row, :] * row_keep
            piece_s[20:24] = window_s[0, col, :] * col_keep
            upper = window_s[1, main, :]
            piece_s[24:32] = join_halves(upper[0:8], upper[8:16])
            piece_s[32:36] = join_halves(
                window_s[1, row, :] * row_keep, window_s[1, col, :] * col_keep
            )
            piece_s[36:37] = window_s[0, corner, :] * keep
            piece_s[37:38] = window_s[1, corner, :] * keep
            out_ref[a * blocks + c] = piece_s[...].astype(bf16)
        return carry

    piece_s[...] = jnp.zeros_like(piece_s)
    lax.fori_loop(0, WS, scatter, 0)


def shuffled_attention(got, gains, qkv_weight, proj_weight, table):
    shape = (got.shape[0], RETURN_ROWS, LANES)
    return pl.pallas_call(
        shuffled_kernel,
        in_specs=[RESIDENT] * 5,
        out_specs=RESIDENT,
        out_shape=pltpu.VMEM(shape, bf16),
        scratch_shapes=attention_scratch()
        + [
            pltpu.VMEM((2, 2 * SEGMENT * WINDOW_ROWS, LANES), f32),
            pltpu.VMEM((RETURN_ROWS, LANES), f32),
        ],
        compiler_params=PARAMS,
        cost_estimate=work(1e10),
        name="shuffled_attention",
    )(*resident(got, gains, qkv_weight, proj_weight, table))


def prepare_finish(layer, taps_ref, down_ref, taps_s, down_s):
    for t in range(KS * KS):
        taps_s[t] = jnp.broadcast_to(
            taps_ref[t, layer : layer + 1, :], (16, D)
        ).astype(bf16)
    down_s[...] = down_ref[layer].T


def convolve_row(padded_s, taps_s, row, width):
    total = None
    for v in range(KS):
        part = None
        for u in range(KS):
            x = padded_s[row + u].reshape(-1, 16, D)
            term = x * taps_s[u * KS + v][None]
            part = term if part is None else part + term
        part = part.reshape(-1, D).astype(f32)
        shift = v - HALO
        if shift < 0:
            part = jnp.concatenate([part[RING + shift :], part[: width + shift]], axis=0)
        else:
            part = part[shift : shift + width]
        total = part if total is None else total + part
    return total


def feed_forward(after, gain, up, down):
    normed = layer_norm(after, gain).astype(bf16)
    raised = mxu(normed, up)
    hidden = (0.5 * raised * (1.0 + lax.erf(raised * 0.5**0.5))).astype(bf16)
    return (after + mxu(hidden, down)).astype(bf16)


def ring(middle, right, left):
    return jnp.concatenate(
        [middle.astype(f32), right.astype(f32), left.astype(f32)], axis=0
    ).astype(bf16)


def middle_kernel(
    sum_ref,
    normed_ref,
    left_ref,
    right_ref,
    gain_ref,
    taps_ref,
    up_ref,
    down_ref,
    out_ref,
    padded_s,
    after_s,
    taps_s,
    down_s,
):
    step = pl.program_id(0)
    rows = WS
    width = sum_ref.shape[1]
    first = WS - HALO

    @pl.when(step == 0)
    def _():
        def body(r, carry):
            padded_s[r] = ring(normed_ref[first + r], right_ref[first + r], left_ref[first + r])
            return carry

        lax.fori_loop(0, padded_s.shape[0], body, 0)
        prepare_finish(0, taps_ref, down_ref, taps_s, down_s)

    def row(j, carry):
        total = sum_ref[WS + step * rows + j] + convolve_row(
            padded_s, taps_s, step * rows + j, width
        )
        after_s[pl.ds(pl.multiple_of(j * width, width), width), :] = total
        return carry

    lax.fori_loop(0, rows, row, 0)
    outcome = feed_forward(after_s[...], gain_ref[2, 0:1, :], up_ref[0], down_s[...])
    out_ref[pl.ds(step * rows, rows)] = outcome.reshape(rows, width, D)


def middle_finish(after, normed, left, right, gains, taps, up_weight, down_weight):
    height, width = normed.shape[:2]
    inner = height - 2 * WS
    return pl.pallas_call(
        middle_kernel,
        grid=(inner // WS,),
        in_specs=[RESIDENT] * 8,
        out_specs=RESIDENT,
        out_shape=pltpu.VMEM((inner, width, D), bf16),
        scratch_shapes=[
            pltpu.VMEM((inner + 2 * HALO, RING, D), bf16),
            pltpu.VMEM((WS * width, D), f32),
            pltpu.VMEM((KS * KS, 16, D), bf16),
            pltpu.VMEM((HID, D), bf16),
        ],
        compiler_params=PARAMS,
        cost_estimate=work(8e9),
        name="middle_finish",
    )(*resident(after, normed, left, right, gains, taps, up_weight, down_weight))


def outer_kernel(
    sum_ref,
    middle_ref,
    normed_ref,
    top_ref,
    bottom_ref,
    left_ref,
    right_ref,
    gain_ref,
    taps_ref,
    up_ref,
    down_ref,
    send_ref,
    padded_s,
    after_s,
    taps_s,
    down_s,
    piece_s,
):
    step = pl.program_id(0)
    height, width, _ = normed_ref.shape
    rows = WS // 2
    repeats = height // WS

    @pl.when(step == 0)
    def _():
        for r in range(HALO):
            padded_s[r] = top_ref[r]
            padded_s[height + HALO + r] = bottom_ref[r]

        def body(r, carry):
            padded_s[r + HALO] = ring(normed_ref[r], right_ref[r], left_ref[r])
            return carry

        lax.fori_loop(0, WS + HALO, body, 0)
        lax.fori_loop(height - WS - HALO, height, body, 0)
        prepare_finish(0, taps_ref, down_ref, taps_s, down_s)

    def row(j, carry):
        part, q = j // rows, j % rows
        r = part * (height - WS) + step * rows + q
        total = sum_ref[r] + convolve_row(padded_s, taps_s, r, width)
        after_s[pl.ds(pl.multiple_of(j * width, width), width), :] = total
        return carry

    lax.fori_loop(0, 2 * rows, row, 0)
    outcome = feed_forward(after_s[...], gain_ref[2, 0:1, :], up_ref[0], down_s[...]).astype(f32)
    for m in range(repeats):
        for q in range(rows):
            if m in (0, repeats - 1):
                start = ((m > 0) * rows + q) * width
                line = outcome[start : start + width]
            else:
                line = middle_ref[(m - 1) * WS + step * rows + q].astype(f32)
            for n in range(width // SEGMENT):
                value = line[n * SEGMENT : (n + 1) * SEGMENT]
                place = pl.ds((q * SEGMENT + m * 4 + n) * PIECE_ROWS, SEGMENT)
                piece_s[0, place, :] = value[:, 0:LANES]
                piece_s[1, place, 0 : D - LANES] = value[:, LANES:D]
    for q in range(rows):
        for c in range(SEGMENT):
            place = pl.ds(q * SEGMENT * PIECE_ROWS + c, SEGMENT, stride=PIECE_ROWS)
            upper = piece_s[1, place, :]
            send_ref[(step * rows + q) * SEGMENT + c] = jnp.concatenate(
                [piece_s[0, place, :], join_halves(upper[0:8], upper[8:16])], axis=0
            ).astype(bf16)


def outer_finish(
    after, middle, normed, top, bottom, left, right, gains, taps, up_weight, down_weight, group
):
    height, width = normed.shape[:2]
    rows = WS // 2
    return pl.pallas_call(
        outer_kernel,
        grid=(WS // rows,),
        in_specs=[RESIDENT] * 11,
        out_specs=RESIDENT,
        out_shape=pltpu.VMEM((group, PIECE_ROWS, LANES), bf16),
        scratch_shapes=[
            pltpu.VMEM((height + 2 * HALO, RING, D), bf16),
            pltpu.VMEM((2 * rows * width, D), f32),
            pltpu.VMEM((KS * KS, 16, D), bf16),
            pltpu.VMEM((HID, D), bf16),
            pltpu.VMEM((2, rows * SEGMENT * PIECE_ROWS, LANES), f32),
        ],
        compiler_params=PARAMS,
        cost_estimate=work(8e9),
        name="outer_finish",
    )(
        *resident(
            after,
            middle,
            normed,
            top,
            bottom,
            left,
            right,
            gains,
            taps,
            up_weight,
            down_weight,
        )
    )


def second_kernel(
    back_ref,
    gain_ref,
    taps_ref,
    up_ref,
    down_ref,
    out_ref,
    padded_s,
    sum_s,
    after_s,
    taps_s,
    down_s,
    piece_s,
):
    step = pl.program_id(0)
    rows, width, _ = out_ref.shape
    height = sum_s.shape[0]
    repeats = height // WS

    @pl.when(step == 0)
    def _():
        prepare_finish(1, taps_ref, down_ref, taps_s, down_s)

        def build(r, n, target, keep):
            pieces = []
            for m in range(width // SEGMENT + 1):
                if n < 4 and m < 4:
                    low, high, half = 4 * n + m, 24 + (4 * n + m) % 8, (4 * n + m) // 8
                elif m < 4:
                    low, high, half = 16 + m, 32 + m, 0
                elif n < 4:
                    low, high, half = 20 + n, 32 + n, 1
                else:
                    low, high, half = 36, 37, 0
                at = lambda k: piece_s[pl.ds(k, SEGMENT, stride=RETURN_ROWS), :]
                upper = at(high)
                if half:
                    upper = pltpu.roll(upper, D - LANES, 1)
                pieces.append(jnp.concatenate([at(low), upper], axis=1)[:, 0:D])
            value = jnp.concatenate(pieces, axis=0)
            if keep:
                sum_s[target - HALO] = value[0:width]
            padded_s[target] = layer_norm(value, gain_ref[1, 1:2, :]).astype(bf16)

        def body(r, carry):
            def load(c, carry):
                piece_s[pl.ds(pl.multiple_of(c * RETURN_ROWS, 8), RETURN_ROWS), :] = back_ref[
                    r * SEGMENT + c
                ].astype(f32)
                return carry

            lax.fori_loop(0, SEGMENT, load, 0, unroll=True)
            for n in range(repeats):
                build(r, n, HALO + r + WS * n, True)

            @pl.when(r < HALO)
            def _():
                build(r, repeats, HALO + height + r, False)

            @pl.when(r >= WS - HALO)
            def _():
                build(r, repeats, HALO + r - WS, False)

            return carry

        lax.fori_loop(0, WS, body, 0)

    def row(j, carry):
        r = step * rows + j
        total = sum_s[r] + convolve_row(padded_s, taps_s, r, width)
        after_s[pl.ds(pl.multiple_of(j * width, width), width), :] = total
        return carry

    lax.fori_loop(0, rows, row, 0)
    outcome = feed_forward(after_s[...], gain_ref[2, 1:2, :], up_ref[1], down_s[...])
    out_ref[...] = outcome.reshape(rows, width, D)


def second_finish(back, shape, gains, taps, up_weight, down_weight):
    height, width = shape[:2]
    return pl.pallas_call(
        second_kernel,
        grid=(height // WS,),
        in_specs=[RESIDENT] * 5,
        out_specs=pl.BlockSpec((WS, width, D), lambda i: (i, 0, 0)),
        out_shape=jax.ShapeDtypeStruct(shape, bf16),
        scratch_shapes=[
            pltpu.VMEM((height + 2 * HALO, RING, D), bf16),
            pltpu.VMEM((height, width, D), f32),
            pltpu.VMEM((WS * width, D), f32),
            pltpu.VMEM((KS * KS, 16, D), bf16),
            pltpu.VMEM((HID, D), bf16),
            pltpu.VMEM((SEGMENT * RETURN_ROWS, LANES), f32),
        ],
        compiler_params=PARAMS,
        cost_estimate=work(1e10),
        name="second_finish",
    )(*resident(back, gains, taps, up_weight, down_weight))


def shift(value, axes, forward):
    count = lax.axis_size(axes)
    pairs = [(i, i + 1) if forward else (i + 1, i) for i in range(count - 1)]
    return lax.ppermute(value, axes, pairs)


def on_device(
    tokens, norm_gain, qkv_weight, proj_weight, bias_table, conv_weight, up_weight, down_weight
):
    members = ("row", "block", "core")
    columns = ("block", "core")
    gains = norm_gain.transpose(1, 0, 2)
    table = bias_table.transpose(1, 0, 2)
    taps = conv_weight.transpose(1, 0, 2)
    down_weight = down_weight.transpose(0, 2, 1)
    *edges, bias, padded = edge_attention(tokens, gains, qkv_weight, proj_weight, table)
    left = shift(edges[3], columns, True)
    right = shift(edges[2], columns, False)
    after, normed = inner_attention(tokens, gains, padded, proj_weight, bias, edges)
    around = lambda rows: jnp.concatenate([normed[rows], right[rows], left[rows]], axis=1)
    height = tokens.shape[0]
    top = shift(around(slice(height - HALO, height)), "row", True)
    bottom = shift(around(slice(0, HALO)), "row", False)
    middle = middle_finish(after, normed, left, right, gains, taps, up_weight, down_weight)
    outgoing = outer_finish(
        after,
        middle,
        normed,
        top,
        bottom,
        left,
        right,
        gains,
        taps,
        up_weight,
        down_weight,
        lax.axis_size(members),
    )
    got = lax.all_to_all(outgoing, members, 0, 0, tiled=True)
    branch = shuffled_attention(got, gains, qkv_weight, proj_weight, table)
    back = lax.all_to_all(branch, members, 0, 0, tiled=True)
    return second_finish(back, tokens.shape, gains, taps, up_weight, down_weight)


def solution(mesh):
    split = Mesh(
        mesh.devices.reshape(mesh.shape["row"], mesh.shape["col"] // 2, 2), ("row", "block", "core")
    )
    spec = P("row", ("block", "core"), None)
    return jax.shard_map(
        on_device, mesh=split, in_specs=(spec,) + (P(),) * 7, out_specs=spec, check_vma=False
    )
```

```python
import functools
import jax
import jax.numpy as jnp
from jax import lax
from jax.experimental import pallas as pl
from jax.experimental.pallas import tpu as pltpu
from jax.sharding import Mesh, PartitionSpec as P

D = 192
HEADS = 6
HID = 768
WS = 8
KS = 7
HEAD = 32
AREA = WS * WS
PAD = 256
LANES = 128
HALO = KS // 2
TOGETHER = 16
WINDOW_ROWS = AREA + 4
PIECE_ROWS = 24
PIECE_STRIDE = PIECE_ROWS + 4
RETURN_ROWS = 40
RETURN_STRIDE = RETURN_ROWS + 4
RING = 80
SEGMENT = 16
EPSILON = 1e-05

f32 = jnp.float32
bf16 = jnp.bfloat16


def layer_norm(values, gain):
    centre = jnp.mean(values, axis=-1, keepdims=True)
    centred = values - centre
    spread = jnp.mean(centred * centred, axis=-1, keepdims=True)
    return centred * lax.rsqrt(spread + EPSILON) * gain


def mxu(a, b):
    return jnp.dot(a, b, preferred_element_type=f32)


def prepare_attention(layer, table_ref, qkv_ref, bias_s, rows_s, qkv_s):
    table = table_ref[:, layer, :]
    high = table.astype(bf16)
    rest = table - high.astype(f32)
    middle = rest.astype(bf16)
    low = (rest - middle.astype(f32)).astype(bf16)
    entries = (2 * WS - 1) ** 2
    lane = lax.broadcasted_iota(jnp.int32, (entries, WS * LANES), 1)
    entry = lax.broadcasted_iota(jnp.int32, (entries, WS * LANES), 0)
    target = (
        (2 * WS - 2 - ((lane & (LANES - 1)) >> 3)) * (2 * WS - 1)
        + (lane >> 7)
        - (lane & 7)
        + WS
        - 1
    )
    chosen = jnp.where(entry == target, 1.0, 0.0).astype(bf16)
    spread = mxu(high, chosen) + mxu(middle, chosen) + mxu(low, chosen)
    for place in range(WS):
        rows_s[place, 0:HEADS, :] = spread[:, place * LANES : (place + 1) * LANES]
    first = lax.broadcasted_iota(jnp.int32, (WS, LANES), 1) < AREA
    for group in range(HEADS // 2):
        left = rows_s[:, 2 * group, :]
        right = rows_s[:, 2 * group + 1, :]
        for row in range(WS):
            shift = LANES - (WS - 1 - row) * WS
            piece = jnp.where(
                first,
                pltpu.roll(left, shift % LANES, 1),
                pltpu.roll(right, (shift + AREA) % LANES, 1),
            )
            bias_s[group * AREA + row * WS : group * AREA + (row + 1) * WS, :] = piece
    weights = qkv_ref[layer].astype(f32)
    gap = jnp.zeros((D, PAD - D), f32)
    qkv_s[...] = jnp.concatenate(
        [
            weights[:, 0:D],
            gap,
            weights[:, D : 2 * D],
            gap,
            weights[:, 2 * D : 3 * D],
            gap,
        ],
        axis=1,
    ).astype(bf16)


def attention_masks():
    lane = lax.broadcasted_iota(jnp.int32, (1, PAD), 1)
    groups = [
        jnp.where((lane >> 6) == g, 1.0, 0.0).astype(bf16) for g in range(HEADS // 2)
    ]
    parities = [
        jnp.where(((lane >> 5) & 1) == h, 1.0, 0.0).astype(bf16) for h in range(2)
    ]
    rows = lax.broadcasted_iota(jnp.int32, (LANES, LANES), 0) >> 6
    cols = lax.broadcasted_iota(jnp.int32, (LANES, LANES), 1) >> 6
    summing = jnp.where(rows == cols, 1.0, 0.0).astype(bf16)
    return groups, parities, summing


def attend(projected, bias, masks):
    groups, parities, summing = masks
    count = projected.shape[0] // AREA
    window = lambda n, t: projected[n * AREA : (n + 1) * AREA, t * PAD : (t + 1) * PAD]
    spread = lambda x, ms: jnp.concatenate([x * m for m in ms], axis=0)
    scores = [
        lax.dot_general(
            spread(window(n, 0), groups),
            spread(window(n, 1), parities),
            (((1,), (1,)), ((), ())),
            preferred_element_type=f32,
        )
        for n in range(count)
    ]
    weights = [jnp.exp(x * HEAD ** (-0.5) + bias) for x in scores]
    totals = [mxu(x.astype(bf16), summing) for x in weights]
    weights = [(x / y).astype(bf16) for x, y in zip(weights, totals)]
    mixed = [mxu(x, spread(window(n, 2), parities)) for n, x in enumerate(weights)]
    lane = lax.broadcasted_iota(jnp.int32, (AREA, PAD), 1) >> 6
    return [
        jnp.where(
            lane == 0, x[0:AREA], jnp.where(lane == 1, x[AREA : 2 * AREA], x[2 * AREA :])
        )[:, 0:D].astype(bf16)
        for x in mixed
    ]


def attention(current, gain, qkv, proj, bias, masks, together):
    normed = layer_norm(current, gain).astype(bf16)
    projected = mxu(normed, qkv).astype(bf16)
    outs = []
    for start in range(0, current.shape[0], together * AREA):
        outs += attend(projected[start : start + together * AREA], bias, masks)
    return current + mxu(jnp.concatenate(outs, axis=0), proj)


def edge_kernel(
    first_ref,
    last_ref,
    gain_ref,
    qkv_ref,
    proj_ref,
    table_ref,
    sum_left_ref,
    sum_right_ref,
    left_out_ref,
    right_out_ref,
    bias_ref,
    pad_ref,
    rows_s,
):
    prepare_attention(0, table_ref, qkv_ref, bias_ref, rows_s, pad_ref)
    sides = [side[...].astype(f32).reshape(-1, D) for side in (first_ref, last_ref)]
    after = attention(
        jnp.concatenate(sides, axis=0),
        gain_ref[0, 0:1, :],
        pad_ref[...],
        proj_ref[0],
        bias_ref[...],
        attention_masks(),
        TOGETHER,
    )
    normed = layer_norm(after, gain_ref[1, 0:1, :])
    half = after.shape[0] // 2
    shape = sum_left_ref.shape
    sum_left_ref[...] = after[:half].reshape(shape)
    sum_right_ref[...] = after[half:].reshape(shape)
    left_out_ref[...] = normed[:half].reshape(shape).astype(bf16)
    right_out_ref[...] = normed[half:].reshape(shape).astype(bf16)


def inner_kernel(
    x_ref,
    gain_ref,
    pad_ref,
    proj_ref,
    bias_ref,
    sum_left_ref,
    sum_right_ref,
    left_ref,
    right_ref,
    sum_ref,
    normed_ref,
):
    high = 4 * WS
    rows = pl.ds(pl.program_id(0) * high, high)
    inner = range(1, x_ref.shape[1] // WS - 1)
    grid = x_ref[rows].astype(f32)
    places = [(i, j) for i in range(high // WS) for j in inner]
    current = jnp.concatenate(
        [
            grid[i * WS : (i + 1) * WS, j * WS : (j + 1) * WS, :].reshape(AREA, D)
            for i, j in places
        ],
        axis=0,
    )
    after = attention(
        current,
        gain_ref[0, 0:1, :],
        pad_ref[...],
        proj_ref[0],
        bias_ref[...],
        attention_masks(),
        len(places),
    )
    normed = layer_norm(after, gain_ref[1, 0:1, :])

    def spatial(first, value, last):
        pieces = [
            value[n * AREA : (n + 1) * AREA].reshape(WS, WS, D) for n in range(len(places))
        ]
        lines = [
            jnp.concatenate(pieces[i * len(inner) : (i + 1) * len(inner)], axis=1)
            for i in range(high // WS)
        ]
        return jnp.concatenate([first, jnp.concatenate(lines, axis=0), last], axis=1)

    sum_ref[rows] = spatial(sum_left_ref[rows], after, sum_right_ref[rows])
    normed_ref[rows] = spatial(
        left_ref[rows].astype(f32), normed, right_ref[rows].astype(f32)
    ).astype(bf16)


def attention_scratch():
    return [
        pltpu.VMEM((HEADS // 2 * AREA, LANES), f32),
        pltpu.VMEM((WS, WS, LANES), f32),
        pltpu.VMEM((D, 3 * PAD), bf16),
    ]


RESIDENT = pl.BlockSpec(memory_space=pltpu.VMEM)
PARAMS = pltpu.CompilerParams(vmem_limit_bytes=24 << 20)


def resident(*arrays):
    return [pltpu.with_memory_space_constraint(a, pltpu.VMEM) for a in arrays]


def work(flops):
    return pl.CostEstimate(flops=int(flops), transcendentals=0, bytes_accessed=1 << 20)


def edge_attention(tokens, gains, qkv_weight, proj_weight, table):
    side = (tokens.shape[0], WS, D)
    last = tokens.shape[1] // WS - 1
    full = lambda a: pl.BlockSpec(a.shape, lambda i: (0,) * a.ndim)
    return pl.pallas_call(
        edge_kernel,
        grid=(1,),
        in_specs=[
            pl.BlockSpec(side, lambda i: (0, 0, 0)),
            pl.BlockSpec(side, lambda i: (0, last, 0)),
            full(gains),
            full(qkv_weight),
            full(proj_weight),
            full(table),
        ],
        out_specs=[RESIDENT] * 6,
        out_shape=[
            pltpu.VMEM(side, f32),
            pltpu.VMEM(side, f32),
            pltpu.VMEM(side, bf16),
            pltpu.VMEM(side, bf16),
            pltpu.VMEM((HEADS // 2 * AREA, LANES), f32),
            pltpu.VMEM((D, 3 * PAD), bf16),
        ],
        scratch_shapes=[pltpu.VMEM((WS, WS, LANES), f32)],
        compiler_params=PARAMS,
        cost_estimate=work(5e8),
        name="edge_attention",
    )(
        *[
            pltpu.with_memory_space_constraint(a, pltpu.HBM)
            for a in (tokens, tokens, gains, qkv_weight, proj_weight, table)
        ]
    )


def inner_attention(tokens, gains, padded, proj_weight, bias, edges):
    return pl.pallas_call(
        inner_kernel,
        grid=(tokens.shape[0] // (4 * WS),),
        in_specs=[RESIDENT] * 9,
        out_specs=[RESIDENT] * 2,
        out_shape=[pltpu.VMEM(tokens.shape, f32), pltpu.VMEM(tokens.shape, bf16)],
        compiler_params=PARAMS,
        cost_estimate=work(8e9),
        name="inner_attention",
    )(*resident(tokens, gains, padded, proj_weight, bias, *edges))


def low_half(value):
    lane = lax.broadcasted_iota(jnp.int32, value.shape, value.ndim - 1)
    return jnp.where(lane < D - LANES, value, 0.0)


def join_halves(first, second):
    lane = lax.broadcasted_iota(jnp.int32, first.shape, 1)
    return jnp.where(lane < D - LANES, first, pltpu.roll(second, D - LANES, 1))


def shuffled_kernel(
    got_ref, gain_ref, qkv_ref, proj_ref, table_ref, out_ref, bias_s, rows_s, qkv_s, window_s, piece_s
):
    prepare_attention(1, table_ref, qkv_ref, bias_s, rows_s, qkv_s)
    blocks = WS * 2

    def gather(a, carry):
        for c in range(blocks):
            piece = got_ref[a * blocks + c].astype(f32)
            upper = piece[SEGMENT:]
            upper = jnp.concatenate(
                [low_half(upper), low_half(pltpu.roll(upper, D - LANES, 1))], axis=0
            )
            place = pl.ds(
                (c % 2) * SEGMENT * WINDOW_ROWS + a * WS + c // 2, SEGMENT, stride=WINDOW_ROWS
            )
            window_s[0, place, :] = piece[:SEGMENT]
            window_s[1, place, :] = upper
        return carry

    lax.fori_loop(0, WS, gather, 0)
    masks = attention_masks()

    def windows(c, carry):
        starts = [(c * TOGETHER + n) * WINDOW_ROWS for n in range(TOGETHER)]
        current = jnp.concatenate(
            [
                jnp.concatenate(
                    [window_s[t, pl.ds(start, AREA), :] for start in starts], axis=0
                )
                for t in range(2)
            ],
            axis=1,
        )[:, 0:D]
        after = attention(
            current, gain_ref[0, 1:2, :], qkv_s[...], proj_ref[1], bias_s[...], masks, TOGETHER
        )
        for n, start in enumerate(starts):
            window_s[0, pl.ds(start, AREA), :] = after[n * AREA : (n + 1) * AREA, 0:LANES]
            window_s[1, pl.ds(start, AREA), 0 : D - LANES] = after[
                n * AREA : (n + 1) * AREA, LANES:D
            ]
        return carry

    lax.fori_loop(0, 2 * SEGMENT // TOGETHER, windows, 0)

    below = lax.axis_index("row") < WS // 2
    beside = lax.axis_index("block") < WS // 2
    row_step = jnp.where(below, 1, -1)
    row_window = jnp.where(below, 0, 3)
    col_window = jnp.where(beside, 0, 3)

    def scatter(a, carry):
        other_a = a + row_step
        row_keep = jnp.where((other_a >= 0) & (other_a < WS), 1.0, 0.0).astype(f32)
        other_a = jnp.clip(other_a, 0, WS - 1)
        for c in range(blocks):
            b, core = c // 2, c % 2
            other_b = b + (jnp.where(beside, 1, 0) if core else jnp.where(beside, 0, -1))
            col_keep = jnp.where((other_b >= 0) & (other_b < WS), 1.0, 0.0).astype(f32)
            other_b = jnp.clip(other_b, 0, WS - 1)
            base = core * SEGMENT
            other = (1 - core) * SEGMENT
            main = pl.ds(base * WINDOW_ROWS + a * WS + b, SEGMENT, stride=WINDOW_ROWS)
            row = pl.ds(
                (base + row_window * 4) * WINDOW_ROWS + other_a * WS + b, 4, stride=WINDOW_ROWS
            )
            col = pl.ds(
                (other + col_window) * WINDOW_ROWS + a * WS + other_b, 4, stride=4 * WINDOW_ROWS
            )
            corner = pl.ds(
                (other + row_window * 4 + col_window) * WINDOW_ROWS + other_a * WS + other_b, 1
            )
            keep = row_keep * col_keep
            piece_s[0:16] = window_s[0, main, :]
            piece_s[16:20] = window_s[0, row, :] * row_keep
            piece_s[20:24] = window_s[0, col, :] * col_keep
            upper = window_s[1, main, :]
            piece_s[24:32] = join_halves(upper[0:8], upper[8:16])
            piece_s[32:36] = join_halves(
                window_s[1, row, :] * row_keep, window_s[1, col, :] * col_keep
            )
            piece_s[36:37] = window_s[0, corner, :] * keep
            piece_s[37:38] = window_s[1, corner, :] * keep
            out_ref[a * blocks + c] = piece_s[...].astype(bf16)
        return carry

    piece_s[...] = jnp.zeros_like(piece_s)
    lax.fori_loop(0, WS, scatter, 0)


def shuffled_attention(got, gains, qkv_weight, proj_weight, table):
    shape = (got.shape[0], RETURN_ROWS, LANES)
    return pl.pallas_call(
        shuffled_kernel,
        in_specs=[RESIDENT] * 5,
        out_specs=RESIDENT,
        out_shape=pltpu.VMEM(shape, bf16),
        scratch_shapes=attention_scratch()
        + [
            pltpu.VMEM((2, 2 * SEGMENT * WINDOW_ROWS, LANES), f32),
            pltpu.VMEM((RETURN_ROWS, LANES), f32),
        ],
        compiler_params=PARAMS,
        cost_estimate=work(1e10),
        name="shuffled_attention",
    )(*resident(got, gains, qkv_weight, proj_weight, table))


def prepare_finish(layer, taps_ref, down_ref, taps_s, down_s):
    for t in range(KS * KS):
        taps_s[t] = jnp.broadcast_to(
            taps_ref[t, layer : layer + 1, :], (16, D)
        ).astype(bf16)
    down_s[...] = down_ref[layer].T


def convolve_row(padded_s, taps_s, shift_s, row, width):
    total = None
    for v in range(KS):
        part = None
        for u in range(KS):
            x = padded_s[row + u].reshape(-1, 16, D)
            term = x * taps_s[u * KS + v][None]
            part = term if part is None else part + term
        part = part.reshape(-1, D).astype(f32)
        if v == HALO:
            part = part[:width]
        else:
            pieces = []
            for n, value in enumerate((part[:, :LANES], part[:, LANES:])):
                lanes = slice(0, value.shape[1])
                shift_s[v, n, SEGMENT : SEGMENT + RING, lanes] = value
                shift_s[v, n, WS:SEGMENT, lanes] = value[RING - WS :]
                start = SEGMENT + v - HALO
                pieces.append(shift_s[v, n, start : start + width, :])
            part = jnp.concatenate(pieces, axis=1)[:, 0:D]
        total = part if total is None else total + part
    return total


def feed_forward(after, gain, up, down):
    normed = layer_norm(after, gain).astype(bf16)
    raised = mxu(normed, up)
    hidden = (0.5 * raised * (1.0 + lax.erf(raised * 0.5**0.5))).astype(bf16)
    return (after + mxu(hidden, down)).astype(bf16)


def ring(middle, right, left):
    return jnp.concatenate(
        [middle.astype(f32), right.astype(f32), left.astype(f32)], axis=0
    ).astype(bf16)


def middle_kernel(
    sum_ref,
    normed_ref,
    left_ref,
    right_ref,
    gain_ref,
    taps_ref,
    up_ref,
    down_ref,
    out_ref,
    padded_s,
    after_s,
    taps_s,
    shift_s,
    down_s,
):
    step = pl.program_id(0)
    rows = 2 * WS
    width = sum_ref.shape[1]
    first = WS - HALO

    @pl.when(step == 0)
    def _():
        def body(r, carry):
            padded_s[r] = ring(normed_ref[first + r], right_ref[first + r], left_ref[first + r])
            return carry

        lax.fori_loop(0, padded_s.shape[0], body, 0)
        prepare_finish(0, taps_ref, down_ref, taps_s, down_s)

    def row(j, carry):
        total = sum_ref[WS + step * rows + j] + convolve_row(
            padded_s, taps_s, shift_s, step * rows + j, width
        )
        after_s[pl.ds(pl.multiple_of(j * width, width), width), :] = total
        return carry

    lax.fori_loop(0, rows, row, 0)
    outcome = feed_forward(after_s[...], gain_ref[2, 0:1, :], up_ref[0], down_s[...])
    out_ref[pl.ds(step * rows, rows)] = outcome.reshape(rows, width, D)


def middle_finish(after, normed, left, right, gains, taps, up_weight, down_weight):
    height, width = normed.shape[:2]
    inner = height - 2 * WS
    return pl.pallas_call(
        middle_kernel,
        grid=(inner // (2 * WS),),
        in_specs=[RESIDENT] * 8,
        out_specs=RESIDENT,
        out_shape=pltpu.VMEM((inner, width, D), bf16),
        scratch_shapes=[
            pltpu.VMEM((inner + 2 * HALO, RING, D), bf16),
            pltpu.VMEM((2 * WS * width, D), f32),
            pltpu.VMEM((KS * KS, 16, D), bf16),
            pltpu.VMEM((KS, 2, SEGMENT + RING, LANES), f32),
            pltpu.VMEM((HID, D), bf16),
        ],
        compiler_params=PARAMS,
        cost_estimate=work(8e9),
        name="middle_finish",
    )(*resident(after, normed, left, right, gains, taps, up_weight, down_weight))


def outer_kernel(
    sum_ref,
    middle_ref,
    normed_ref,
    top_ref,
    bottom_ref,
    left_ref,
    right_ref,
    gain_ref,
    taps_ref,
    up_ref,
    down_ref,
    send_ref,
    padded_s,
    after_s,
    taps_s,
    shift_s,
    down_s,
    piece_s,
):
    step = pl.program_id(0)
    height, width, _ = normed_ref.shape
    rows = WS
    repeats = height // WS

    @pl.when(step == 0)
    def _():
        for r in range(HALO):
            padded_s[r] = top_ref[r]
            padded_s[height + HALO + r] = bottom_ref[r]

        def body(r, carry):
            padded_s[r + HALO] = ring(normed_ref[r], right_ref[r], left_ref[r])
            return carry

        lax.fori_loop(0, WS + HALO, body, 0)
        lax.fori_loop(height - WS - HALO, height, body, 0)
        prepare_finish(0, taps_ref, down_ref, taps_s, down_s)

    def row(j, carry):
        part, q = j // rows, j % rows
        r = part * (height - WS) + step * rows + q
        total = sum_ref[r] + convolve_row(padded_s, taps_s, shift_s, r, width)
        after_s[pl.ds(pl.multiple_of(j * width, width), width), :] = total
        return carry

    lax.fori_loop(0, 2 * rows, row, 0)
    outcome = feed_forward(after_s[...], gain_ref[2, 0:1, :], up_ref[0], down_s[...]).astype(f32)
    for m in range(repeats):
        for q in range(rows):
            if m in (0, repeats - 1):
                start = ((m > 0) * rows + q) * width
                line = outcome[start : start + width]
            else:
                line = middle_ref[(m - 1) * WS + step * rows + q].astype(f32)
            for n in range(width // SEGMENT):
                value = line[n * SEGMENT : (n + 1) * SEGMENT]
                place = pl.ds((q * SEGMENT + m * 4 + n) * PIECE_STRIDE, SEGMENT)
                piece_s[0, place, :] = value[:, 0:LANES]
                piece_s[1, place, 0 : D - LANES] = value[:, LANES:D]
    for q in range(rows):
        for c in range(SEGMENT):
            place = pl.ds(q * SEGMENT * PIECE_STRIDE + c, SEGMENT, stride=PIECE_STRIDE)
            upper = piece_s[1, place, :]
            send_ref[(step * rows + q) * SEGMENT + c] = jnp.concatenate(
                [piece_s[0, place, :], join_halves(upper[0:8], upper[8:16])], axis=0
            ).astype(bf16)


def outer_finish(
    after, middle, normed, top, bottom, left, right, gains, taps, up_weight, down_weight, group
):
    height, width = normed.shape[:2]
    rows = WS
    return pl.pallas_call(
        outer_kernel,
        grid=(WS // rows,),
        in_specs=[RESIDENT] * 11,
        out_specs=RESIDENT,
        out_shape=pltpu.VMEM((group, PIECE_ROWS, LANES), bf16),
        scratch_shapes=[
            pltpu.VMEM((height + 2 * HALO, RING, D), bf16),
            pltpu.VMEM((2 * rows * width, D), f32),
            pltpu.VMEM((KS * KS, 16, D), bf16),
            pltpu.VMEM((KS, 2, SEGMENT + RING, LANES), f32),
            pltpu.VMEM((HID, D), bf16),
            pltpu.VMEM((2, rows * SEGMENT * PIECE_STRIDE, LANES), f32),
        ],
        compiler_params=PARAMS,
        cost_estimate=work(8e9),
        name="outer_finish",
    )(
        *resident(
            after,
            middle,
            normed,
            top,
            bottom,
            left,
            right,
            gains,
            taps,
            up_weight,
            down_weight,
        )
    )


def second_kernel(
    back_ref,
    gain_ref,
    taps_ref,
    up_ref,
    down_ref,
    out_ref,
    padded_s,
    sum_s,
    after_s,
    taps_s,
    shift_s,
    down_s,
    piece_s,
):
    step = pl.program_id(0)
    rows, width, _ = out_ref.shape
    height = sum_s.shape[0]
    repeats = height // WS

    @pl.when(step == 0)
    def _():
        prepare_finish(1, taps_ref, down_ref, taps_s, down_s)

        def line(n):
            pieces = []
            for m in range(width // SEGMENT + 1):
                if n < 4 and m < 4:
                    low, high, half = 4 * n + m, 24 + (4 * n + m) % 8, (4 * n + m) // 8
                elif m < 4:
                    low, high, half = 16 + m, 32 + m, 0
                elif n < 4:
                    low, high, half = 20 + n, 32 + n, 1
                else:
                    low, high, half = 36, 37, 0
                at = lambda k: piece_s[pl.ds(k, SEGMENT, stride=RETURN_STRIDE), :]
                upper = at(high)
                if half:
                    upper = pltpu.roll(upper, D - LANES, 1)
                pieces.append(jnp.concatenate([at(low), upper], axis=1)[:, 0:D])
            return jnp.concatenate(pieces, axis=0)

        def body(r, carry):
            for c in range(SEGMENT):
                piece_s[c * RETURN_STRIDE : c * RETURN_STRIDE + RETURN_ROWS, :] = back_ref[
                    r * SEGMENT + c
                ].astype(f32)
            lines = [line(n) for n in range(repeats + 1)]
            normed = layer_norm(jnp.concatenate(lines, axis=0), gain_ref[1, 1:2, :]).astype(bf16)
            for n in range(repeats):
                sum_s[r + WS * n] = lines[n][0:width]
                padded_s[HALO + r + WS * n] = normed[n * RING : (n + 1) * RING]
            spare = height + 2 * HALO
            target = jnp.where(
                r < HALO, HALO + height + r, jnp.where(r >= WS - HALO, HALO + r - WS, spare)
            )
            padded_s[target] = normed[repeats * RING :]
            return carry

        lax.fori_loop(0, WS, body, 0)

    def row(j, carry):
        r = step * rows + j
        total = sum_s[r] + convolve_row(padded_s, taps_s, shift_s, r, width)
        after_s[pl.ds(pl.multiple_of(j * width, width), width), :] = total
        return carry

    lax.fori_loop(0, rows, row, 0)
    outcome = feed_forward(after_s[...], gain_ref[2, 1:2, :], up_ref[1], down_s[...])
    out_ref[...] = outcome.reshape(rows, width, D)


def second_finish(back, shape, gains, taps, up_weight, down_weight):
    height, width = shape[:2]
    return pl.pallas_call(
        second_kernel,
        grid=(height // (2 * WS),),
        in_specs=[RESIDENT] * 5,
        out_specs=pl.BlockSpec((2 * WS, width, D), lambda i: (i, 0, 0)),
        out_shape=jax.ShapeDtypeStruct(shape, bf16),
        scratch_shapes=[
            pltpu.VMEM((height + 2 * HALO + 1, RING, D), bf16),
            pltpu.VMEM((height, width, D), f32),
            pltpu.VMEM((2 * WS * width, D), f32),
            pltpu.VMEM((KS * KS, 16, D), bf16),
            pltpu.VMEM((KS, 2, SEGMENT + RING, LANES), f32),
            pltpu.VMEM((HID, D), bf16),
            pltpu.VMEM((SEGMENT * RETURN_STRIDE, LANES), f32),
        ],
        compiler_params=PARAMS,
        cost_estimate=work(1e10),
        name="second_finish",
    )(*resident(back, gains, taps, up_weight, down_weight))


def shift(value, axes, forward):
    count = lax.axis_size(axes)
    pairs = [(i, i + 1) if forward else (i + 1, i) for i in range(count - 1)]
    return lax.ppermute(value, axes, pairs)


def on_device(
    tokens, norm_gain, qkv_weight, proj_weight, bias_table, conv_weight, up_weight, down_weight
):
    members = ("row", "block", "core")
    columns = ("block", "core")
    gains = norm_gain.transpose(1, 0, 2)
    table = bias_table.transpose(1, 0, 2)
    taps = conv_weight.transpose(1, 0, 2)
    down_weight = down_weight.transpose(0, 2, 1)
    *edges, bias, padded = edge_attention(tokens, gains, qkv_weight, proj_weight, table)
    left = shift(edges[3], columns, True)
    right = shift(edges[2], columns, False)
    after, normed = inner_attention(tokens, gains, padded, proj_weight, bias, edges)
    around = lambda rows: jnp.concatenate([normed[rows], right[rows], left[rows]], axis=1)
    height = tokens.shape[0]
    top = shift(around(slice(height - HALO, height)), "row", True)
    bottom = shift(around(slice(0, HALO)), "row", False)
    middle = middle_finish(after, normed, left, right, gains, taps, up_weight, down_weight)
    outgoing = outer_finish(
        after,
        middle,
        normed,
        top,
        bottom,
        left,
        right,
        gains,
        taps,
        up_weight,
        down_weight,
        lax.axis_size(members),
    )
    got = lax.all_to_all(outgoing, members, 0, 0, tiled=True)
    branch = shuffled_attention(got, gains, qkv_weight, proj_weight, table)
    back = lax.all_to_all(branch, members, 0, 0, tiled=True)
    return second_finish(back, tokens.shape, gains, taps, up_weight, down_weight)


def solution(mesh):
    split = Mesh(
        mesh.devices.reshape(mesh.shape["row"], mesh.shape["col"] // 2, 2), ("row", "block", "core")
    )
    spec = P("row", ("block", "core"), None)
    return jax.shard_map(
        on_device, mesh=split, in_specs=(spec,) + (P(),) * 7, out_specs=spec, check_vma=False
    )
```

```python
import functools
import jax
import jax.numpy as jnp
from jax import lax
from jax.experimental import pallas as pl
from jax.experimental.pallas import tpu as pltpu
from jax.sharding import Mesh, PartitionSpec as P

D = 192
HEADS = 6
HID = 768
WS = 8
KS = 7
HEAD = 32
AREA = WS * WS
PAD = 256
LANES = 128
HALO = KS // 2
TOGETHER = 16
WINDOW_ROWS = AREA + 4
PIECE_ROWS = 24
PIECE_STRIDE = PIECE_ROWS + 4
RETURN_ROWS = 40
RETURN_STRIDE = RETURN_ROWS + 4
RING = 80
SEGMENT = 16
EPSILON = 1e-05

f32 = jnp.float32
bf16 = jnp.bfloat16


def layer_norm(values, gain):
    centre = jnp.mean(values, axis=-1, keepdims=True)
    centred = values - centre
    spread = jnp.mean(centred * centred, axis=-1, keepdims=True)
    return centred * lax.rsqrt(spread + EPSILON) * gain


def mxu(a, b):
    return jnp.dot(a, b, preferred_element_type=f32)


def prepare_attention(layer, table_ref, qkv_ref, bias_s, rows_s, qkv_s):
    table = table_ref[:, layer, :]
    high = table.astype(bf16)
    rest = table - high.astype(f32)
    middle = rest.astype(bf16)
    low = (rest - middle.astype(f32)).astype(bf16)
    entries = (2 * WS - 1) ** 2
    lane = lax.broadcasted_iota(jnp.int32, (entries, WS * LANES), 1)
    entry = lax.broadcasted_iota(jnp.int32, (entries, WS * LANES), 0)
    target = (
        (2 * WS - 2 - ((lane & (LANES - 1)) >> 3)) * (2 * WS - 1)
        + (lane >> 7)
        - (lane & 7)
        + WS
        - 1
    )
    chosen = jnp.where(entry == target, 1.0, 0.0).astype(bf16)
    spread = mxu(high, chosen) + mxu(middle, chosen) + mxu(low, chosen)
    for place in range(WS):
        rows_s[place, 0:HEADS, :] = spread[:, place * LANES : (place + 1) * LANES]
    first = lax.broadcasted_iota(jnp.int32, (WS, LANES), 1) < AREA
    for group in range(HEADS // 2):
        left = rows_s[:, 2 * group, :]
        right = rows_s[:, 2 * group + 1, :]
        for row in range(WS):
            shift = LANES - (WS - 1 - row) * WS
            piece = jnp.where(
                first,
                pltpu.roll(left, shift % LANES, 1),
                pltpu.roll(right, (shift + AREA) % LANES, 1),
            )
            bias_s[group * AREA + row * WS : group * AREA + (row + 1) * WS, :] = piece
    weights = qkv_ref[layer].astype(f32)
    gap = jnp.zeros((D, PAD - D), f32)
    qkv_s[...] = jnp.concatenate(
        [
            weights[:, 0:D],
            gap,
            weights[:, D : 2 * D],
            gap,
            weights[:, 2 * D : 3 * D],
            gap,
        ],
        axis=1,
    ).astype(bf16)


def attention_masks():
    lane = lax.broadcasted_iota(jnp.int32, (1, PAD), 1)
    groups = [
        jnp.where((lane >> 6) == g, 1.0, 0.0).astype(bf16) for g in range(HEADS // 2)
    ]
    parities = [
        jnp.where(((lane >> 5) & 1) == h, 1.0, 0.0).astype(bf16) for h in range(2)
    ]
    rows = lax.broadcasted_iota(jnp.int32, (LANES, LANES), 0) >> 6
    cols = lax.broadcasted_iota(jnp.int32, (LANES, LANES), 1) >> 6
    summing = jnp.where(rows == cols, 1.0, 0.0).astype(bf16)
    return groups, parities, summing


def attend(projected, bias, masks):
    groups, parities, summing = masks
    count = projected.shape[0] // AREA
    window = lambda n, t: projected[n * AREA : (n + 1) * AREA, t * PAD : (t + 1) * PAD]
    spread = lambda x, ms: jnp.concatenate([x * m for m in ms], axis=0)
    scores = [
        lax.dot_general(
            spread(window(n, 0), groups),
            spread(window(n, 1), parities),
            (((1,), (1,)), ((), ())),
            preferred_element_type=f32,
        )
        for n in range(count)
    ]
    weights = [jnp.exp(x * HEAD ** (-0.5) + bias) for x in scores]
    totals = [mxu(x.astype(bf16), summing) for x in weights]
    weights = [(x / y).astype(bf16) for x, y in zip(weights, totals)]
    mixed = [mxu(x, spread(window(n, 2), parities)) for n, x in enumerate(weights)]
    lane = lax.broadcasted_iota(jnp.int32, (AREA, PAD), 1) >> 6
    return [
        jnp.where(
            lane == 0, x[0:AREA], jnp.where(lane == 1, x[AREA : 2 * AREA], x[2 * AREA :])
        )[:, 0:D].astype(bf16)
        for x in mixed
    ]


def attention(current, gain, qkv, proj, bias, masks, together):
    normed = layer_norm(current, gain).astype(bf16)
    projected = mxu(normed, qkv).astype(bf16)
    outs = []
    for start in range(0, current.shape[0], together * AREA):
        outs += attend(projected[start : start + together * AREA], bias, masks)
    return current + mxu(jnp.concatenate(outs, axis=0), proj)


def edge_kernel(
    first_ref,
    last_ref,
    gain_ref,
    qkv_ref,
    proj_ref,
    table_ref,
    sum_left_ref,
    sum_right_ref,
    left_out_ref,
    right_out_ref,
    bias_ref,
    pad_ref,
    rows_s,
):
    prepare_attention(0, table_ref, qkv_ref, bias_ref, rows_s, pad_ref)
    sides = [side[...].astype(f32).reshape(-1, D) for side in (first_ref, last_ref)]
    after = attention(
        jnp.concatenate(sides, axis=0),
        gain_ref[0, 0:1, :],
        pad_ref[...],
        proj_ref[0],
        bias_ref[...],
        attention_masks(),
        TOGETHER,
    )
    normed = layer_norm(after, gain_ref[1, 0:1, :])
    half = after.shape[0] // 2
    shape = sum_left_ref.shape
    sum_left_ref[...] = after[:half].reshape(shape)
    sum_right_ref[...] = after[half:].reshape(shape)
    left_out_ref[...] = normed[:half].reshape(shape).astype(bf16)
    right_out_ref[...] = normed[half:].reshape(shape).astype(bf16)


def inner_kernel(
    x_ref,
    gain_ref,
    pad_ref,
    proj_ref,
    bias_ref,
    sum_left_ref,
    sum_right_ref,
    left_ref,
    right_ref,
    sum_ref,
    normed_ref,
):
    high = 4 * WS
    rows = pl.ds(pl.program_id(0) * high, high)
    inner = range(1, x_ref.shape[1] // WS - 1)
    grid = x_ref[rows].astype(f32)
    places = [(i, j) for i in range(high // WS) for j in inner]
    current = jnp.concatenate(
        [
            grid[i * WS : (i + 1) * WS, j * WS : (j + 1) * WS, :].reshape(AREA, D)
            for i, j in places
        ],
        axis=0,
    )
    after = attention(
        current,
        gain_ref[0, 0:1, :],
        pad_ref[...],
        proj_ref[0],
        bias_ref[...],
        attention_masks(),
        len(places),
    )
    normed = layer_norm(after, gain_ref[1, 0:1, :])

    def spatial(first, value, last):
        pieces = [
            value[n * AREA : (n + 1) * AREA].reshape(WS, WS, D) for n in range(len(places))
        ]
        lines = [
            jnp.concatenate(pieces[i * len(inner) : (i + 1) * len(inner)], axis=1)
            for i in range(high // WS)
        ]
        return jnp.concatenate([first, jnp.concatenate(lines, axis=0), last], axis=1)

    sum_ref[rows] = spatial(sum_left_ref[rows], after, sum_right_ref[rows])
    normed_ref[rows] = spatial(
        left_ref[rows].astype(f32), normed, right_ref[rows].astype(f32)
    ).astype(bf16)


def attention_scratch():
    return [
        pltpu.VMEM((HEADS // 2 * AREA, LANES), f32),
        pltpu.VMEM((WS, WS, LANES), f32),
        pltpu.VMEM((D, 3 * PAD), bf16),
    ]


RESIDENT = pl.BlockSpec(memory_space=pltpu.VMEM)
PARAMS = pltpu.CompilerParams(vmem_limit_bytes=24 << 20)


def resident(*arrays):
    return [pltpu.with_memory_space_constraint(a, pltpu.VMEM) for a in arrays]


def work(flops):
    return pl.CostEstimate(flops=int(flops), transcendentals=0, bytes_accessed=1 << 20)


def edge_attention(tokens, gains, qkv_weight, proj_weight, table):
    side = (tokens.shape[0], WS, D)
    last = tokens.shape[1] // WS - 1
    full = lambda a: pl.BlockSpec(a.shape, lambda i: (0,) * a.ndim)
    return pl.pallas_call(
        edge_kernel,
        grid=(1,),
        in_specs=[
            pl.BlockSpec(side, lambda i: (0, 0, 0)),
            pl.BlockSpec(side, lambda i: (0, last, 0)),
            full(gains),
            full(qkv_weight),
            full(proj_weight),
            full(table),
        ],
        out_specs=[RESIDENT] * 6,
        out_shape=[
            pltpu.VMEM(side, f32),
            pltpu.VMEM(side, f32),
            pltpu.VMEM(side, bf16),
            pltpu.VMEM(side, bf16),
            pltpu.VMEM((HEADS // 2 * AREA, LANES), f32),
            pltpu.VMEM((D, 3 * PAD), bf16),
        ],
        scratch_shapes=[pltpu.VMEM((WS, WS, LANES), f32)],
        compiler_params=PARAMS,
        cost_estimate=work(5e8),
        name="edge_attention",
    )(
        *[
            pltpu.with_memory_space_constraint(a, pltpu.HBM)
            for a in (tokens, tokens, gains, qkv_weight, proj_weight, table)
        ]
    )


def inner_attention(tokens, gains, padded, proj_weight, bias, edges):
    return pl.pallas_call(
        inner_kernel,
        grid=(tokens.shape[0] // (4 * WS),),
        in_specs=[RESIDENT] * 9,
        out_specs=[RESIDENT] * 2,
        out_shape=[pltpu.VMEM(tokens.shape, f32), pltpu.VMEM(tokens.shape, bf16)],
        compiler_params=PARAMS,
        cost_estimate=work(8e9),
        name="inner_attention",
    )(*resident(tokens, gains, padded, proj_weight, bias, *edges))


def low_half(value):
    lane = lax.broadcasted_iota(jnp.int32, value.shape, value.ndim - 1)
    return jnp.where(lane < D - LANES, value, 0.0)


def join_halves(first, second):
    lane = lax.broadcasted_iota(jnp.int32, first.shape, 1)
    return jnp.where(lane < D - LANES, first, pltpu.roll(second, D - LANES, 1))


def shuffled_kernel(
    got_ref, gain_ref, qkv_ref, proj_ref, table_ref, out_ref, bias_s, rows_s, qkv_s, window_s, piece_s
):
    prepare_attention(1, table_ref, qkv_ref, bias_s, rows_s, qkv_s)
    blocks = WS * 2

    def gather(a, carry):
        for c in range(blocks):
            piece = got_ref[a * blocks + c].astype(f32)
            upper = piece[SEGMENT:]
            upper = jnp.concatenate(
                [low_half(upper), low_half(pltpu.roll(upper, D - LANES, 1))], axis=0
            )
            place = pl.ds(
                (c % 2) * SEGMENT * WINDOW_ROWS + a * WS + c // 2, SEGMENT, stride=WINDOW_ROWS
            )
            window_s[0, place, :] = piece[:SEGMENT]
            window_s[1, place, :] = upper
        return carry

    lax.fori_loop(0, WS, gather, 0)
    masks = attention_masks()

    def windows(c, carry):
        starts = [(c * TOGETHER + n) * WINDOW_ROWS for n in range(TOGETHER)]
        current = jnp.concatenate(
            [
                jnp.concatenate(
                    [window_s[t, pl.ds(start, AREA), :] for start in starts], axis=0
                )
                for t in range(2)
            ],
            axis=1,
        )[:, 0:D]
        after = attention(
            current, gain_ref[0, 1:2, :], qkv_s[...], proj_ref[1], bias_s[...], masks, TOGETHER
        )
        for n, start in enumerate(starts):
            window_s[0, pl.ds(start, AREA), :] = after[n * AREA : (n + 1) * AREA, 0:LANES]
            window_s[1, pl.ds(start, AREA), 0 : D - LANES] = after[
                n * AREA : (n + 1) * AREA, LANES:D
            ]
        return carry

    lax.fori_loop(0, 2 * SEGMENT // TOGETHER, windows, 0)

    below = lax.axis_index("row") < WS // 2
    beside = lax.axis_index("block") < WS // 2
    row_step = jnp.where(below, 1, -1)
    row_window = jnp.where(below, 0, 3)
    col_window = jnp.where(beside, 0, 3)

    def scatter(a, carry):
        other_a = a + row_step
        row_keep = jnp.where((other_a >= 0) & (other_a < WS), 1.0, 0.0).astype(f32)
        other_a = jnp.clip(other_a, 0, WS - 1)
        for c in range(blocks):
            b, core = c // 2, c % 2
            other_b = b + (jnp.where(beside, 1, 0) if core else jnp.where(beside, 0, -1))
            col_keep = jnp.where((other_b >= 0) & (other_b < WS), 1.0, 0.0).astype(f32)
            other_b = jnp.clip(other_b, 0, WS - 1)
            base = core * SEGMENT
            other = (1 - core) * SEGMENT
            main = pl.ds(base * WINDOW_ROWS + a * WS + b, SEGMENT, stride=WINDOW_ROWS)
            row = pl.ds(
                (base + row_window * 4) * WINDOW_ROWS + other_a * WS + b, 4, stride=WINDOW_ROWS
            )
            col = pl.ds(
                (other + col_window) * WINDOW_ROWS + a * WS + other_b, 4, stride=4 * WINDOW_ROWS
            )
            corner = pl.ds(
                (other + row_window * 4 + col_window) * WINDOW_ROWS + other_a * WS + other_b, 1
            )
            keep = row_keep * col_keep
            piece_s[0:16] = window_s[0, main, :]
            piece_s[16:20] = window_s[0, row, :] * row_keep
            piece_s[20:24] = window_s[0, col, :] * col_keep
            upper = window_s[1, main, :]
            piece_s[24:32] = join_halves(upper[0:8], upper[8:16])
            piece_s[32:36] = join_halves(
                window_s[1, row, :] * row_keep, window_s[1, col, :] * col_keep
            )
            piece_s[36:37] = window_s[0, corner, :] * keep
            piece_s[37:38] = window_s[1, corner, :] * keep
            out_ref[a * blocks + c] = piece_s[...].astype(bf16)
        return carry

    piece_s[...] = jnp.zeros_like(piece_s)
    lax.fori_loop(0, WS, scatter, 0)


def shuffled_attention(got, gains, qkv_weight, proj_weight, table):
    shape = (got.shape[0], RETURN_ROWS, LANES)
    return pl.pallas_call(
        shuffled_kernel,
        in_specs=[RESIDENT] * 5,
        out_specs=RESIDENT,
        out_shape=pltpu.VMEM(shape, bf16),
        scratch_shapes=attention_scratch()
        + [
            pltpu.VMEM((2, 2 * SEGMENT * WINDOW_ROWS, LANES), f32),
            pltpu.VMEM((RETURN_ROWS, LANES), f32),
        ],
        compiler_params=PARAMS,
        cost_estimate=work(1e10),
        name="shuffled_attention",
    )(*resident(got, gains, qkv_weight, proj_weight, table))


def prepare_finish(layer, taps_ref, down_ref, taps_s, down_s):
    for t in range(KS * KS):
        taps_s[t] = jnp.broadcast_to(
            taps_ref[t, layer : layer + 1, :], (16, D)
        ).astype(bf16)
    down_s[...] = down_ref[layer].T


def convolve_row(padded_s, taps_s, shift_s, row, width):
    total = None
    for v in range(KS):
        part = None
        for u in range(KS):
            x = padded_s[row + u].reshape(-1, 16, D)
            term = x * taps_s[u * KS + v][None]
            part = term if part is None else part + term
        part = part.reshape(-1, D).astype(f32)
        if v == HALO:
            part = part[:width]
        else:
            pieces = []
            for n, value in enumerate((part[:, :LANES], part[:, LANES:])):
                lanes = slice(0, value.shape[1])
                shift_s[v, n, SEGMENT : SEGMENT + RING, lanes] = value
                shift_s[v, n, WS:SEGMENT, lanes] = value[RING - WS :]
                start = SEGMENT + v - HALO
                pieces.append(shift_s[v, n, start : start + width, :])
            part = jnp.concatenate(pieces, axis=1)[:, 0:D]
        total = part if total is None else total + part
    return total


def feed_forward(after, gain, up, down):
    normed = layer_norm(after, gain).astype(bf16)
    raised = mxu(normed, up)
    hidden = (0.5 * raised * (1.0 + lax.erf(raised * 0.5**0.5))).astype(bf16)
    return (after + mxu(hidden, down)).astype(bf16)


def ring(middle, right, left):
    return jnp.concatenate(
        [middle.astype(f32), right.astype(f32), left.astype(f32)], axis=0
    ).astype(bf16)


def middle_kernel(
    sum_ref,
    normed_ref,
    left_ref,
    right_ref,
    gain_ref,
    taps_ref,
    up_ref,
    down_ref,
    out_ref,
    padded_s,
    after_s,
    taps_s,
    shift_s,
    down_s,
):
    step = pl.program_id(0)
    rows = 2 * WS
    width = sum_ref.shape[1]
    first = WS - HALO

    @pl.when(step == 0)
    def _():
        def body(r, carry):
            padded_s[r] = ring(normed_ref[first + r], right_ref[first + r], left_ref[first + r])
            return carry

        lax.fori_loop(0, padded_s.shape[0], body, 0)
        prepare_finish(0, taps_ref, down_ref, taps_s, down_s)

    def row(j, carry):
        total = sum_ref[WS + step * rows + j] + convolve_row(
            padded_s, taps_s, shift_s, step * rows + j, width
        )
        after_s[pl.ds(pl.multiple_of(j * width, width), width), :] = total
        return carry

    lax.fori_loop(0, rows, row, 0)
    outcome = feed_forward(after_s[...], gain_ref[2, 0:1, :], up_ref[0], down_s[...])
    out_ref[pl.ds(step * rows, rows)] = outcome.reshape(rows, width, D)


def middle_finish(after, normed, left, right, gains, taps, up_weight, down_weight):
    height, width = normed.shape[:2]
    inner = height - 2 * WS
    return pl.pallas_call(
        middle_kernel,
        grid=(inner // (2 * WS),),
        in_specs=[RESIDENT] * 8,
        out_specs=RESIDENT,
        out_shape=pltpu.VMEM((inner, width, D), bf16),
        scratch_shapes=[
            pltpu.VMEM((inner + 2 * HALO, RING, D), bf16),
            pltpu.VMEM((2 * WS * width, D), f32),
            pltpu.VMEM((KS * KS, 16, D), bf16),
            pltpu.VMEM((KS, 2, SEGMENT + RING, LANES), f32),
            pltpu.VMEM((HID, D), bf16),
        ],
        compiler_params=PARAMS,
        cost_estimate=work(8e9),
        name="middle_finish",
    )(*resident(after, normed, left, right, gains, taps, up_weight, down_weight))


def outer_kernel(
    sum_ref,
    middle_ref,
    normed_ref,
    top_ref,
    bottom_ref,
    left_ref,
    right_ref,
    gain_ref,
    taps_ref,
    up_ref,
    down_ref,
    send_ref,
    padded_s,
    after_s,
    taps_s,
    shift_s,
    down_s,
    piece_s,
):
    step = pl.program_id(0)
    height, width, _ = normed_ref.shape
    rows = WS
    repeats = height // WS

    @pl.when(step == 0)
    def _():
        for r in range(HALO):
            padded_s[r] = top_ref[r]
            padded_s[height + HALO + r] = bottom_ref[r]

        def body(r, carry):
            padded_s[r + HALO] = ring(normed_ref[r], right_ref[r], left_ref[r])
            return carry

        lax.fori_loop(0, WS + HALO, body, 0)
        lax.fori_loop(height - WS - HALO, height, body, 0)
        prepare_finish(0, taps_ref, down_ref, taps_s, down_s)

    def row(j, carry):
        part, q = j // rows, j % rows
        r = part * (height - WS) + step * rows + q
        total = sum_ref[r] + convolve_row(padded_s, taps_s, shift_s, r, width)
        after_s[pl.ds(pl.multiple_of(j * width, width), width), :] = total
        return carry

    lax.fori_loop(0, 2 * rows, row, 0)
    outcome = feed_forward(after_s[...], gain_ref[2, 0:1, :], up_ref[0], down_s[...]).astype(f32)
    for m in range(repeats):
        for q in range(rows):
            if m in (0, repeats - 1):
                start = ((m > 0) * rows + q) * width
                line = outcome[start : start + width]
            else:
                line = middle_ref[(m - 1) * WS + step * rows + q].astype(f32)
            for n in range(width // SEGMENT):
                value = line[n * SEGMENT : (n + 1) * SEGMENT]
                place = pl.ds((q * SEGMENT + m * 4 + n) * PIECE_STRIDE, SEGMENT)
                piece_s[0, place, :] = value[:, 0:LANES]
                piece_s[1, place, 0 : D - LANES] = value[:, LANES:D]
    for q in range(rows):
        for c in range(SEGMENT):
            place = pl.ds(q * SEGMENT * PIECE_STRIDE + c, SEGMENT, stride=PIECE_STRIDE)
            upper = piece_s[1, place, :]
            send_ref[(step * rows + q) * SEGMENT + c] = jnp.concatenate(
                [piece_s[0, place, :], join_halves(upper[0:8], upper[8:16])], axis=0
            ).astype(bf16)


def outer_finish(
    after, middle, normed, top, bottom, left, right, gains, taps, up_weight, down_weight, group
):
    height, width = normed.shape[:2]
    rows = WS
    return pl.pallas_call(
        outer_kernel,
        grid=(WS // rows,),
        in_specs=[RESIDENT] * 11,
        out_specs=RESIDENT,
        out_shape=pltpu.VMEM((group, PIECE_ROWS, LANES), bf16),
        scratch_shapes=[
            pltpu.VMEM((height + 2 * HALO, RING, D), bf16),
            pltpu.VMEM((2 * rows * width, D), f32),
            pltpu.VMEM((KS * KS, 16, D), bf16),
            pltpu.VMEM((KS, 2, SEGMENT + RING, LANES), f32),
            pltpu.VMEM((HID, D), bf16),
            pltpu.VMEM((2, rows * SEGMENT * PIECE_STRIDE, LANES), f32),
        ],
        compiler_params=PARAMS,
        cost_estimate=work(8e9),
        name="outer_finish",
    )(
        *resident(
            after,
            middle,
            normed,
            top,
            bottom,
            left,
            right,
            gains,
            taps,
            up_weight,
            down_weight,
        )
    )


def second_kernel(
    back_ref,
    gain_ref,
    taps_ref,
    up_ref,
    down_ref,
    out_ref,
    padded_s,
    sum_s,
    after_s,
    taps_s,
    shift_s,
    down_s,
    piece_s,
):
    step = pl.program_id(0)
    rows, width, _ = out_ref.shape
    height = sum_s.shape[0]
    repeats = height // WS

    @pl.when(step == 0)
    def _():
        prepare_finish(1, taps_ref, down_ref, taps_s, down_s)

        def line(n):
            pieces = []
            for m in range(width // SEGMENT + 1):
                if n < 4 and m < 4:
                    low, high, half = 4 * n + m, 24 + (4 * n + m) % 8, (4 * n + m) // 8
                elif m < 4:
                    low, high, half = 16 + m, 32 + m, 0
                elif n < 4:
                    low, high, half = 20 + n, 32 + n, 1
                else:
                    low, high, half = 36, 37, 0
                at = lambda k: piece_s[pl.ds(k, SEGMENT, stride=RETURN_STRIDE), :]
                upper = at(high)
                if half:
                    upper = pltpu.roll(upper, D - LANES, 1)
                pieces.append(jnp.concatenate([at(low), upper], axis=1)[:, 0:D])
            return jnp.concatenate(pieces, axis=0)

        def body(r, carry):
            for c in range(SEGMENT):
                piece_s[c * RETURN_STRIDE : c * RETURN_STRIDE + RETURN_ROWS, :] = back_ref[
                    r * SEGMENT + c
                ].astype(f32)
            lines = [line(n) for n in range(repeats + 1)]
            normed = layer_norm(jnp.concatenate(lines, axis=0), gain_ref[1, 1:2, :]).astype(bf16)
            for n in range(repeats):
                sum_s[r + WS * n] = lines[n][0:width]
                padded_s[HALO + r + WS * n] = normed[n * RING : (n + 1) * RING]
            spare = height + 2 * HALO
            target = jnp.where(
                r < HALO, HALO + height + r, jnp.where(r >= WS - HALO, HALO + r - WS, spare)
            )
            padded_s[target] = normed[repeats * RING :]
            return carry

        lax.fori_loop(0, WS, body, 0)

    def row(j, carry):
        r = step * rows + j
        total = sum_s[r] + convolve_row(padded_s, taps_s, shift_s, r, width)
        after_s[pl.ds(pl.multiple_of(j * width, width), width), :] = total
        return carry

    lax.fori_loop(0, rows, row, 0)
    outcome = feed_forward(after_s[...], gain_ref[2, 1:2, :], up_ref[1], down_s[...])
    out_ref[...] = outcome.reshape(rows, width, D)


def second_finish(back, shape, gains, taps, up_weight, down_weight):
    height, width = shape[:2]
    return pl.pallas_call(
        second_kernel,
        grid=(height // (2 * WS),),
        in_specs=[RESIDENT] * 5,
        out_specs=pl.BlockSpec((2 * WS, width, D), lambda i: (i, 0, 0)),
        out_shape=jax.ShapeDtypeStruct(shape, bf16),
        scratch_shapes=[
            pltpu.VMEM((height + 2 * HALO + 1, RING, D), bf16),
            pltpu.VMEM((height, width, D), f32),
            pltpu.VMEM((2 * WS * width, D), f32),
            pltpu.VMEM((KS * KS, 16, D), bf16),
            pltpu.VMEM((KS, 2, SEGMENT + RING, LANES), f32),
            pltpu.VMEM((HID, D), bf16),
            pltpu.VMEM((SEGMENT * RETURN_STRIDE, LANES), f32),
        ],
        compiler_params=PARAMS,
        cost_estimate=work(1e10),
        name="second_finish",
    )(*resident(back, gains, taps, up_weight, down_weight))


def swap(first, last, axes):
    count = lax.axis_size(axes)
    even = lax.axis_index(axes) % 2 == 0
    results = []
    for start in range(2):
        pairs = [
            pair for i in range(start, count - 1, 2) for pair in ((i, i + 1), (i + 1, i))
        ]
        facing = jnp.where(even, last, first) if start == 0 else jnp.where(even, first, last)
        results.append(lax.ppermute(facing, axes, pairs))
    partner, other = results
    return jnp.where(even, other, partner), jnp.where(even, partner, other)


def on_device(
    tokens, norm_gain, qkv_weight, proj_weight, bias_table, conv_weight, up_weight, down_weight
):
    members = ("row", "block", "core")
    columns = ("block", "core")
    gains = norm_gain.transpose(1, 0, 2)
    table = bias_table.transpose(1, 0, 2)
    taps = conv_weight.transpose(1, 0, 2)
    down_weight = down_weight.transpose(0, 2, 1)
    *edges, bias, padded = edge_attention(tokens, gains, qkv_weight, proj_weight, table)
    left, right = swap(edges[2], edges[3], columns)
    after, normed = inner_attention(tokens, gains, padded, proj_weight, bias, edges)
    around = lambda rows: jnp.concatenate([normed[rows], right[rows], left[rows]], axis=1)
    height = tokens.shape[0]
    top, bottom = swap(around(slice(0, HALO)), around(slice(height - HALO, height)), "row")
    middle = middle_finish(after, normed, left, right, gains, taps, up_weight, down_weight)
    outgoing = outer_finish(
        after,
        middle,
        normed,
        top,
        bottom,
        left,
        right,
        gains,
        taps,
        up_weight,
        down_weight,
        lax.axis_size(members),
    )
    got = lax.all_to_all(outgoing, members, 0, 0, tiled=True)
    branch = shuffled_attention(got, gains, qkv_weight, proj_weight, table)
    back = lax.all_to_all(branch, members, 0, 0, tiled=True)
    return second_finish(back, tokens.shape, gains, taps, up_weight, down_weight)


def solution(mesh):
    split = Mesh(
        mesh.devices.reshape(mesh.shape["row"], mesh.shape["col"] // 2, 2), ("row", "block", "core")
    )
    spec = P("row", ("block", "core"), None)
    return jax.shard_map(
        on_device, mesh=split, in_specs=(spec,) + (P(),) * 7, out_specs=spec, check_vma=False
    )
```

```python
import functools
import jax
import jax.numpy as jnp
from jax import lax
from jax.experimental import pallas as pl
from jax.experimental.pallas import tpu as pltpu
from jax.sharding import Mesh, PartitionSpec as P

D = 192
HEADS = 6
HID = 768
WS = 8
KS = 7
HEAD = 32
AREA = WS * WS
PAD = 256
LANES = 128
HALO = KS // 2
TOGETHER = 16
WINDOW_ROWS = AREA + 4
PIECE_ROWS = 24
PIECE_STRIDE = PIECE_ROWS + 4
RETURN_ROWS = 40
RETURN_STRIDE = RETURN_ROWS + 4
RING = 80
SEGMENT = 16
EPSILON = 1e-05

f32 = jnp.float32
bf16 = jnp.bfloat16


def layer_norm(values, gain):
    centre = jnp.mean(values, axis=-1, keepdims=True)
    centred = values - centre
    spread = jnp.mean(centred * centred, axis=-1, keepdims=True)
    return centred * lax.rsqrt(spread + EPSILON) * gain


def mxu(a, b):
    return jnp.dot(a, b, preferred_element_type=f32)


def prepare_attention(layer, table_ref, qkv_ref, bias_s, rows_s, qkv_s):
    table = table_ref[:, layer, :]
    high = table.astype(bf16)
    rest = table - high.astype(f32)
    middle = rest.astype(bf16)
    low = (rest - middle.astype(f32)).astype(bf16)
    entries = (2 * WS - 1) ** 2
    lane = lax.broadcasted_iota(jnp.int32, (entries, WS * LANES), 1)
    entry = lax.broadcasted_iota(jnp.int32, (entries, WS * LANES), 0)
    target = (
        (2 * WS - 2 - ((lane & (LANES - 1)) >> 3)) * (2 * WS - 1)
        + (lane >> 7)
        - (lane & 7)
        + WS
        - 1
    )
    chosen = jnp.where(entry == target, 1.0, 0.0).astype(bf16)
    spread = mxu(high, chosen) + mxu(middle, chosen) + mxu(low, chosen)
    for place in range(WS):
        rows_s[place, 0:HEADS, :] = spread[:, place * LANES : (place + 1) * LANES]
    first = lax.broadcasted_iota(jnp.int32, (WS, LANES), 1) < AREA
    for group in range(HEADS // 2):
        left = rows_s[:, 2 * group, :]
        right = rows_s[:, 2 * group + 1, :]
        for row in range(WS):
            shift = LANES - (WS - 1 - row) * WS
            piece = jnp.where(
                first,
                pltpu.roll(left, shift % LANES, 1),
                pltpu.roll(right, (shift + AREA) % LANES, 1),
            )
            bias_s[group * AREA + row * WS : group * AREA + (row + 1) * WS, :] = piece
    weights = qkv_ref[layer].astype(f32)
    gap = jnp.zeros((D, PAD - D), f32)
    qkv_s[...] = jnp.concatenate(
        [
            weights[:, 0:D],
            gap,
            weights[:, D : 2 * D],
            gap,
            weights[:, 2 * D : 3 * D],
            gap,
        ],
        axis=1,
    ).astype(bf16)


def attention_masks():
    lane = lax.broadcasted_iota(jnp.int32, (1, PAD), 1)
    groups = [
        jnp.where((lane >> 6) == g, 1.0, 0.0).astype(bf16) for g in range(HEADS // 2)
    ]
    parities = [
        jnp.where(((lane >> 5) & 1) == h, 1.0, 0.0).astype(bf16) for h in range(2)
    ]
    rows = lax.broadcasted_iota(jnp.int32, (LANES, LANES), 0) >> 6
    cols = lax.broadcasted_iota(jnp.int32, (LANES, LANES), 1) >> 6
    summing = jnp.where(rows == cols, 1.0, 0.0).astype(bf16)
    return groups, parities, summing


def attend(projected, bias, masks):
    groups, parities, summing = masks
    count = projected.shape[0] // AREA
    window = lambda n, t: projected[n * AREA : (n + 1) * AREA, t * PAD : (t + 1) * PAD]
    spread = lambda x, ms: jnp.concatenate([x * m for m in ms], axis=0)
    scores = [
        lax.dot_general(
            spread(window(n, 0), groups),
            spread(window(n, 1), parities),
            (((1,), (1,)), ((), ())),
            preferred_element_type=f32,
        )
        for n in range(count)
    ]
    weights = [jnp.exp(x * HEAD ** (-0.5) + bias) for x in scores]
    totals = [mxu(x.astype(bf16), summing) for x in weights]
    weights = [(x / y).astype(bf16) for x, y in zip(weights, totals)]
    mixed = [mxu(x, spread(window(n, 2), parities)) for n, x in enumerate(weights)]
    lane = lax.broadcasted_iota(jnp.int32, (AREA, PAD), 1) >> 6
    return [
        jnp.where(
            lane == 0, x[0:AREA], jnp.where(lane == 1, x[AREA : 2 * AREA], x[2 * AREA :])
        )[:, 0:D].astype(bf16)
        for x in mixed
    ]


def attention(current, gain, qkv, proj, bias, masks, together):
    normed = layer_norm(current, gain).astype(bf16)
    projected = mxu(normed, qkv).astype(bf16)
    outs = []
    for start in range(0, current.shape[0], together * AREA):
        outs += attend(projected[start : start + together * AREA], bias, masks)
    return current + mxu(jnp.concatenate(outs, axis=0), proj)


def edge_kernel(
    first_ref,
    last_ref,
    gain_ref,
    qkv_ref,
    proj_ref,
    table_ref,
    sum_left_ref,
    sum_right_ref,
    left_out_ref,
    right_out_ref,
    facing_ref,
    behind_ref,
    bias_ref,
    pad_ref,
    rows_s,
):
    prepare_attention(0, table_ref, qkv_ref, bias_ref, rows_s, pad_ref)
    sides = [side[...].astype(f32).reshape(-1, D) for side in (first_ref, last_ref)]
    after = attention(
        jnp.concatenate(sides, axis=0),
        gain_ref[0, 0:1, :],
        pad_ref[...],
        proj_ref[0],
        bias_ref[...],
        attention_masks(),
        TOGETHER,
    )
    normed = layer_norm(after, gain_ref[1, 0:1, :])
    half = after.shape[0] // 2
    shape = sum_left_ref.shape
    sum_left_ref[...] = after[:half].reshape(shape)
    sum_right_ref[...] = after[half:].reshape(shape)
    left = normed[:half].reshape(shape)
    right = normed[half:].reshape(shape)
    left_out_ref[...] = left.astype(bf16)
    right_out_ref[...] = right.astype(bf16)
    even = lax.axis_index("core") == 0
    facing_ref[...] = jnp.where(even, right, left).astype(bf16)
    behind_ref[...] = jnp.where(even, left, right).astype(bf16)


def inner_kernel(
    x_ref,
    gain_ref,
    pad_ref,
    proj_ref,
    bias_ref,
    sum_left_ref,
    sum_right_ref,
    left_ref,
    right_ref,
    sum_ref,
    normed_ref,
):
    high = 4 * WS
    rows = pl.ds(pl.program_id(0) * high, high)
    inner = range(1, x_ref.shape[1] // WS - 1)
    grid = x_ref[rows].astype(f32)
    places = [(i, j) for i in range(high // WS) for j in inner]
    current = jnp.concatenate(
        [
            grid[i * WS : (i + 1) * WS, j * WS : (j + 1) * WS, :].reshape(AREA, D)
            for i, j in places
        ],
        axis=0,
    )
    after = attention(
        current,
        gain_ref[0, 0:1, :],
        pad_ref[...],
        proj_ref[0],
        bias_ref[...],
        attention_masks(),
        len(places),
    )
    normed = layer_norm(after, gain_ref[1, 0:1, :])

    def spatial(first, value, last):
        pieces = [
            value[n * AREA : (n + 1) * AREA].reshape(WS, WS, D) for n in range(len(places))
        ]
        lines = [
            jnp.concatenate(pieces[i * len(inner) : (i + 1) * len(inner)], axis=1)
            for i in range(high // WS)
        ]
        return jnp.concatenate([first, jnp.concatenate(lines, axis=0), last], axis=1)

    sum_ref[rows] = spatial(sum_left_ref[rows], after, sum_right_ref[rows])
    normed_ref[rows] = spatial(
        left_ref[rows].astype(f32), normed, right_ref[rows].astype(f32)
    ).astype(bf16)


def attention_scratch():
    return [
        pltpu.VMEM((HEADS // 2 * AREA, LANES), f32),
        pltpu.VMEM((WS, WS, LANES), f32),
        pltpu.VMEM((D, 3 * PAD), bf16),
    ]


RESIDENT = pl.BlockSpec(memory_space=pltpu.VMEM)
PARAMS = pltpu.CompilerParams(vmem_limit_bytes=24 << 20)


def resident(*arrays):
    return [pltpu.with_memory_space_constraint(a, pltpu.VMEM) for a in arrays]


def work(flops):
    return pl.CostEstimate(flops=int(flops), transcendentals=0, bytes_accessed=1 << 20)


def edge_attention(tokens, gains, qkv_weight, proj_weight, table):
    side = (tokens.shape[0], WS, D)
    last = tokens.shape[1] // WS - 1
    full = lambda a: pl.BlockSpec(a.shape, lambda i: (0,) * a.ndim)
    return pl.pallas_call(
        edge_kernel,
        grid=(1,),
        in_specs=[
            pl.BlockSpec(side, lambda i: (0, 0, 0)),
            pl.BlockSpec(side, lambda i: (0, last, 0)),
            full(gains),
            full(qkv_weight),
            full(proj_weight),
            full(table),
        ],
        out_specs=[RESIDENT] * 8,
        out_shape=[
            pltpu.VMEM(side, f32),
            pltpu.VMEM(side, f32),
            pltpu.VMEM(side, bf16),
            pltpu.VMEM(side, bf16),
            pltpu.VMEM(side, bf16),
            pltpu.VMEM(side, bf16),
            pltpu.VMEM((HEADS // 2 * AREA, LANES), f32),
            pltpu.VMEM((D, 3 * PAD), bf16),
        ],
        scratch_shapes=[pltpu.VMEM((WS, WS, LANES), f32)],
        compiler_params=PARAMS,
        cost_estimate=work(5e8),
        name="edge_attention",
    )(
        *[
            pltpu.with_memory_space_constraint(a, pltpu.HBM)
            for a in (tokens, tokens, gains, qkv_weight, proj_weight, table)
        ]
    )


def inner_attention(tokens, gains, padded, proj_weight, bias, edges):
    return pl.pallas_call(
        inner_kernel,
        grid=(tokens.shape[0] // (4 * WS),),
        in_specs=[RESIDENT] * 9,
        out_specs=[RESIDENT] * 2,
        out_shape=[pltpu.VMEM(tokens.shape, f32), pltpu.VMEM(tokens.shape, bf16)],
        compiler_params=PARAMS,
        cost_estimate=work(8e9),
        name="inner_attention",
    )(*resident(tokens, gains, padded, proj_weight, bias, *edges))


def low_half(value):
    lane = lax.broadcasted_iota(jnp.int32, value.shape, value.ndim - 1)
    return jnp.where(lane < D - LANES, value, 0.0)


def join_halves(first, second):
    lane = lax.broadcasted_iota(jnp.int32, first.shape, 1)
    return jnp.where(lane < D - LANES, first, pltpu.roll(second, D - LANES, 1))


def shuffled_kernel(
    got_ref, gain_ref, qkv_ref, proj_ref, table_ref, out_ref, bias_s, rows_s, qkv_s, window_s, piece_s
):
    prepare_attention(1, table_ref, qkv_ref, bias_s, rows_s, qkv_s)
    blocks = WS * 2

    def gather(a, carry):
        for c in range(blocks):
            piece = got_ref[a * blocks + c].astype(f32)
            upper = piece[SEGMENT:]
            upper = jnp.concatenate(
                [low_half(upper), low_half(pltpu.roll(upper, D - LANES, 1))], axis=0
            )
            place = pl.ds(
                (c % 2) * SEGMENT * WINDOW_ROWS + a * WS + c // 2, SEGMENT, stride=WINDOW_ROWS
            )
            window_s[0, place, :] = piece[:SEGMENT]
            window_s[1, place, :] = upper
        return carry

    lax.fori_loop(0, WS, gather, 0)
    masks = attention_masks()

    def windows(c, carry):
        starts = [(c * TOGETHER + n) * WINDOW_ROWS for n in range(TOGETHER)]
        current = jnp.concatenate(
            [
                jnp.concatenate(
                    [window_s[t, pl.ds(start, AREA), :] for start in starts], axis=0
                )
                for t in range(2)
            ],
            axis=1,
        )[:, 0:D]
        after = attention(
            current, gain_ref[0, 1:2, :], qkv_s[...], proj_ref[1], bias_s[...], masks, TOGETHER
        )
        for n, start in enumerate(starts):
            window_s[0, pl.ds(start, AREA), :] = after[n * AREA : (n + 1) * AREA, 0:LANES]
            window_s[1, pl.ds(start, AREA), 0 : D - LANES] = after[
                n * AREA : (n + 1) * AREA, LANES:D
            ]
        return carry

    lax.fori_loop(0, 2 * SEGMENT // TOGETHER, windows, 0)

    below = lax.axis_index("row") < WS // 2
    beside = lax.axis_index("block") < WS // 2
    row_step = jnp.where(below, 1, -1)
    row_window = jnp.where(below, 0, 3)
    col_window = jnp.where(beside, 0, 3)

    def scatter(a, carry):
        other_a = a + row_step
        row_keep = jnp.where((other_a >= 0) & (other_a < WS), 1.0, 0.0).astype(f32)
        other_a = jnp.clip(other_a, 0, WS - 1)
        for c in range(blocks):
            b, core = c // 2, c % 2
            other_b = b + (jnp.where(beside, 1, 0) if core else jnp.where(beside, 0, -1))
            col_keep = jnp.where((other_b >= 0) & (other_b < WS), 1.0, 0.0).astype(f32)
            other_b = jnp.clip(other_b, 0, WS - 1)
            base = core * SEGMENT
            other = (1 - core) * SEGMENT
            main = pl.ds(base * WINDOW_ROWS + a * WS + b, SEGMENT, stride=WINDOW_ROWS)
            row = pl.ds(
                (base + row_window * 4) * WINDOW_ROWS + other_a * WS + b, 4, stride=WINDOW_ROWS
            )
            col = pl.ds(
                (other + col_window) * WINDOW_ROWS + a * WS + other_b, 4, stride=4 * WINDOW_ROWS
            )
            corner = pl.ds(
                (other + row_window * 4 + col_window) * WINDOW_ROWS + other_a * WS + other_b, 1
            )
            keep = row_keep * col_keep
            piece_s[0:16] = window_s[0, main, :]
            piece_s[16:20] = window_s[0, row, :] * row_keep
            piece_s[20:24] = window_s[0, col, :] * col_keep
            upper = window_s[1, main, :]
            piece_s[24:32] = join_halves(upper[0:8], upper[8:16])
            piece_s[32:36] = join_halves(
                window_s[1, row, :] * row_keep, window_s[1, col, :] * col_keep
            )
            piece_s[36:37] = window_s[0, corner, :] * keep
            piece_s[37:38] = window_s[1, corner, :] * keep
            out_ref[a * blocks + c] = piece_s[...].astype(bf16)
        return carry

    piece_s[...] = jnp.zeros_like(piece_s)
    lax.fori_loop(0, WS, scatter, 0)


def shuffled_attention(got, gains, qkv_weight, proj_weight, table):
    shape = (got.shape[0], RETURN_ROWS, LANES)
    return pl.pallas_call(
        shuffled_kernel,
        in_specs=[RESIDENT] * 5,
        out_specs=RESIDENT,
        out_shape=pltpu.VMEM(shape, bf16),
        scratch_shapes=attention_scratch()
        + [
            pltpu.VMEM((2, 2 * SEGMENT * WINDOW_ROWS, LANES), f32),
            pltpu.VMEM((RETURN_ROWS, LANES), f32),
        ],
        compiler_params=PARAMS,
        cost_estimate=work(1e10),
        name="shuffled_attention",
    )(*resident(got, gains, qkv_weight, proj_weight, table))


def prepare_finish(layer, taps_ref, down_ref, taps_s, down_s):
    for t in range(KS * KS):
        taps_s[t] = jnp.broadcast_to(
            taps_ref[t, layer : layer + 1, :], (16, D)
        ).astype(bf16)
    down_s[...] = down_ref[layer].T


def convolve_row(padded_s, taps_s, shift_s, row, width):
    total = None
    for v in range(KS):
        part = None
        for u in range(KS):
            x = padded_s[row + u].reshape(-1, 16, D)
            term = x * taps_s[u * KS + v][None]
            part = term if part is None else part + term
        part = part.reshape(-1, D).astype(f32)
        if v == HALO:
            part = part[:width]
        else:
            pieces = []
            for n, value in enumerate((part[:, :LANES], part[:, LANES:])):
                lanes = slice(0, value.shape[1])
                shift_s[v, n, SEGMENT : SEGMENT + RING, lanes] = value
                shift_s[v, n, WS:SEGMENT, lanes] = value[RING - WS :]
                start = SEGMENT + v - HALO
                pieces.append(shift_s[v, n, start : start + width, :])
            part = jnp.concatenate(pieces, axis=1)[:, 0:D]
        total = part if total is None else total + part
    return total


def feed_forward(after, gain, up, down):
    normed = layer_norm(after, gain).astype(bf16)
    raised = mxu(normed, up)
    hidden = (0.5 * raised * (1.0 + lax.erf(raised * 0.5**0.5))).astype(bf16)
    return (after + mxu(hidden, down)).astype(bf16)


def ring(middle, right, left):
    return jnp.concatenate(
        [middle.astype(f32), right.astype(f32), left.astype(f32)], axis=0
    ).astype(bf16)


def middle_kernel(
    sum_ref,
    normed_ref,
    left_ref,
    right_ref,
    gain_ref,
    taps_ref,
    up_ref,
    down_ref,
    out_ref,
    padded_s,
    after_s,
    taps_s,
    shift_s,
    down_s,
):
    step = pl.program_id(0)
    rows = 2 * WS
    width = sum_ref.shape[1]
    first = WS - HALO

    @pl.when(step == 0)
    def _():
        def body(r, carry):
            padded_s[r] = ring(normed_ref[first + r], right_ref[first + r], left_ref[first + r])
            return carry

        lax.fori_loop(0, padded_s.shape[0], body, 0)
        prepare_finish(0, taps_ref, down_ref, taps_s, down_s)

    def row(j, carry):
        total = sum_ref[WS + step * rows + j] + convolve_row(
            padded_s, taps_s, shift_s, step * rows + j, width
        )
        after_s[pl.ds(pl.multiple_of(j * width, width), width), :] = total
        return carry

    lax.fori_loop(0, rows, row, 0)
    outcome = feed_forward(after_s[...], gain_ref[2, 0:1, :], up_ref[0], down_s[...])
    out_ref[pl.ds(step * rows, rows)] = outcome.reshape(rows, width, D)


def middle_finish(after, normed, left, right, gains, taps, up_weight, down_weight):
    height, width = normed.shape[:2]
    inner = height - 2 * WS
    return pl.pallas_call(
        middle_kernel,
        grid=(inner // (2 * WS),),
        in_specs=[RESIDENT] * 8,
        out_specs=RESIDENT,
        out_shape=pltpu.VMEM((inner, width, D), bf16),
        scratch_shapes=[
            pltpu.VMEM((inner + 2 * HALO, RING, D), bf16),
            pltpu.VMEM((2 * WS * width, D), f32),
            pltpu.VMEM((KS * KS, 16, D), bf16),
            pltpu.VMEM((KS, 2, SEGMENT + RING, LANES), f32),
            pltpu.VMEM((HID, D), bf16),
        ],
        compiler_params=PARAMS,
        cost_estimate=work(8e9),
        name="middle_finish",
    )(*resident(after, normed, left, right, gains, taps, up_weight, down_weight))


def turn_kernel(
    normed_ref, partner_ref, other_ref, left_ref, right_ref, facing_ref, behind_ref
):
    height = normed_ref.shape[0]
    even = lax.axis_index("core") == 0
    partner = partner_ref[...].astype(f32)
    other = other_ref[...].astype(f32)
    left_ref[...] = jnp.where(even, other, partner).astype(bf16)
    right_ref[...] = jnp.where(even, partner, other).astype(bf16)
    even = lax.axis_index("row") % 2 == 0
    for r in range(HALO):
        first = ring(normed_ref[r], right_ref[r], left_ref[r]).astype(f32)
        n = height - HALO + r
        last = ring(normed_ref[n], right_ref[n], left_ref[n]).astype(f32)
        facing_ref[r] = jnp.where(even, last, first).astype(bf16)
        behind_ref[r] = jnp.where(even, first, last).astype(bf16)


def turn(normed, partner, other):
    rows = (HALO, RING, D)
    return pl.pallas_call(
        turn_kernel,
        in_specs=[RESIDENT] * 3,
        out_specs=[RESIDENT] * 4,
        out_shape=[
            pltpu.VMEM(partner.shape, bf16),
            pltpu.VMEM(partner.shape, bf16),
            pltpu.VMEM(rows, bf16),
            pltpu.VMEM(rows, bf16),
        ],
        compiler_params=PARAMS,
        name="turn",
    )(*resident(normed, partner, other))


def outer_kernel(
    sum_ref,
    middle_ref,
    normed_ref,
    partner_ref,
    other_ref,
    left_ref,
    right_ref,
    gain_ref,
    taps_ref,
    up_ref,
    down_ref,
    send_ref,
    padded_s,
    after_s,
    taps_s,
    shift_s,
    down_s,
    piece_s,
):
    step = pl.program_id(0)
    height, width, _ = normed_ref.shape
    rows = WS
    repeats = height // WS

    @pl.when(step == 0)
    def _():
        even = lax.axis_index("row") % 2 == 0
        for r in range(HALO):
            partner = partner_ref[r].astype(f32)
            other = other_ref[r].astype(f32)
            padded_s[r] = jnp.where(even, other, partner).astype(bf16)
            padded_s[height + HALO + r] = jnp.where(even, partner, other).astype(bf16)

        def body(r, carry):
            padded_s[r + HALO] = ring(normed_ref[r], right_ref[r], left_ref[r])
            return carry

        lax.fori_loop(0, WS + HALO, body, 0)
        lax.fori_loop(height - WS - HALO, height, body, 0)
        prepare_finish(0, taps_ref, down_ref, taps_s, down_s)

    def row(j, carry):
        part, q = j // rows, j % rows
        r = part * (height - WS) + step * rows + q
        total = sum_ref[r] + convolve_row(padded_s, taps_s, shift_s, r, width)
        after_s[pl.ds(pl.multiple_of(j * width, width), width), :] = total
        return carry

    lax.fori_loop(0, 2 * rows, row, 0)
    outcome = feed_forward(after_s[...], gain_ref[2, 0:1, :], up_ref[0], down_s[...]).astype(f32)
    for m in range(repeats):
        for q in range(rows):
            if m in (0, repeats - 1):
                start = ((m > 0) * rows + q) * width
                line = outcome[start : start + width]
            else:
                line = middle_ref[(m - 1) * WS + step * rows + q].astype(f32)
            for n in range(width // SEGMENT):
                value = line[n * SEGMENT : (n + 1) * SEGMENT]
                place = pl.ds((q * SEGMENT + m * 4 + n) * PIECE_STRIDE, SEGMENT)
                piece_s[0, place, :] = value[:, 0:LANES]
                piece_s[1, place, 0 : D - LANES] = value[:, LANES:D]
    for q in range(rows):
        for c in range(SEGMENT):
            place = pl.ds(q * SEGMENT * PIECE_STRIDE + c, SEGMENT, stride=PIECE_STRIDE)
            upper = piece_s[1, place, :]
            send_ref[(step * rows + q) * SEGMENT + c] = jnp.concatenate(
                [piece_s[0, place, :], join_halves(upper[0:8], upper[8:16])], axis=0
            ).astype(bf16)


def outer_finish(
    after, middle, normed, top, bottom, left, right, gains, taps, up_weight, down_weight, group
):
    height, width = normed.shape[:2]
    rows = WS
    return pl.pallas_call(
        outer_kernel,
        grid=(WS // rows,),
        in_specs=[RESIDENT] * 11,
        out_specs=RESIDENT,
        out_shape=pltpu.VMEM((group, PIECE_ROWS, LANES), bf16),
        scratch_shapes=[
            pltpu.VMEM((height + 2 * HALO, RING, D), bf16),
            pltpu.VMEM((2 * rows * width, D), f32),
            pltpu.VMEM((KS * KS, 16, D), bf16),
            pltpu.VMEM((KS, 2, SEGMENT + RING, LANES), f32),
            pltpu.VMEM((HID, D), bf16),
            pltpu.VMEM((2, rows * SEGMENT * PIECE_STRIDE, LANES), f32),
        ],
        compiler_params=PARAMS,
        cost_estimate=work(8e9),
        name="outer_finish",
    )(
        *resident(
            after,
            middle,
            normed,
            top,
            bottom,
            left,
            right,
            gains,
            taps,
            up_weight,
            down_weight,
        )
    )


def second_kernel(
    back_ref,
    gain_ref,
    taps_ref,
    up_ref,
    down_ref,
    out_ref,
    padded_s,
    sum_s,
    after_s,
    taps_s,
    shift_s,
    down_s,
    piece_s,
):
    step = pl.program_id(0)
    rows, width, _ = out_ref.shape
    height = sum_s.shape[0]
    repeats = height // WS

    @pl.when(step == 0)
    def _():
        prepare_finish(1, taps_ref, down_ref, taps_s, down_s)

        def line(n):
            pieces = []
            for m in range(width // SEGMENT + 1):
                if n < 4 and m < 4:
                    low, high, half = 4 * n + m, 24 + (4 * n + m) % 8, (4 * n + m) // 8
                elif m < 4:
                    low, high, half = 16 + m, 32 + m, 0
                elif n < 4:
                    low, high, half = 20 + n, 32 + n, 1
                else:
                    low, high, half = 36, 37, 0
                at = lambda k: piece_s[pl.ds(k, SEGMENT, stride=RETURN_STRIDE), :]
                upper = at(high)
                if half:
                    upper = pltpu.roll(upper, D - LANES, 1)
                pieces.append(jnp.concatenate([at(low), upper], axis=1)[:, 0:D])
            return jnp.concatenate(pieces, axis=0)

        def body(r, carry):
            for c in range(SEGMENT):
                piece_s[c * RETURN_STRIDE : c * RETURN_STRIDE + RETURN_ROWS, :] = back_ref[
                    r * SEGMENT + c
                ].astype(f32)
            lines = [line(n) for n in range(repeats + 1)]
            normed = layer_norm(jnp.concatenate(lines, axis=0), gain_ref[1, 1:2, :]).astype(bf16)
            for n in range(repeats):
                sum_s[r + WS * n] = lines[n][0:width]
                padded_s[HALO + r + WS * n] = normed[n * RING : (n + 1) * RING]
            spare = height + 2 * HALO
            target = jnp.where(
                r < HALO, HALO + height + r, jnp.where(r >= WS - HALO, HALO + r - WS, spare)
            )
            padded_s[target] = normed[repeats * RING :]
            return carry

        lax.fori_loop(0, WS, body, 0)

    def row(j, carry):
        r = step * rows + j
        total = sum_s[r] + convolve_row(padded_s, taps_s, shift_s, r, width)
        after_s[pl.ds(pl.multiple_of(j * width, width), width), :] = total
        return carry

    lax.fori_loop(0, rows, row, 0)
    outcome = feed_forward(after_s[...], gain_ref[2, 1:2, :], up_ref[1], down_s[...])
    out_ref[...] = outcome.reshape(rows, width, D)


def second_finish(back, shape, gains, taps, up_weight, down_weight):
    height, width = shape[:2]
    return pl.pallas_call(
        second_kernel,
        grid=(height // (2 * WS),),
        in_specs=[RESIDENT] * 5,
        out_specs=pl.BlockSpec((2 * WS, width, D), lambda i: (i, 0, 0)),
        out_shape=jax.ShapeDtypeStruct(shape, bf16),
        scratch_shapes=[
            pltpu.VMEM((height + 2 * HALO + 1, RING, D), bf16),
            pltpu.VMEM((height, width, D), f32),
            pltpu.VMEM((2 * WS * width, D), f32),
            pltpu.VMEM((KS * KS, 16, D), bf16),
            pltpu.VMEM((KS, 2, SEGMENT + RING, LANES), f32),
            pltpu.VMEM((HID, D), bf16),
            pltpu.VMEM((SEGMENT * RETURN_STRIDE, LANES), f32),
        ],
        compiler_params=PARAMS,
        cost_estimate=work(1e10),
        name="second_finish",
    )(*resident(back, gains, taps, up_weight, down_weight))


def swap(facing, behind, axes):
    count = lax.axis_size(axes)

    def pairs(start):
        return [pair for i in range(start, count - 1, 2) for pair in ((i, i + 1), (i + 1, i))]

    return lax.ppermute(facing, axes, pairs(0)), lax.ppermute(behind, axes, pairs(1))


def on_device(
    tokens, norm_gain, qkv_weight, proj_weight, bias_table, conv_weight, up_weight, down_weight
):
    members = ("row", "block", "core")
    columns = ("block", "core")
    gains = norm_gain.transpose(1, 0, 2)
    table = bias_table.transpose(1, 0, 2)
    taps = conv_weight.transpose(1, 0, 2)
    down_weight = down_weight.transpose(0, 2, 1)
    *edges, facing, behind, bias, padded = edge_attention(tokens, gains, qkv_weight, proj_weight, table)
    partner, other = swap(facing, behind, columns)
    after, normed = inner_attention(tokens, gains, padded, proj_weight, bias, edges)
    left, right, facing, behind = turn(normed, partner, other)
    partner, other = swap(facing, behind, "row")
    middle = middle_finish(after, normed, left, right, gains, taps, up_weight, down_weight)
    outgoing = outer_finish(
        after,
        middle,
        normed,
        partner,
        other,
        left,
        right,
        gains,
        taps,
        up_weight,
        down_weight,
        lax.axis_size(members),
    )
    got = lax.all_to_all(outgoing, members, 0, 0, tiled=True)
    branch = shuffled_attention(got, gains, qkv_weight, proj_weight, table)
    back = lax.all_to_all(branch, members, 0, 0, tiled=True)
    return second_finish(back, tokens.shape, gains, taps, up_weight, down_weight)


def solution(mesh):
    split = Mesh(
        mesh.devices.reshape(mesh.shape["row"], mesh.shape["col"] // 2, 2), ("row", "block", "core")
    )
    spec = P("row", ("block", "core"), None)
    return jax.shard_map(
        on_device, mesh=split, in_specs=(spec,) + (P(),) * 7, out_specs=spec, check_vma=False
    )
```

```python
import functools
import jax
import jax.numpy as jnp
from jax import lax
from jax.experimental import pallas as pl
from jax.experimental.pallas import tpu as pltpu
from jax.sharding import Mesh, PartitionSpec as P

D = 192
HEADS = 6
HID = 768
WS = 8
KS = 7
HEAD = 32
AREA = WS * WS
PAD = 256
LANES = 128
HALO = KS // 2
TOGETHER = 32
WINDOW_ROWS = AREA + 4
PIECE_ROWS = 24
PIECE_STRIDE = PIECE_ROWS + 4
RETURN_ROWS = 40
RETURN_STRIDE = RETURN_ROWS + 4
RING = 80
SEGMENT = 16
EPSILON = 1e-05

f32 = jnp.float32
bf16 = jnp.bfloat16


def layer_norm(values, gain):
    centre = jnp.mean(values, axis=-1, keepdims=True)
    centred = values - centre
    spread = jnp.mean(centred * centred, axis=-1, keepdims=True)
    return centred * lax.rsqrt(spread + EPSILON) * gain


def mxu(a, b):
    return jnp.dot(a, b, preferred_element_type=f32)


def prepare_attention(layer, table_ref, qkv_ref, bias_s, rows_s, qkv_s):
    table = table_ref[:, layer, :]
    high = table.astype(bf16)
    rest = table - high.astype(f32)
    middle = rest.astype(bf16)
    low = (rest - middle.astype(f32)).astype(bf16)
    entries = (2 * WS - 1) ** 2
    lane = lax.broadcasted_iota(jnp.int32, (entries, WS * LANES), 1)
    entry = lax.broadcasted_iota(jnp.int32, (entries, WS * LANES), 0)
    target = (
        (2 * WS - 2 - ((lane & (LANES - 1)) >> 3)) * (2 * WS - 1)
        + (lane >> 7)
        - (lane & 7)
        + WS
        - 1
    )
    chosen = jnp.where(entry == target, 1.0, 0.0).astype(bf16)
    spread = mxu(high, chosen) + mxu(middle, chosen) + mxu(low, chosen)
    for place in range(WS):
        rows_s[place, 0:HEADS, :] = spread[:, place * LANES : (place + 1) * LANES]
    first = lax.broadcasted_iota(jnp.int32, (WS, LANES), 1) < AREA
    for group in range(HEADS // 2):
        left = rows_s[:, 2 * group, :]
        right = rows_s[:, 2 * group + 1, :]
        for row in range(WS):
            shift = LANES - (WS - 1 - row) * WS
            piece = jnp.where(
                first,
                pltpu.roll(left, shift % LANES, 1),
                pltpu.roll(right, (shift + AREA) % LANES, 1),
            )
            bias_s[group * AREA + row * WS : group * AREA + (row + 1) * WS, :] = piece
    weights = qkv_ref[layer].astype(f32)
    gap = jnp.zeros((D, PAD - D), f32)
    qkv_s[...] = jnp.concatenate(
        [
            weights[:, 0:D],
            gap,
            weights[:, D : 2 * D],
            gap,
            weights[:, 2 * D : 3 * D],
            gap,
        ],
        axis=1,
    ).astype(bf16)


def attention_masks():
    lane = lax.broadcasted_iota(jnp.int32, (1, PAD), 1)
    groups = [
        jnp.where((lane >> 6) == g, 1.0, 0.0).astype(bf16) for g in range(HEADS // 2)
    ]
    parities = [
        jnp.where(((lane >> 5) & 1) == h, 1.0, 0.0).astype(bf16) for h in range(2)
    ]
    rows = lax.broadcasted_iota(jnp.int32, (LANES, LANES), 0) >> 6
    cols = lax.broadcasted_iota(jnp.int32, (LANES, LANES), 1) >> 6
    summing = jnp.where(rows == cols, 1.0, 0.0).astype(bf16)
    return groups, parities, summing


def attend(projected, bias, masks):
    groups, parities, summing = masks
    count = projected.shape[0] // AREA
    window = lambda n, t: projected[n * AREA : (n + 1) * AREA, t * PAD : (t + 1) * PAD]
    spread = lambda x, ms: jnp.concatenate([x * m for m in ms], axis=0)
    scores = [
        lax.dot_general(
            spread(window(n, 0), groups),
            spread(window(n, 1), parities),
            (((1,), (1,)), ((), ())),
            preferred_element_type=f32,
        )
        for n in range(count)
    ]
    weights = [jnp.exp(x * HEAD ** (-0.5) + bias) for x in scores]
    totals = [mxu(x.astype(bf16), summing) for x in weights]
    weights = [(x / y).astype(bf16) for x, y in zip(weights, totals)]
    mixed = [mxu(x, spread(window(n, 2), parities)) for n, x in enumerate(weights)]
    lane = lax.broadcasted_iota(jnp.int32, (AREA, PAD), 1) >> 6
    return [
        jnp.where(
            lane == 0, x[0:AREA], jnp.where(lane == 1, x[AREA : 2 * AREA], x[2 * AREA :])
        )[:, 0:D].astype(bf16)
        for x in mixed
    ]


def attention(current, gain, qkv, proj, bias, masks, together):
    normed = layer_norm(current, gain).astype(bf16)
    projected = mxu(normed, qkv).astype(bf16)
    outs = []
    for start in range(0, current.shape[0], together * AREA):
        outs += attend(projected[start : start + together * AREA], bias, masks)
    return current + mxu(jnp.concatenate(outs, axis=0), proj)


def edge_kernel(
    first_ref,
    last_ref,
    gain_ref,
    qkv_ref,
    proj_ref,
    table_ref,
    sum_left_ref,
    sum_right_ref,
    left_out_ref,
    right_out_ref,
    facing_ref,
    behind_ref,
    bias_ref,
    pad_ref,
    rows_s,
):
    prepare_attention(0, table_ref, qkv_ref, bias_ref, rows_s, pad_ref)
    sides = [side[...].astype(f32).reshape(-1, D) for side in (first_ref, last_ref)]
    after = attention(
        jnp.concatenate(sides, axis=0),
        gain_ref[0, 0:1, :],
        pad_ref[...],
        proj_ref[0],
        bias_ref[...],
        attention_masks(),
        TOGETHER,
    )
    normed = layer_norm(after, gain_ref[1, 0:1, :])
    half = after.shape[0] // 2
    shape = sum_left_ref.shape
    sum_left_ref[...] = after[:half].reshape(shape)
    sum_right_ref[...] = after[half:].reshape(shape)
    left = normed[:half].reshape(shape)
    right = normed[half:].reshape(shape)
    left_out_ref[...] = left.astype(bf16)
    right_out_ref[...] = right.astype(bf16)
    even = lax.axis_index("core") == 0
    facing_ref[...] = jnp.where(even, right, left).astype(bf16)
    behind_ref[...] = jnp.where(even, left, right).astype(bf16)


def inner_kernel(
    x_ref,
    gain_ref,
    pad_ref,
    proj_ref,
    bias_ref,
    sum_left_ref,
    sum_right_ref,
    left_ref,
    right_ref,
    sum_ref,
    normed_ref,
):
    high = 4 * WS
    rows = pl.ds(pl.program_id(0) * high, high)
    inner = range(1, x_ref.shape[1] // WS - 1)
    grid = x_ref[rows].astype(f32)
    places = [(i, j) for i in range(high // WS) for j in inner]
    current = jnp.concatenate(
        [
            grid[i * WS : (i + 1) * WS, j * WS : (j + 1) * WS, :].reshape(AREA, D)
            for i, j in places
        ],
        axis=0,
    )
    after = attention(
        current,
        gain_ref[0, 0:1, :],
        pad_ref[...],
        proj_ref[0],
        bias_ref[...],
        attention_masks(),
        len(places),
    )
    normed = layer_norm(after, gain_ref[1, 0:1, :])

    def spatial(first, value, last):
        pieces = [
            value[n * AREA : (n + 1) * AREA].reshape(WS, WS, D) for n in range(len(places))
        ]
        lines = [
            jnp.concatenate(pieces[i * len(inner) : (i + 1) * len(inner)], axis=1)
            for i in range(high // WS)
        ]
        return jnp.concatenate([first, jnp.concatenate(lines, axis=0), last], axis=1)

    sum_ref[rows] = spatial(sum_left_ref[rows], after, sum_right_ref[rows])
    normed_ref[rows] = spatial(
        left_ref[rows].astype(f32), normed, right_ref[rows].astype(f32)
    ).astype(bf16)


def attention_scratch():
    return [
        pltpu.VMEM((HEADS // 2 * AREA, LANES), f32),
        pltpu.VMEM((WS, WS, LANES), f32),
        pltpu.VMEM((D, 3 * PAD), bf16),
    ]


RESIDENT = pl.BlockSpec(memory_space=pltpu.VMEM)
PARAMS = pltpu.CompilerParams(vmem_limit_bytes=24 << 20)


def resident(*arrays):
    return [pltpu.with_memory_space_constraint(a, pltpu.VMEM) for a in arrays]


def work(flops):
    return pl.CostEstimate(flops=int(flops), transcendentals=0, bytes_accessed=1 << 20)


def edge_attention(tokens, gains, qkv_weight, proj_weight, table):
    side = (tokens.shape[0], WS, D)
    last = tokens.shape[1] // WS - 1
    full = lambda a: pl.BlockSpec(a.shape, lambda i: (0,) * a.ndim)
    return pl.pallas_call(
        edge_kernel,
        grid=(1,),
        in_specs=[
            pl.BlockSpec(side, lambda i: (0, 0, 0)),
            pl.BlockSpec(side, lambda i: (0, last, 0)),
            full(gains),
            full(qkv_weight),
            full(proj_weight),
            full(table),
        ],
        out_specs=[RESIDENT] * 8,
        out_shape=[
            pltpu.VMEM(side, f32),
            pltpu.VMEM(side, f32),
            pltpu.VMEM(side, bf16),
            pltpu.VMEM(side, bf16),
            pltpu.VMEM(side, bf16),
            pltpu.VMEM(side, bf16),
            pltpu.VMEM((HEADS // 2 * AREA, LANES), f32),
            pltpu.VMEM((D, 3 * PAD), bf16),
        ],
        scratch_shapes=[pltpu.VMEM((WS, WS, LANES), f32)],
        compiler_params=PARAMS,
        cost_estimate=work(5e8),
        name="edge_attention",
    )(
        *[
            pltpu.with_memory_space_constraint(a, pltpu.HBM)
            for a in (tokens, tokens, gains, qkv_weight, proj_weight, table)
        ]
    )


def inner_attention(tokens, gains, padded, proj_weight, bias, edges):
    return pl.pallas_call(
        inner_kernel,
        grid=(tokens.shape[0] // (4 * WS),),
        in_specs=[RESIDENT] * 9,
        out_specs=[RESIDENT] * 2,
        out_shape=[pltpu.VMEM(tokens.shape, f32), pltpu.VMEM(tokens.shape, bf16)],
        compiler_params=PARAMS,
        cost_estimate=work(8e9),
        name="inner_attention",
    )(*resident(tokens, gains, padded, proj_weight, bias, *edges))


def low_half(value):
    lane = lax.broadcasted_iota(jnp.int32, value.shape, value.ndim - 1)
    return jnp.where(lane < D - LANES, value, 0.0)


def join_halves(first, second):
    lane = lax.broadcasted_iota(jnp.int32, first.shape, 1)
    return jnp.where(lane < D - LANES, first, pltpu.roll(second, D - LANES, 1))


def shuffled_kernel(
    got_ref, gain_ref, qkv_ref, proj_ref, table_ref, out_ref, bias_s, rows_s, qkv_s, window_s, piece_s
):
    prepare_attention(1, table_ref, qkv_ref, bias_s, rows_s, qkv_s)
    blocks = WS * 2

    def gather(a, carry):
        for c in range(blocks):
            piece = got_ref[a * blocks + c].astype(f32)
            upper = piece[SEGMENT:]
            upper = jnp.concatenate(
                [low_half(upper), low_half(pltpu.roll(upper, D - LANES, 1))], axis=0
            )
            place = pl.ds(
                (c % 2) * SEGMENT * WINDOW_ROWS + a * WS + c // 2, SEGMENT, stride=WINDOW_ROWS
            )
            window_s[0, place, :] = piece[:SEGMENT]
            window_s[1, place, :] = upper
        return carry

    lax.fori_loop(0, WS, gather, 0, unroll=2)
    masks = attention_masks()

    def windows(c, carry):
        starts = [(c * TOGETHER + n) * WINDOW_ROWS for n in range(TOGETHER)]
        current = jnp.concatenate(
            [
                jnp.concatenate(
                    [window_s[t, pl.ds(start, AREA), :] for start in starts], axis=0
                )
                for t in range(2)
            ],
            axis=1,
        )[:, 0:D]
        after = attention(
            current, gain_ref[0, 1:2, :], qkv_s[...], proj_ref[1], bias_s[...], masks, TOGETHER
        )
        for n, start in enumerate(starts):
            window_s[0, pl.ds(start, AREA), :] = after[n * AREA : (n + 1) * AREA, 0:LANES]
            window_s[1, pl.ds(start, AREA), 0 : D - LANES] = after[
                n * AREA : (n + 1) * AREA, LANES:D
            ]
        return carry

    lax.fori_loop(0, 2 * SEGMENT // TOGETHER, windows, 0)

    below = lax.axis_index("row") < WS // 2
    beside = lax.axis_index("block") < WS // 2
    row_step = jnp.where(below, 1, -1)
    row_window = jnp.where(below, 0, 3)
    col_window = jnp.where(beside, 0, 3)

    def scatter(a, carry):
        other_a = a + row_step
        row_keep = jnp.where((other_a >= 0) & (other_a < WS), 1.0, 0.0).astype(f32)
        other_a = jnp.clip(other_a, 0, WS - 1)
        for c in range(blocks):
            b, core = c // 2, c % 2
            other_b = b + (jnp.where(beside, 1, 0) if core else jnp.where(beside, 0, -1))
            col_keep = jnp.where((other_b >= 0) & (other_b < WS), 1.0, 0.0).astype(f32)
            other_b = jnp.clip(other_b, 0, WS - 1)
            base = core * SEGMENT
            other = (1 - core) * SEGMENT
            main = pl.ds(base * WINDOW_ROWS + a * WS + b, SEGMENT, stride=WINDOW_ROWS)
            row = pl.ds(
                (base + row_window * 4) * WINDOW_ROWS + other_a * WS + b, 4, stride=WINDOW_ROWS
            )
            col = pl.ds(
                (other + col_window) * WINDOW_ROWS + a * WS + other_b, 4, stride=4 * WINDOW_ROWS
            )
            corner = pl.ds(
                (other + row_window * 4 + col_window) * WINDOW_ROWS + other_a * WS + other_b, 1
            )
            keep = row_keep * col_keep
            piece_s[0:16] = window_s[0, main, :]
            piece_s[16:20] = window_s[0, row, :] * row_keep
            piece_s[20:24] = window_s[0, col, :] * col_keep
            upper = window_s[1, main, :]
            piece_s[24:32] = join_halves(upper[0:8], upper[8:16])
            piece_s[32:36] = join_halves(
                window_s[1, row, :] * row_keep, window_s[1, col, :] * col_keep
            )
            piece_s[36:37] = window_s[0, corner, :] * keep
            piece_s[37:38] = window_s[1, corner, :] * keep
            out_ref[a * blocks + c] = piece_s[...].astype(bf16)
        return carry

    piece_s[...] = jnp.zeros_like(piece_s)
    lax.fori_loop(0, WS, scatter, 0, unroll=2)


def shuffled_attention(got, gains, qkv_weight, proj_weight, table):
    shape = (got.shape[0], RETURN_ROWS, LANES)
    return pl.pallas_call(
        shuffled_kernel,
        in_specs=[RESIDENT] * 5,
        out_specs=RESIDENT,
        out_shape=pltpu.VMEM(shape, bf16),
        scratch_shapes=attention_scratch()
        + [
            pltpu.VMEM((2, 2 * SEGMENT * WINDOW_ROWS, LANES), f32),
            pltpu.VMEM((RETURN_ROWS, LANES), f32),
        ],
        compiler_params=PARAMS,
        cost_estimate=work(1e10),
        name="shuffled_attention",
    )(*resident(got, gains, qkv_weight, proj_weight, table))


def prepare_finish(layer, taps_ref, down_ref, taps_s, down_s):
    for t in range(KS * KS):
        taps_s[t] = jnp.broadcast_to(
            taps_ref[t, layer : layer + 1, :], (16, D)
        ).astype(bf16)
    down_s[...] = down_ref[layer].T


def convolve_row(padded_s, taps_s, shift_s, row, width):
    total = None
    for v in range(KS):
        part = None
        for u in range(KS):
            x = padded_s[row + u].reshape(-1, 16, D)
            term = x * taps_s[u * KS + v][None]
            part = term if part is None else part + term
        part = part.reshape(-1, D).astype(f32)
        if v == HALO:
            part = part[:width]
        else:
            pieces = []
            for n, value in enumerate((part[:, :LANES], part[:, LANES:])):
                lanes = slice(0, value.shape[1])
                shift_s[v, n, SEGMENT : SEGMENT + RING, lanes] = value
                shift_s[v, n, WS:SEGMENT, lanes] = value[RING - WS :]
                start = SEGMENT + v - HALO
                pieces.append(shift_s[v, n, start : start + width, :])
            part = jnp.concatenate(pieces, axis=1)[:, 0:D]
        total = part if total is None else total + part
    return total


def feed_forward(after, gain, up, down):
    normed = layer_norm(after, gain).astype(bf16)
    raised = mxu(normed, up)
    hidden = (0.5 * raised * (1.0 + lax.erf(raised * 0.5**0.5))).astype(bf16)
    return (after + mxu(hidden, down)).astype(bf16)


def ring(middle, right, left):
    return jnp.concatenate(
        [middle.astype(f32), right.astype(f32), left.astype(f32)], axis=0
    ).astype(bf16)


def middle_kernel(
    sum_ref,
    normed_ref,
    left_ref,
    right_ref,
    gain_ref,
    taps_ref,
    up_ref,
    down_ref,
    out_ref,
    padded_s,
    after_s,
    taps_s,
    shift_s,
    down_s,
):
    step = pl.program_id(0)
    rows = 2 * WS
    width = sum_ref.shape[1]
    first = WS - HALO

    @pl.when(step == 0)
    def _():
        def body(r, carry):
            padded_s[r] = ring(normed_ref[first + r], right_ref[first + r], left_ref[first + r])
            return carry

        lax.fori_loop(0, padded_s.shape[0], body, 0)
        prepare_finish(0, taps_ref, down_ref, taps_s, down_s)

    def row(j, carry):
        total = sum_ref[WS + step * rows + j] + convolve_row(
            padded_s, taps_s, shift_s, step * rows + j, width
        )
        after_s[pl.ds(pl.multiple_of(j * width, width), width), :] = total
        return carry

    lax.fori_loop(0, rows, row, 0)
    outcome = feed_forward(after_s[...], gain_ref[2, 0:1, :], up_ref[0], down_s[...])
    out_ref[pl.ds(step * rows, rows)] = outcome.reshape(rows, width, D)


def middle_finish(after, normed, left, right, gains, taps, up_weight, down_weight):
    height, width = normed.shape[:2]
    inner = height - 2 * WS
    return pl.pallas_call(
        middle_kernel,
        grid=(inner // (2 * WS),),
        in_specs=[RESIDENT] * 8,
        out_specs=RESIDENT,
        out_shape=pltpu.VMEM((inner, width, D), bf16),
        scratch_shapes=[
            pltpu.VMEM((inner + 2 * HALO, RING, D), bf16),
            pltpu.VMEM((2 * WS * width, D), f32),
            pltpu.VMEM((KS * KS, 16, D), bf16),
            pltpu.VMEM((KS, 2, SEGMENT + RING, LANES), f32),
            pltpu.VMEM((HID, D), bf16),
        ],
        compiler_params=PARAMS,
        cost_estimate=work(8e9),
        name="middle_finish",
    )(*resident(after, normed, left, right, gains, taps, up_weight, down_weight))


def turn_kernel(
    normed_ref, partner_ref, other_ref, left_ref, right_ref, facing_ref, behind_ref
):
    height = normed_ref.shape[0]
    even = lax.axis_index("core") == 0
    partner = partner_ref[...].astype(f32)
    other = other_ref[...].astype(f32)
    left_ref[...] = jnp.where(even, other, partner).astype(bf16)
    right_ref[...] = jnp.where(even, partner, other).astype(bf16)
    even = lax.axis_index("row") % 2 == 0
    for r in range(HALO):
        first = ring(normed_ref[r], right_ref[r], left_ref[r]).astype(f32)
        n = height - HALO + r
        last = ring(normed_ref[n], right_ref[n], left_ref[n]).astype(f32)
        facing_ref[r] = jnp.where(even, last, first).astype(bf16)
        behind_ref[r] = jnp.where(even, first, last).astype(bf16)


def turn(normed, partner, other):
    rows = (HALO, RING, D)
    return pl.pallas_call(
        turn_kernel,
        in_specs=[RESIDENT] * 3,
        out_specs=[RESIDENT] * 4,
        out_shape=[
            pltpu.VMEM(partner.shape, bf16),
            pltpu.VMEM(partner.shape, bf16),
            pltpu.VMEM(rows, bf16),
            pltpu.VMEM(rows, bf16),
        ],
        compiler_params=PARAMS,
        name="turn",
    )(*resident(normed, partner, other))


def outer_kernel(
    sum_ref,
    middle_ref,
    normed_ref,
    partner_ref,
    other_ref,
    left_ref,
    right_ref,
    gain_ref,
    taps_ref,
    up_ref,
    down_ref,
    send_ref,
    padded_s,
    after_s,
    taps_s,
    shift_s,
    down_s,
    piece_s,
):
    step = pl.program_id(0)
    height, width, _ = normed_ref.shape
    rows = WS
    repeats = height // WS

    @pl.when(step == 0)
    def _():
        even = lax.axis_index("row") % 2 == 0
        for r in range(HALO):
            partner = partner_ref[r].astype(f32)
            other = other_ref[r].astype(f32)
            padded_s[r] = jnp.where(even, other, partner).astype(bf16)
            padded_s[height + HALO + r] = jnp.where(even, partner, other).astype(bf16)

        def body(r, carry):
            padded_s[r + HALO] = ring(normed_ref[r], right_ref[r], left_ref[r])
            return carry

        lax.fori_loop(0, WS + HALO, body, 0)
        lax.fori_loop(height - WS - HALO, height, body, 0)
        prepare_finish(0, taps_ref, down_ref, taps_s, down_s)

    def row(j, carry):
        part, q = j // rows, j % rows
        r = part * (height - WS) + step * rows + q
        total = sum_ref[r] + convolve_row(padded_s, taps_s, shift_s, r, width)
        after_s[pl.ds(pl.multiple_of(j * width, width), width), :] = total
        return carry

    lax.fori_loop(0, 2 * rows, row, 0)
    outcome = feed_forward(after_s[...], gain_ref[2, 0:1, :], up_ref[0], down_s[...]).astype(f32)
    for m in range(repeats):
        for q in range(rows):
            if m in (0, repeats - 1):
                start = ((m > 0) * rows + q) * width
                line = outcome[start : start + width]
            else:
                line = middle_ref[(m - 1) * WS + step * rows + q].astype(f32)
            for n in range(width // SEGMENT):
                value = line[n * SEGMENT : (n + 1) * SEGMENT]
                place = pl.ds((q * SEGMENT + m * 4 + n) * PIECE_STRIDE, SEGMENT)
                piece_s[0, place, :] = value[:, 0:LANES]
                piece_s[1, place, 0 : D - LANES] = value[:, LANES:D]
    for q in range(rows):
        for c in range(SEGMENT):
            place = pl.ds(q * SEGMENT * PIECE_STRIDE + c, SEGMENT, stride=PIECE_STRIDE)
            upper = piece_s[1, place, :]
            send_ref[(step * rows + q) * SEGMENT + c] = jnp.concatenate(
                [piece_s[0, place, :], join_halves(upper[0:8], upper[8:16])], axis=0
            ).astype(bf16)


def outer_finish(
    after, middle, normed, top, bottom, left, right, gains, taps, up_weight, down_weight, group
):
    height, width = normed.shape[:2]
    rows = WS
    return pl.pallas_call(
        outer_kernel,
        grid=(WS // rows,),
        in_specs=[RESIDENT] * 11,
        out_specs=RESIDENT,
        out_shape=pltpu.VMEM((group, PIECE_ROWS, LANES), bf16),
        scratch_shapes=[
            pltpu.VMEM((height + 2 * HALO, RING, D), bf16),
            pltpu.VMEM((2 * rows * width, D), f32),
            pltpu.VMEM((KS * KS, 16, D), bf16),
            pltpu.VMEM((KS, 2, SEGMENT + RING, LANES), f32),
            pltpu.VMEM((HID, D), bf16),
            pltpu.VMEM((2, rows * SEGMENT * PIECE_STRIDE, LANES), f32),
        ],
        compiler_params=PARAMS,
        cost_estimate=work(8e9),
        name="outer_finish",
    )(
        *resident(
            after,
            middle,
            normed,
            top,
            bottom,
            left,
            right,
            gains,
            taps,
            up_weight,
            down_weight,
        )
    )


def second_kernel(
    back_ref,
    gain_ref,
    taps_ref,
    up_ref,
    down_ref,
    out_ref,
    padded_s,
    sum_s,
    after_s,
    taps_s,
    shift_s,
    down_s,
    piece_s,
):
    step = pl.program_id(0)
    rows, width, _ = out_ref.shape
    height = sum_s.shape[0]
    repeats = height // WS

    @pl.when(step == 0)
    def _():
        prepare_finish(1, taps_ref, down_ref, taps_s, down_s)

        def line(n):
            pieces = []
            for m in range(width // SEGMENT + 1):
                if n < 4 and m < 4:
                    low, high, half = 4 * n + m, 24 + (4 * n + m) % 8, (4 * n + m) // 8
                elif m < 4:
                    low, high, half = 16 + m, 32 + m, 0
                elif n < 4:
                    low, high, half = 20 + n, 32 + n, 1
                else:
                    low, high, half = 36, 37, 0
                at = lambda k: piece_s[pl.ds(k, SEGMENT, stride=RETURN_STRIDE), :]
                upper = at(high)
                if half:
                    upper = pltpu.roll(upper, D - LANES, 1)
                pieces.append(jnp.concatenate([at(low), upper], axis=1)[:, 0:D])
            return jnp.concatenate(pieces, axis=0)

        def body(r, carry):
            for c in range(SEGMENT):
                piece_s[c * RETURN_STRIDE : c * RETURN_STRIDE + RETURN_ROWS, :] = back_ref[
                    r * SEGMENT + c
                ].astype(f32)
            lines = [line(n) for n in range(repeats + 1)]
            normed = layer_norm(jnp.concatenate(lines, axis=0), gain_ref[1, 1:2, :]).astype(bf16)
            for n in range(repeats):
                sum_s[r + WS * n] = lines[n][0:width]
                padded_s[HALO + r + WS * n] = normed[n * RING : (n + 1) * RING]
            spare = height + 2 * HALO
            target = jnp.where(
                r < HALO, HALO + height + r, jnp.where(r >= WS - HALO, HALO + r - WS, spare)
            )
            padded_s[target] = normed[repeats * RING :]
            return carry

        lax.fori_loop(0, WS, body, 0, unroll=2)

    def row(j, carry):
        r = step * rows + j
        total = sum_s[r] + convolve_row(padded_s, taps_s, shift_s, r, width)
        after_s[pl.ds(pl.multiple_of(j * width, width), width), :] = total
        return carry

    lax.fori_loop(0, rows, row, 0)
    outcome = feed_forward(after_s[...], gain_ref[2, 1:2, :], up_ref[1], down_s[...])
    out_ref[...] = outcome.reshape(rows, width, D)


def second_finish(back, shape, gains, taps, up_weight, down_weight):
    height, width = shape[:2]
    return pl.pallas_call(
        second_kernel,
        grid=(height // (2 * WS),),
        in_specs=[RESIDENT] * 5,
        out_specs=pl.BlockSpec((2 * WS, width, D), lambda i: (i, 0, 0)),
        out_shape=jax.ShapeDtypeStruct(shape, bf16),
        scratch_shapes=[
            pltpu.VMEM((height + 2 * HALO + 1, RING, D), bf16),
            pltpu.VMEM((height, width, D), f32),
            pltpu.VMEM((2 * WS * width, D), f32),
            pltpu.VMEM((KS * KS, 16, D), bf16),
            pltpu.VMEM((KS, 2, SEGMENT + RING, LANES), f32),
            pltpu.VMEM((HID, D), bf16),
            pltpu.VMEM((SEGMENT * RETURN_STRIDE, LANES), f32),
        ],
        compiler_params=PARAMS,
        cost_estimate=work(1e10),
        name="second_finish",
    )(*resident(back, gains, taps, up_weight, down_weight))


def swap(facing, behind, axes):
    count = lax.axis_size(axes)

    def pairs(start):
        return [pair for i in range(start, count - 1, 2) for pair in ((i, i + 1), (i + 1, i))]

    return lax.ppermute(facing, axes, pairs(0)), lax.ppermute(behind, axes, pairs(1))


def on_device(
    tokens, norm_gain, qkv_weight, proj_weight, bias_table, conv_weight, up_weight, down_weight
):
    members = ("row", "block", "core")
    columns = ("block", "core")
    gains = norm_gain.transpose(1, 0, 2)
    table = bias_table.transpose(1, 0, 2)
    taps = conv_weight.transpose(1, 0, 2)
    down_weight = down_weight.transpose(0, 2, 1)
    *edges, facing, behind, bias, padded = edge_attention(tokens, gains, qkv_weight, proj_weight, table)
    partner, other = swap(facing, behind, columns)
    after, normed = inner_attention(tokens, gains, padded, proj_weight, bias, edges)
    left, right, facing, behind = turn(normed, partner, other)
    partner, other = swap(facing, behind, "row")
    middle = middle_finish(after, normed, left, right, gains, taps, up_weight, down_weight)
    outgoing = outer_finish(
        after,
        middle,
        normed,
        partner,
        other,
        left,
        right,
        gains,
        taps,
        up_weight,
        down_weight,
        lax.axis_size(members),
    )
    got = lax.all_to_all(outgoing, members, 0, 0, tiled=True)
    branch = shuffled_attention(got, gains, qkv_weight, proj_weight, table)
    back = lax.all_to_all(branch, members, 0, 0, tiled=True)
    return second_finish(back, tokens.shape, gains, taps, up_weight, down_weight)


def solution(mesh):
    split = Mesh(
        mesh.devices.reshape(mesh.shape["row"], mesh.shape["col"] // 2, 2), ("row", "block", "core")
    )
    spec = P("row", ("block", "core"), None)
    return jax.shard_map(
        on_device, mesh=split, in_specs=(spec,) + (P(),) * 7, out_specs=spec, check_vma=False
    )
```

```python
import functools
import jax
import jax.numpy as jnp
from jax import lax
from jax.experimental import pallas as pl
from jax.experimental.pallas import tpu as pltpu
from jax.sharding import Mesh, PartitionSpec as P

D = 192
HEADS = 6
HID = 768
WS = 8
KS = 7
HEAD = 32
AREA = WS * WS
PAD = 256
LANES = 128
HALO = KS // 2
TOGETHER = 32
WINDOW_ROWS = AREA + 4
PIECE_ROWS = 24
PIECE_STRIDE = PIECE_ROWS + 4
RETURN_ROWS = 40
RETURN_STRIDE = RETURN_ROWS + 4
RING = 80
SEGMENT = 16
EPSILON = 1e-05

f32 = jnp.float32
bf16 = jnp.bfloat16


def layer_norm(values, gain):
    centre = jnp.mean(values, axis=-1, keepdims=True)
    centred = values - centre
    spread = jnp.mean(centred * centred, axis=-1, keepdims=True)
    return centred * lax.rsqrt(spread + EPSILON) * gain


def mxu(a, b):
    return jnp.dot(a, b, preferred_element_type=f32)


def prepare_attention(layer, table_ref, qkv_ref, bias_s, rows_s, qkv_s):
    table = table_ref[:, layer, :]
    high = table.astype(bf16)
    rest = table - high.astype(f32)
    middle = rest.astype(bf16)
    low = (rest - middle.astype(f32)).astype(bf16)
    entries = (2 * WS - 1) ** 2
    lane = lax.broadcasted_iota(jnp.int32, (entries, WS * LANES), 1)
    entry = lax.broadcasted_iota(jnp.int32, (entries, WS * LANES), 0)
    target = (
        (2 * WS - 2 - ((lane & (LANES - 1)) >> 3)) * (2 * WS - 1)
        + (lane >> 7)
        - (lane & 7)
        + WS
        - 1
    )
    chosen = jnp.where(entry == target, 1.0, 0.0).astype(bf16)
    spread = mxu(high, chosen) + mxu(middle, chosen) + mxu(low, chosen)
    for place in range(WS):
        rows_s[place, 0:HEADS, :] = spread[:, place * LANES : (place + 1) * LANES]
    first = lax.broadcasted_iota(jnp.int32, (WS, LANES), 1) < AREA
    for group in range(HEADS // 2):
        left = rows_s[:, 2 * group, :]
        right = rows_s[:, 2 * group + 1, :]
        for row in range(WS):
            shift = LANES - (WS - 1 - row) * WS
            piece = jnp.where(
                first,
                pltpu.roll(left, shift % LANES, 1),
                pltpu.roll(right, (shift + AREA) % LANES, 1),
            )
            bias_s[group * AREA + row * WS : group * AREA + (row + 1) * WS, :] = piece
    weights = qkv_ref[layer].astype(f32)
    gap = jnp.zeros((D, PAD - D), f32)
    qkv_s[...] = jnp.concatenate(
        [
            weights[:, 0:D],
            gap,
            weights[:, D : 2 * D],
            gap,
            weights[:, 2 * D : 3 * D],
            gap,
        ],
        axis=1,
    ).astype(bf16)


def attention_masks():
    lane = lax.broadcasted_iota(jnp.int32, (1, PAD), 1)
    groups = [
        jnp.where((lane >> 6) == g, 1.0, 0.0).astype(bf16) for g in range(HEADS // 2)
    ]
    parities = [
        jnp.where(((lane >> 5) & 1) == h, 1.0, 0.0).astype(bf16) for h in range(2)
    ]
    rows = lax.broadcasted_iota(jnp.int32, (LANES, LANES), 0) >> 6
    cols = lax.broadcasted_iota(jnp.int32, (LANES, LANES), 1) >> 6
    summing = jnp.where(rows == cols, 1.0, 0.0).astype(bf16)
    return groups, parities, summing


def attend(projected, bias, masks):
    groups, parities, summing = masks
    count = projected.shape[0] // AREA
    window = lambda n, t: projected[n * AREA : (n + 1) * AREA, t * PAD : (t + 1) * PAD]
    spread = lambda x, ms: jnp.concatenate([x * m for m in ms], axis=0)
    scores = [
        lax.dot_general(
            spread(window(n, 0), groups),
            spread(window(n, 1), parities),
            (((1,), (1,)), ((), ())),
            preferred_element_type=f32,
        )
        for n in range(count)
    ]
    weights = [jnp.exp(x * HEAD ** (-0.5) + bias) for x in scores]
    totals = [mxu(x.astype(bf16), summing) for x in weights]
    weights = [(x / y).astype(bf16) for x, y in zip(weights, totals)]
    mixed = [mxu(x, spread(window(n, 2), parities)) for n, x in enumerate(weights)]
    lane = lax.broadcasted_iota(jnp.int32, (AREA, PAD), 1) >> 6
    return [
        jnp.where(
            lane == 0, x[0:AREA], jnp.where(lane == 1, x[AREA : 2 * AREA], x[2 * AREA :])
        )[:, 0:D].astype(bf16)
        for x in mixed
    ]


def attention(current, gain, qkv, proj, bias, masks, together):
    normed = layer_norm(current, gain).astype(bf16)
    projected = mxu(normed, qkv).astype(bf16)
    outs = []
    for start in range(0, current.shape[0], together * AREA):
        outs += attend(projected[start : start + together * AREA], bias, masks)
    return current + mxu(jnp.concatenate(outs, axis=0), proj)


def edge_kernel(
    first_ref,
    last_ref,
    gain_ref,
    qkv_ref,
    proj_ref,
    table_ref,
    sum_left_ref,
    sum_right_ref,
    left_out_ref,
    right_out_ref,
    facing_ref,
    behind_ref,
    bias_ref,
    pad_ref,
    rows_s,
):
    prepare_attention(0, table_ref, qkv_ref, bias_ref, rows_s, pad_ref)
    sides = [side[...].astype(f32).reshape(-1, D) for side in (first_ref, last_ref)]
    after = attention(
        jnp.concatenate(sides, axis=0),
        gain_ref[0, 0:1, :],
        pad_ref[...],
        proj_ref[0],
        bias_ref[...],
        attention_masks(),
        TOGETHER,
    )
    normed = layer_norm(after, gain_ref[1, 0:1, :])
    half = after.shape[0] // 2
    shape = sum_left_ref.shape
    sum_left_ref[...] = after[:half].reshape(shape)
    sum_right_ref[...] = after[half:].reshape(shape)
    left = normed[:half].reshape(shape)
    right = normed[half:].reshape(shape)
    left_out_ref[...] = left.astype(bf16)
    right_out_ref[...] = right.astype(bf16)
    even = lax.axis_index("core") == 0
    facing_ref[...] = jnp.where(even, right, left).astype(bf16)
    behind_ref[...] = jnp.where(even, left, right).astype(bf16)


def inner_kernel(
    x_ref,
    gain_ref,
    pad_ref,
    proj_ref,
    bias_ref,
    sum_left_ref,
    sum_right_ref,
    left_ref,
    right_ref,
    sum_ref,
    normed_ref,
):
    high = 4 * WS
    rows = pl.ds(pl.program_id(0) * high, high)
    inner = range(1, x_ref.shape[1] // WS - 1)
    grid = x_ref[rows].astype(f32)
    places = [(i, j) for i in range(high // WS) for j in inner]
    current = jnp.concatenate(
        [
            grid[i * WS : (i + 1) * WS, j * WS : (j + 1) * WS, :].reshape(AREA, D)
            for i, j in places
        ],
        axis=0,
    )
    after = attention(
        current,
        gain_ref[0, 0:1, :],
        pad_ref[...],
        proj_ref[0],
        bias_ref[...],
        attention_masks(),
        len(places),
    )
    normed = layer_norm(after, gain_ref[1, 0:1, :])

    def spatial(first, value, last):
        pieces = [
            value[n * AREA : (n + 1) * AREA].reshape(WS, WS, D) for n in range(len(places))
        ]
        lines = [
            jnp.concatenate(pieces[i * len(inner) : (i + 1) * len(inner)], axis=1)
            for i in range(high // WS)
        ]
        return jnp.concatenate([first, jnp.concatenate(lines, axis=0), last], axis=1)

    sum_ref[rows] = spatial(sum_left_ref[rows], after, sum_right_ref[rows])
    normed_ref[rows] = spatial(
        left_ref[rows].astype(f32), normed, right_ref[rows].astype(f32)
    ).astype(bf16)


def attention_scratch():
    return [
        pltpu.VMEM((HEADS // 2 * AREA, LANES), f32),
        pltpu.VMEM((WS, WS, LANES), f32),
        pltpu.VMEM((D, 3 * PAD), bf16),
    ]


RESIDENT = pl.BlockSpec(memory_space=pltpu.VMEM)
PARAMS = pltpu.CompilerParams(vmem_limit_bytes=24 << 20)


def resident(*arrays):
    return [pltpu.with_memory_space_constraint(a, pltpu.VMEM) for a in arrays]


def work(flops):
    return pl.CostEstimate(flops=int(flops), transcendentals=0, bytes_accessed=1 << 20)


def edge_attention(tokens, gains, qkv_weight, proj_weight, table):
    side = (tokens.shape[0], WS, D)
    last = tokens.shape[1] // WS - 1
    full = lambda a: pl.BlockSpec(a.shape, lambda i: (0,) * a.ndim)
    return pl.pallas_call(
        edge_kernel,
        grid=(1,),
        in_specs=[
            pl.BlockSpec(side, lambda i: (0, 0, 0)),
            pl.BlockSpec(side, lambda i: (0, last, 0)),
            full(gains),
            full(qkv_weight),
            full(proj_weight),
            full(table),
        ],
        out_specs=[RESIDENT] * 8,
        out_shape=[
            pltpu.VMEM(side, f32),
            pltpu.VMEM(side, f32),
            pltpu.VMEM(side, bf16),
            pltpu.VMEM(side, bf16),
            pltpu.VMEM(side, bf16),
            pltpu.VMEM(side, bf16),
            pltpu.VMEM((HEADS // 2 * AREA, LANES), f32),
            pltpu.VMEM((D, 3 * PAD), bf16),
        ],
        scratch_shapes=[pltpu.VMEM((WS, WS, LANES), f32)],
        compiler_params=PARAMS,
        cost_estimate=work(5e8),
        name="edge_attention",
    )(
        *[
            pltpu.with_memory_space_constraint(a, pltpu.HBM)
            for a in (tokens, tokens, gains, qkv_weight, proj_weight, table)
        ]
    )


def inner_attention(tokens, gains, padded, proj_weight, bias, edges):
    return pl.pallas_call(
        inner_kernel,
        grid=(tokens.shape[0] // (4 * WS),),
        in_specs=[RESIDENT] * 9,
        out_specs=[RESIDENT] * 2,
        out_shape=[pltpu.VMEM(tokens.shape, f32), pltpu.VMEM(tokens.shape, bf16)],
        compiler_params=PARAMS,
        cost_estimate=work(8e9),
        name="inner_attention",
    )(*resident(tokens, gains, padded, proj_weight, bias, *edges))


def low_half(value):
    lane = lax.broadcasted_iota(jnp.int32, value.shape, value.ndim - 1)
    return jnp.where(lane < D - LANES, value, 0.0)


def join_halves(first, second):
    lane = lax.broadcasted_iota(jnp.int32, first.shape, 1)
    return jnp.where(lane < D - LANES, first, pltpu.roll(second, D - LANES, 1))


def shuffled_kernel(
    got_ref, gain_ref, qkv_ref, proj_ref, table_ref, out_ref, bias_s, rows_s, qkv_s, window_s, piece_s
):
    prepare_attention(1, table_ref, qkv_ref, bias_s, rows_s, qkv_s)
    blocks = WS * 2

    def gather(a, carry):
        for c in range(blocks):
            piece = got_ref[a * blocks + c].astype(f32)
            upper = piece[SEGMENT:]
            upper = jnp.concatenate(
                [low_half(upper), low_half(pltpu.roll(upper, D - LANES, 1))], axis=0
            )
            place = pl.ds(
                (c % 2) * SEGMENT * WINDOW_ROWS + a * WS + c // 2, SEGMENT, stride=WINDOW_ROWS
            )
            window_s[0, place, :] = piece[:SEGMENT]
            window_s[1, place, :] = upper
        return carry

    lax.fori_loop(0, WS, gather, 0, unroll=4)
    masks = attention_masks()

    def windows(c, carry):
        starts = [(c * TOGETHER + n) * WINDOW_ROWS for n in range(TOGETHER)]
        current = jnp.concatenate(
            [
                jnp.concatenate(
                    [window_s[t, pl.ds(start, AREA), :] for start in starts], axis=0
                )
                for t in range(2)
            ],
            axis=1,
        )[:, 0:D]
        after = attention(
            current, gain_ref[0, 1:2, :], qkv_s[...], proj_ref[1], bias_s[...], masks, TOGETHER
        )
        for n, start in enumerate(starts):
            window_s[0, pl.ds(start, AREA), :] = after[n * AREA : (n + 1) * AREA, 0:LANES]
            window_s[1, pl.ds(start, AREA), 0 : D - LANES] = after[
                n * AREA : (n + 1) * AREA, LANES:D
            ]
        return carry

    lax.fori_loop(0, 2 * SEGMENT // TOGETHER, windows, 0)

    below = lax.axis_index("row") < WS // 2
    beside = lax.axis_index("block") < WS // 2
    row_step = jnp.where(below, 1, -1)
    row_window = jnp.where(below, 0, 3)
    col_window = jnp.where(beside, 0, 3)

    def scatter(a, carry):
        other_a = a + row_step
        row_keep = jnp.where((other_a >= 0) & (other_a < WS), 1.0, 0.0).astype(f32)
        other_a = jnp.clip(other_a, 0, WS - 1)
        for c in range(blocks):
            b, core = c // 2, c % 2
            other_b = b + (jnp.where(beside, 1, 0) if core else jnp.where(beside, 0, -1))
            col_keep = jnp.where((other_b >= 0) & (other_b < WS), 1.0, 0.0).astype(f32)
            other_b = jnp.clip(other_b, 0, WS - 1)
            base = core * SEGMENT
            other = (1 - core) * SEGMENT
            main = pl.ds(base * WINDOW_ROWS + a * WS + b, SEGMENT, stride=WINDOW_ROWS)
            row = pl.ds(
                (base + row_window * 4) * WINDOW_ROWS + other_a * WS + b, 4, stride=WINDOW_ROWS
            )
            col = pl.ds(
                (other + col_window) * WINDOW_ROWS + a * WS + other_b, 4, stride=4 * WINDOW_ROWS
            )
            corner = pl.ds(
                (other + row_window * 4 + col_window) * WINDOW_ROWS + other_a * WS + other_b, 1
            )
            keep = row_keep * col_keep
            piece_s[0:16] = window_s[0, main, :]
            piece_s[16:20] = window_s[0, row, :] * row_keep
            piece_s[20:24] = window_s[0, col, :] * col_keep
            upper = window_s[1, main, :]
            piece_s[24:32] = join_halves(upper[0:8], upper[8:16])
            piece_s[32:36] = join_halves(
                window_s[1, row, :] * row_keep, window_s[1, col, :] * col_keep
            )
            piece_s[36:37] = window_s[0, corner, :] * keep
            piece_s[37:38] = window_s[1, corner, :] * keep
            out_ref[a * blocks + c] = piece_s[...].astype(bf16)
        return carry

    piece_s[...] = jnp.zeros_like(piece_s)
    lax.fori_loop(0, WS, scatter, 0, unroll=4)


def shuffled_attention(got, gains, qkv_weight, proj_weight, table):
    shape = (got.shape[0], RETURN_ROWS, LANES)
    return pl.pallas_call(
        shuffled_kernel,
        in_specs=[RESIDENT] * 5,
        out_specs=RESIDENT,
        out_shape=pltpu.VMEM(shape, bf16),
        scratch_shapes=attention_scratch()
        + [
            pltpu.VMEM((2, 2 * SEGMENT * WINDOW_ROWS, LANES), f32),
            pltpu.VMEM((RETURN_ROWS, LANES), f32),
        ],
        compiler_params=PARAMS,
        cost_estimate=work(1e10),
        name="shuffled_attention",
    )(*resident(got, gains, qkv_weight, proj_weight, table))


def prepare_finish(layer, taps_ref, down_ref, taps_s, down_s):
    for t in range(KS * KS):
        taps_s[t] = jnp.broadcast_to(
            taps_ref[t, layer : layer + 1, :], (16, D)
        ).astype(bf16)
    down_s[...] = down_ref[layer].T


def convolve_row(padded_s, taps_s, shift_s, row, width):
    total = None
    for v in range(KS):
        part = None
        for u in range(KS):
            x = padded_s[row + u].reshape(-1, 16, D)
            term = x * taps_s[u * KS + v][None]
            part = term if part is None else part + term
        part = part.reshape(-1, D).astype(f32)
        if v == HALO:
            part = part[:width]
        else:
            pieces = []
            for n, value in enumerate((part[:, :LANES], part[:, LANES:])):
                lanes = slice(0, value.shape[1])
                shift_s[v, n, SEGMENT : SEGMENT + RING, lanes] = value
                shift_s[v, n, WS:SEGMENT, lanes] = value[RING - WS :]
                start = SEGMENT + v - HALO
                pieces.append(shift_s[v, n, start : start + width, :])
            part = jnp.concatenate(pieces, axis=1)[:, 0:D]
        total = part if total is None else total + part
    return total


def feed_forward(after, gain, up, down):
    normed = layer_norm(after, gain).astype(bf16)
    raised = mxu(normed, up)
    hidden = (0.5 * raised * (1.0 + lax.erf(raised * 0.5**0.5))).astype(bf16)
    return (after + mxu(hidden, down)).astype(bf16)


def ring(middle, right, left):
    return jnp.concatenate(
        [middle.astype(f32), right.astype(f32), left.astype(f32)], axis=0
    ).astype(bf16)


def middle_kernel(
    sum_ref,
    normed_ref,
    left_ref,
    right_ref,
    gain_ref,
    taps_ref,
    up_ref,
    down_ref,
    out_ref,
    padded_s,
    after_s,
    taps_s,
    shift_s,
    down_s,
):
    step = pl.program_id(0)
    rows = 2 * WS
    width = sum_ref.shape[1]
    first = WS - HALO

    @pl.when(step == 0)
    def _():
        def body(r, carry):
            padded_s[r] = ring(normed_ref[first + r], right_ref[first + r], left_ref[first + r])
            return carry

        lax.fori_loop(0, padded_s.shape[0], body, 0)
        prepare_finish(0, taps_ref, down_ref, taps_s, down_s)

    def row(j, carry):
        total = sum_ref[WS + step * rows + j] + convolve_row(
            padded_s, taps_s, shift_s, step * rows + j, width
        )
        after_s[pl.ds(pl.multiple_of(j * width, width), width), :] = total
        return carry

    lax.fori_loop(0, rows, row, 0)
    outcome = feed_forward(after_s[...], gain_ref[2, 0:1, :], up_ref[0], down_s[...])
    out_ref[pl.ds(step * rows, rows)] = outcome.reshape(rows, width, D)


def middle_finish(after, normed, left, right, gains, taps, up_weight, down_weight):
    height, width = normed.shape[:2]
    inner = height - 2 * WS
    return pl.pallas_call(
        middle_kernel,
        grid=(inner // (2 * WS),),
        in_specs=[RESIDENT] * 8,
        out_specs=RESIDENT,
        out_shape=pltpu.VMEM((inner, width, D), bf16),
        scratch_shapes=[
            pltpu.VMEM((inner + 2 * HALO, RING, D), bf16),
            pltpu.VMEM((2 * WS * width, D), f32),
            pltpu.VMEM((KS * KS, 16, D), bf16),
            pltpu.VMEM((KS, 2, SEGMENT + RING, LANES), f32),
            pltpu.VMEM((HID, D), bf16),
        ],
        compiler_params=PARAMS,
        cost_estimate=work(8e9),
        name="middle_finish",
    )(*resident(after, normed, left, right, gains, taps, up_weight, down_weight))


def turn_kernel(
    normed_ref, partner_ref, other_ref, left_ref, right_ref, facing_ref, behind_ref
):
    height = normed_ref.shape[0]
    even = lax.axis_index("core") == 0
    partner = partner_ref[...].astype(f32)
    other = other_ref[...].astype(f32)
    left_ref[...] = jnp.where(even, other, partner).astype(bf16)
    right_ref[...] = jnp.where(even, partner, other).astype(bf16)
    even = lax.axis_index("row") % 2 == 0
    for r in range(HALO):
        first = ring(normed_ref[r], right_ref[r], left_ref[r]).astype(f32)
        n = height - HALO + r
        last = ring(normed_ref[n], right_ref[n], left_ref[n]).astype(f32)
        facing_ref[r] = jnp.where(even, last, first).astype(bf16)
        behind_ref[r] = jnp.where(even, first, last).astype(bf16)


def turn(normed, partner, other):
    rows = (HALO, RING, D)
    return pl.pallas_call(
        turn_kernel,
        in_specs=[RESIDENT] * 3,
        out_specs=[RESIDENT] * 4,
        out_shape=[
            pltpu.VMEM(partner.shape, bf16),
            pltpu.VMEM(partner.shape, bf16),
            pltpu.VMEM(rows, bf16),
            pltpu.VMEM(rows, bf16),
        ],
        compiler_params=PARAMS,
        name="turn",
    )(*resident(normed, partner, other))


def outer_kernel(
    sum_ref,
    middle_ref,
    normed_ref,
    partner_ref,
    other_ref,
    left_ref,
    right_ref,
    gain_ref,
    taps_ref,
    up_ref,
    down_ref,
    send_ref,
    padded_s,
    after_s,
    taps_s,
    shift_s,
    down_s,
    piece_s,
):
    step = pl.program_id(0)
    height, width, _ = normed_ref.shape
    rows = WS
    repeats = height // WS

    @pl.when(step == 0)
    def _():
        even = lax.axis_index("row") % 2 == 0
        for r in range(HALO):
            partner = partner_ref[r].astype(f32)
            other = other_ref[r].astype(f32)
            padded_s[r] = jnp.where(even, other, partner).astype(bf16)
            padded_s[height + HALO + r] = jnp.where(even, partner, other).astype(bf16)

        def body(r, carry):
            padded_s[r + HALO] = ring(normed_ref[r], right_ref[r], left_ref[r])
            return carry

        lax.fori_loop(0, WS + HALO, body, 0)
        lax.fori_loop(height - WS - HALO, height, body, 0)
        prepare_finish(0, taps_ref, down_ref, taps_s, down_s)

    def row(j, carry):
        part, q = j // rows, j % rows
        r = part * (height - WS) + step * rows + q
        total = sum_ref[r] + convolve_row(padded_s, taps_s, shift_s, r, width)
        after_s[pl.ds(pl.multiple_of(j * width, width), width), :] = total
        return carry

    lax.fori_loop(0, 2 * rows, row, 0)
    outcome = feed_forward(after_s[...], gain_ref[2, 0:1, :], up_ref[0], down_s[...]).astype(f32)
    for m in range(repeats):
        for q in range(rows):
            if m in (0, repeats - 1):
                start = ((m > 0) * rows + q) * width
                line = outcome[start : start + width]
            else:
                line = middle_ref[(m - 1) * WS + step * rows + q].astype(f32)
            for n in range(width // SEGMENT):
                value = line[n * SEGMENT : (n + 1) * SEGMENT]
                place = pl.ds((q * SEGMENT + m * 4 + n) * PIECE_STRIDE, SEGMENT)
                piece_s[0, place, :] = value[:, 0:LANES]
                piece_s[1, place, 0 : D - LANES] = value[:, LANES:D]
    for q in range(rows):
        for c in range(SEGMENT):
            place = pl.ds(q * SEGMENT * PIECE_STRIDE + c, SEGMENT, stride=PIECE_STRIDE)
            upper = piece_s[1, place, :]
            send_ref[(step * rows + q) * SEGMENT + c] = jnp.concatenate(
                [piece_s[0, place, :], join_halves(upper[0:8], upper[8:16])], axis=0
            ).astype(bf16)


def outer_finish(
    after, middle, normed, top, bottom, left, right, gains, taps, up_weight, down_weight, group
):
    height, width = normed.shape[:2]
    rows = WS
    return pl.pallas_call(
        outer_kernel,
        grid=(WS // rows,),
        in_specs=[RESIDENT] * 11,
        out_specs=RESIDENT,
        out_shape=pltpu.VMEM((group, PIECE_ROWS, LANES), bf16),
        scratch_shapes=[
            pltpu.VMEM((height + 2 * HALO, RING, D), bf16),
            pltpu.VMEM((2 * rows * width, D), f32),
            pltpu.VMEM((KS * KS, 16, D), bf16),
            pltpu.VMEM((KS, 2, SEGMENT + RING, LANES), f32),
            pltpu.VMEM((HID, D), bf16),
            pltpu.VMEM((2, rows * SEGMENT * PIECE_STRIDE, LANES), f32),
        ],
        compiler_params=PARAMS,
        cost_estimate=work(8e9),
        name="outer_finish",
    )(
        *resident(
            after,
            middle,
            normed,
            top,
            bottom,
            left,
            right,
            gains,
            taps,
            up_weight,
            down_weight,
        )
    )


def second_kernel(
    back_ref,
    gain_ref,
    taps_ref,
    up_ref,
    down_ref,
    out_ref,
    padded_s,
    sum_s,
    after_s,
    taps_s,
    shift_s,
    down_s,
    piece_s,
):
    step = pl.program_id(0)
    rows, width, _ = out_ref.shape
    height = sum_s.shape[0]
    repeats = height // WS

    @pl.when(step == 0)
    def _():
        prepare_finish(1, taps_ref, down_ref, taps_s, down_s)

        def line(n):
            pieces = []
            for m in range(width // SEGMENT + 1):
                if n < 4 and m < 4:
                    low, high, half = 4 * n + m, 24 + (4 * n + m) % 8, (4 * n + m) // 8
                elif m < 4:
                    low, high, half = 16 + m, 32 + m, 0
                elif n < 4:
                    low, high, half = 20 + n, 32 + n, 1
                else:
                    low, high, half = 36, 37, 0
                at = lambda k: piece_s[pl.ds(k, SEGMENT, stride=RETURN_STRIDE), :]
                upper = at(high)
                if half:
                    upper = pltpu.roll(upper, D - LANES, 1)
                pieces.append(jnp.concatenate([at(low), upper], axis=1)[:, 0:D])
            return jnp.concatenate(pieces, axis=0)

        def body(r, carry):
            for c in range(SEGMENT):
                piece_s[c * RETURN_STRIDE : c * RETURN_STRIDE + RETURN_ROWS, :] = back_ref[
                    r * SEGMENT + c
                ].astype(f32)
            lines = [line(n) for n in range(repeats + 1)]
            normed = layer_norm(jnp.concatenate(lines, axis=0), gain_ref[1, 1:2, :]).astype(bf16)
            for n in range(repeats):
                sum_s[r + WS * n] = lines[n][0:width]
                padded_s[HALO + r + WS * n] = normed[n * RING : (n + 1) * RING]
            spare = height + 2 * HALO
            target = jnp.where(
                r < HALO, HALO + height + r, jnp.where(r >= WS - HALO, HALO + r - WS, spare)
            )
            padded_s[target] = normed[repeats * RING :]
            return carry

        lax.fori_loop(0, WS, body, 0, unroll=2)

    def row(j, carry):
        r = step * rows + j
        total = sum_s[r] + convolve_row(padded_s, taps_s, shift_s, r, width)
        after_s[pl.ds(pl.multiple_of(j * width, width), width), :] = total
        return carry

    lax.fori_loop(0, rows, row, 0)
    outcome = feed_forward(after_s[...], gain_ref[2, 1:2, :], up_ref[1], down_s[...])
    out_ref[...] = outcome.reshape(rows, width, D)


def second_finish(back, shape, gains, taps, up_weight, down_weight):
    height, width = shape[:2]
    return pl.pallas_call(
        second_kernel,
        grid=(height // (2 * WS),),
        in_specs=[RESIDENT] * 5,
        out_specs=pl.BlockSpec((2 * WS, width, D), lambda i: (i, 0, 0)),
        out_shape=jax.ShapeDtypeStruct(shape, bf16),
        scratch_shapes=[
            pltpu.VMEM((height + 2 * HALO + 1, RING, D), bf16),
            pltpu.VMEM((height, width, D), f32),
            pltpu.VMEM((2 * WS * width, D), f32),
            pltpu.VMEM((KS * KS, 16, D), bf16),
            pltpu.VMEM((KS, 2, SEGMENT + RING, LANES), f32),
            pltpu.VMEM((HID, D), bf16),
            pltpu.VMEM((SEGMENT * RETURN_STRIDE, LANES), f32),
        ],
        compiler_params=PARAMS,
        cost_estimate=work(1e10),
        name="second_finish",
    )(*resident(back, gains, taps, up_weight, down_weight))


def swap(facing, behind, axes):
    count = lax.axis_size(axes)

    def pairs(start):
        return [pair for i in range(start, count - 1, 2) for pair in ((i, i + 1), (i + 1, i))]

    return lax.ppermute(facing, axes, pairs(0)), lax.ppermute(behind, axes, pairs(1))


def on_device(
    tokens, norm_gain, qkv_weight, proj_weight, bias_table, conv_weight, up_weight, down_weight
):
    members = ("row", "block", "core")
    columns = ("block", "core")
    gains = norm_gain.transpose(1, 0, 2)
    table = bias_table.transpose(1, 0, 2)
    taps = conv_weight.transpose(1, 0, 2)
    down_weight = down_weight.transpose(0, 2, 1)
    *edges, facing, behind, bias, padded = edge_attention(tokens, gains, qkv_weight, proj_weight, table)
    partner, other = swap(facing, behind, columns)
    after, normed = inner_attention(tokens, gains, padded, proj_weight, bias, edges)
    left, right, facing, behind = turn(normed, partner, other)
    partner, other = swap(facing, behind, "row")
    middle = middle_finish(after, normed, left, right, gains, taps, up_weight, down_weight)
    outgoing = outer_finish(
        after,
        middle,
        normed,
        partner,
        other,
        left,
        right,
        gains,
        taps,
        up_weight,
        down_weight,
        lax.axis_size(members),
    )
    got = lax.all_to_all(outgoing, members, 0, 0, tiled=True)
    branch = shuffled_attention(got, gains, qkv_weight, proj_weight, table)
    back = lax.all_to_all(branch, members, 0, 0, tiled=True)
    return second_finish(back, tokens.shape, gains, taps, up_weight, down_weight)


def solution(mesh):
    split = Mesh(
        mesh.devices.reshape(mesh.shape["row"], mesh.shape["col"] // 2, 2), ("row", "block", "core")
    )
    spec = P("row", ("block", "core"), None)
    return jax.shard_map(
        on_device, mesh=split, in_specs=(spec,) + (P(),) * 7, out_specs=spec, check_vma=False
    )
```
